32 devices in a mesh: panel: 8 (over z, core), rhs: 4 (over y, x).
Axes of the slice: x: 2, y: 2, z: 4, core: 2. Of those that a mesh axis runs over, the one named last changes fastest.
Arguments:
- pivot_rhs: float32 [2, 2048, 512], P(None, 'panel', 'rhs'), may hold values from -6 to 6
- update_rhs: float32 [4096, 512], P('panel', 'rhs'), may hold values from -6 to 6
- parent_rhs: float32 [4096, 512], P('panel', 'rhs'), may hold values from -6 to 6
- lower_pivot: bfloat16 [2, 2048, 2048], P(None, 'panel', 'rhs'), may hold values from -1 to 1.4, as said below
- lower_update: bfloat16 [4096, 2048], P('panel', 'rhs'), may hold values from -0.125 to 0.125
- parent_lower: bfloat16 [4096, 4096], P('panel', 'rhs'), may hold values from -1 to 1.4, as said below
- parent_upper: bfloat16 [4096, 4096], P('panel', 'rhs'), may hold values from -1 to 1.4, as said below
- upper_pivot: bfloat16 [2, 2048, 2048], P(None, 'panel', 'rhs'), may hold values from -1 to 1.4, as said below
- upper_update: bfloat16 [2, 2048, 2048], P(None, 'panel', 'rhs'), may hold values from -0.125 to 0.125
- maps: int32 [4096], replicated, may hold values from 0 to 4095, as said below
Outputs:
- parent_solution: float32 [4096, 512], P('panel', 'rhs')
- child_solution: float32 [2, 2048, 512], P(None, 'panel', 'rhs')
The draws below stay inside these ranges and needn't reach their ends.
Inputs may be any that keep to these rules, and one draw needn't show every extreme that they name: `maps`: for each child k, entry k * 2048 + i is 2 * i + b with b equal to 0 or 1; both values of b occur for each child in every draw. `lower_pivot`: each block is lower triangular, diagonal 0.6 to 1.4. `upper_pivot`: each block is upper triangular, diagonal 0.6 to 1.4. `parent_lower`: lower triangular, diagonal 0.6 to 1.4. `parent_upper`: upper triangular, diagonal 0.6 to 1.4.
All inputs are finite; a program needn't handle non-finite values.
Results may differ from the reference program's by a relative error of at most 0.0054.
Values may be sent and summed in bfloat16 or wider, within the bound.
A program may use at most 64 MiB of HBM per device.

```python
import math
import jax
import jax.numpy as jnp
from jax import lax

F = 4096
KC = 2048
FU = 2048
RHS = 512


def triangle(random_key, block_count, matrix_order, lower_side):
    shape_full = (block_count, matrix_order, matrix_order)
    noise = jax.random.normal(random_key, shape_full, jnp.float32)
    noise = noise / math.sqrt(matrix_order)
    row_ids = lax.broadcasted_iota(jnp.int32, (matrix_order, matrix_order), 0)
    col_ids = lax.broadcasted_iota(jnp.int32, (matrix_order, matrix_order), 1)
    if lower_side:
        keeper = row_ids > col_ids
    else:
        keeper = row_ids < col_ids
    diagonal_scale = jax.random.uniform(jax.random.fold_in(random_key, 7), (block_count, matrix_order, 1), jnp.float32, 0.6, 1.4)
    identity = jnp.where(row_ids == col_ids, 1.0, 0.0).astype(jnp.float32)
    return jnp.where(keeper[None], noise, 0.0) + identity[None] * diagonal_scale


def draw_lower_pivot(key, part):
    return triangle(jax.random.fold_in(key, 101), 2, KC, True).astype(jnp.bfloat16)


def draw_upper_pivot(key, part):
    return triangle(jax.random.fold_in(key, 103), 2, KC, False).astype(jnp.bfloat16)


def draw_parent_lower(key, part):
    return triangle(jax.random.fold_in(key, 107), 1, F, True).reshape(F, F).astype(jnp.bfloat16)


def draw_parent_upper(key, part):
    return triangle(jax.random.fold_in(key, 109), 1, F, False).reshape(F, F).astype(jnp.bfloat16)


def draw_maps(key, part):
    local = lax.broadcasted_iota(jnp.int32, (FU,), 0)
    first_bits = jax.random.randint(jax.random.fold_in(key, 211), (FU,), 0, 2)
    first_bits = jnp.where(local == 0, 0, first_bits)
    first_bits = jnp.where(local == FU - 1, 1, first_bits)
    second_bits = jax.random.randint(jax.random.fold_in(key, 212), (FU,), 0, 2)
    second_bits = jnp.where(local == 0, 1, second_bits)
    second_bits = jnp.where(local == FU - 1, 0, second_bits)
    return jnp.concatenate([2 * local + first_bits, 2 * local + second_bits]).astype(jnp.int32)


def levels(key, dims, shards, smallest, top_value):
    factor_of, own = 1.0, jax.random.fold_in(key, 6)
    for axis_at, blocks in shards:
        draws = jnp.exp(jax.random.uniform(jax.random.fold_in(own, axis_at), (blocks,), jnp.float32, smallest / len(shards), top_value / len(shards)))
        factor_of = factor_of * jnp.repeat(draws, dims[axis_at] // blocks).reshape([-1 if axis == axis_at else 1 for axis in range(len(dims))])
    return factor_of


def normal_values(stream_key, extent, spread, bound, pieces=(), held_as=jnp.bfloat16):
    level = levels(stream_key, extent, pieces, -0.22, 0.18) if pieces else 1.0
    drawn = jax.random.normal(stream_key, extent, jnp.float32) * spread * level
    return jnp.minimum(jnp.maximum(drawn, -bound), bound).astype(held_as)


def setup_inputs(seed: int = 0) -> dict:
    key_of = jax.random.split(jax.random.key(seed), 11)
    return {
        "pivot_rhs": normal_values(key_of[0], (2, KC, RHS), 1.0, 6.0, ((1, 8), (2, 4)), jnp.float32),
        "update_rhs": normal_values(key_of[1], (2 * FU, RHS), 1.0, 6.0, ((0, 8), (1, 4)), jnp.float32),
        "parent_rhs": normal_values(key_of[2], (F, RHS), 1.0, 6.0, ((0, 8), (1, 4)), jnp.float32),
        "lower_pivot": draw_lower_pivot(jax.random.fold_in(key_of[10], 71), 0),
        "lower_update": normal_values(key_of[4], (2 * FU, KC), KC ** -0.5, 0.125, ((0, 8), (1, 4))),
        "parent_lower": draw_parent_lower(jax.random.fold_in(key_of[10], 71), 0),
        "parent_upper": draw_parent_upper(jax.random.fold_in(key_of[10], 71), 0),
        "upper_pivot": draw_upper_pivot(jax.random.fold_in(key_of[10], 71), 0),
        "upper_update": normal_values(key_of[8], (2, KC, FU), FU ** -0.5, 0.125, ((1, 8), (2, 4))),
        "maps": draw_maps(jax.random.fold_in(key_of[10], 71), 0),
    }


def product(left, right):
    return jnp.dot(left, right, preferred_element_type=jnp.float32)


def reference(pivot_rhs, update_rhs, parent_rhs, lower_pivot, lower_update, parent_lower, parent_upper, upper_pivot, upper_update, maps):
    pivot_input = pivot_rhs.astype(jnp.bfloat16)
    solved = []
    updates = []
    for member in range(2):
        source = pivot_input[member]
        solved.append(product(lower_pivot[member], source))
        updates.append(update_rhs[member * FU:(member + 1) * FU] + product(lower_update[member * FU:(member + 1) * FU], source))
    pivot_half = jnp.stack(solved, axis=0).astype(jnp.bfloat16)
    update_half = jnp.concatenate(updates, axis=0).astype(jnp.bfloat16)
    widened = lax.optimization_barrier(update_half).astype(jnp.float32)
    scattered = jnp.zeros(parent_rhs.shape, jnp.float32).at[maps].add(widened)
    parent_sum = parent_rhs + scattered
    parent_mid = product(parent_lower, parent_sum.astype(jnp.bfloat16))
    parent_solution = product(parent_upper, parent_mid.astype(jnp.bfloat16))
    solution_half = parent_solution.astype(jnp.bfloat16)
    blocks = []
    for member in range(2):
        picked = jnp.take(solution_half, maps[member * FU:(member + 1) * FU], axis=0)
        direct = product(upper_pivot[member], pivot_half[member])
        blocks.append(direct + product(upper_update[member], picked))
    return parent_solution, jnp.stack(blocks, axis=0)
```

```python
import functools

import jax
import jax.numpy as jnp
from jax import lax
from jax.experimental import pallas as pl
from jax.experimental.pallas import tpu as pltpu
from jax.sharding import PartitionSpec as P

BF = jnp.bfloat16
F32 = jnp.float32
MESH = pl.DeviceIdType.MESH


def dot(left, right):
    return jnp.dot(left, right, preferred_element_type=F32)


def plain_kernel(
    panels,
    cols,
    pivot_rhs,
    update_rhs,
    parent_rhs,
    lower_pivot,
    lower_update,
    parent_lower,
    parent_upper,
    upper_pivot,
    upper_update,
    row_map,
    col_map,
    parent_out,
    child_out,
    pin,
    phalf,
    vec,
    x_pin,
    x_half,
    x_par,
    s_up,
    r_up,
    s_piv,
    r_piv,
    s_par,
    r_par,
    s_ch,
    r_ch,
    uhalf,
    moved,
    picked,
    direct,
    par_sum,
    spread_sum,
    child_sum,
    g_send,
    g_recv,
    f_send,
    rs_send,
    rs_recv,
    sh_send,
    sh_recv,
):
    me_p, me_r = lax.axis_index("panel"), lax.axis_index("rhs")
    total = panels * cols
    me = me_p * cols + me_r
    core = lax.rem(me_p, 2)
    mate = me_p + 1 - 2 * core
    per = panels // cols
    half = panels // 2
    m = parent_rhs.shape[0]
    mk = pivot_rhs.shape[1]
    child = me_p // half

    barrier = pltpu.get_barrier_semaphore()

    @pl.loop(1, total)
    def _(step):
        other = lax.rem(me + step, total)
        pl.semaphore_signal(
            barrier,
            inc=1,
            device_id=(other // cols, lax.rem(other, cols)),
            device_id_type=MESH,
        )

    pin[...] = pivot_rhs[...].astype(BF)
    direct[...] = jnp.zeros_like(direct)
    pl.semaphore_wait(barrier, total - 1)

    group = me_p // per
    last = cols - 1

    def every(source, goal):
        return None

    def below(source, goal):
        return goal >= source

    def above(source, goal):
        return goal <= source

    def guard(condition, action):
        if condition is None:
            action()
        else:
            pl.when(condition)(action)

    def both(first, second):
        return second if first is None else jnp.logical_and(first, second)

    def spot(buffer, depth, column, part, lead):
        rows = pl.ds(pl.multiple_of(part * depth, depth), depth)
        return buffer.at[column, slice(None) if lead is None else pl.ds(lead, 1), rows, :]

    class Gather:
        def __init__(self, stage, block, buffer, depth, keep, lead):
            self.stage, self.block, self.buffer, self.depth = stage, block, buffer, depth
            self.keep, self.lead = keep, lead
            self.active = keep(me_r, group)

        def place(self, column, part, panel):
            return spot(self.buffer, self.depth, column, part, self.lead(panel))

        def piece(self, panel):
            lead = self.lead(panel)
            return self.block if lead is None else self.block.at[pl.ds(lead, 1)]

        def goal(self, step):
            return lax.rem(me_p // 2 + step, half) * 2 + core

        def copy(self, step):
            goal = self.goal(step)
            return pltpu.make_async_remote_copy(
                src_ref=self.piece(goal),
                dst_ref=self.place(me_r, lax.rem(me_p, per), goal),
                send_sem=g_send.at[self.stage, step],
                recv_sem=g_recv.at[self.stage, me_r, lax.rem(me_p, per)],
                device_id=(goal, group),
                device_id_type=MESH,
            )

        def sends(self, action):
            for step in list(range(1, half)) + [0]:
                condition = self.keep(group, self.goal(step) // per)
                if step == 0:
                    condition = both(condition, group != me_r)
                guard(condition, functools.partial(action, step))

        def start(self):
            self.sends(lambda step: self.copy(step).start())

            @pl.when(group == me_r)
            def _():
                part = lax.rem(me_p, per)
                pltpu.make_async_copy(
                    self.piece(me_p),
                    self.place(me_r, part, me_p),
                    g_recv.at[self.stage, me_r, part],
                ).start()

        def landed(self, column, part):
            place = self.place(column, part, me_p)
            pltpu.make_async_copy(place, place, g_recv.at[self.stage, column, part]).wait()

        def forward(self, step, pair):
            column = lax.rem(me_r + 1 + step, cols)
            part = 2 * pair + core
            return pltpu.make_async_remote_copy(
                src_ref=self.place(column, part, me_p),
                dst_ref=self.place(column, part, me_p),
                send_sem=f_send.at[self.stage, step, pair],
                recv_sem=g_recv.at[self.stage, column, part],
                device_id=(mate, me_r),
                device_id_type=MESH,
            )

        def pass_on(self):
            def action():
                for step in [last] + list(range(last)):
                    for pair in range(per // 2):
                        self.landed(lax.rem(me_r + 1 + step, cols), 2 * pair + core)
                        self.forward(step, pair).start()

            guard(self.active, action)

        def arrive(self, step):
            column = lax.rem(me_r + 1 + step, cols)
            for pair in range(per // 2):
                self.landed(column, 2 * pair + 1 - core)
            return column

        def finish(self):
            self.sends(lambda step: self.copy(step).wait_send())

            def action():
                for step in range(cols):
                    for pair in range(per // 2):
                        self.forward(step, pair).wait_send()

            guard(self.active, action)

    class Scatter:
        def __init__(self, stage, source, target, keep):
            self.stage, self.source, self.target, self.keep = stage, source, target, keep
            self.active = keep(me_r, group)

        def copy(self, step):
            return pltpu.make_async_remote_copy(
                src_ref=self.source.at[step],
                dst_ref=self.target.at[step],
                send_sem=rs_send.at[self.stage, step],
                recv_sem=rs_recv.at[self.stage, step],
                device_id=(me_p, lax.rem(me_r + 1 + step, cols)),
                device_id_type=MESH,
            )

        def add(self, total_ref):
            for step in range(last):
                sender = lax.rem(me_r + last - step, cols)

                def action(step=step):
                    self.copy(step).wait_recv()
                    total_ref[...] += self.target[step].astype(F32)

                guard(self.keep(sender, group), action)

        def finish(self):
            def action():
                for step in range(last):
                    self.copy(step).wait_send()

            guard(self.active, action)

    def targets(ref, k, index, size, base):
        if ref.shape[0] == 2:
            return ref[k : k + 1, :]
        start = pl.multiple_of(k * (ref.shape[1] // 2) + index * size, 128)
        return ref[:, pl.ds(start, size)] - base

    def whole(panel):
        return None

    def same(panel):
        return panel // half

    def other(panel):
        return 1 - panel // half

    g_own = Gather(0, pin, x_pin, mk, every, same)
    g_other = Gather(5, pin, x_pin, mk, below, other)
    g_low = Gather(1, vec.at[0], x_par.at[0], m, below, whole)
    g_half = Gather(2, phalf, x_half, mk, above, whole)
    g_up = Gather(3, vec.at[1], x_par.at[1], m, above, whole)
    g_all = Gather(4, vec.at[2], x_par.at[2], m, every, whole)
    t_up = Scatter(0, s_up, r_up, every)
    t_piv = Scatter(1, s_piv, r_piv, below)
    t_low = Scatter(2, s_par.at[0], r_par.at[0], below)
    t_high = Scatter(3, s_par.at[1], r_par.at[1], above)
    t_child = Scatter(4, s_ch, r_ch, every)

    g_own.start()
    g_other.start()

    width = upper_update.shape[2]
    for k in range(2):
        rows = lax.broadcasted_iota(jnp.int32, (per * m, width), 0)
        chosen = (rows == targets(col_map, k, me_r, width, me_r * per * m)).astype(F32).astype(BF)
        picked[k] = lax.dot_general(
            upper_update[k], chosen, (((1,), (1,)), ((), ())), preferred_element_type=F32
        ).astype(BF)
    spread_sum[...] = parent_rhs[...]

    g_own.pass_on()
    for step in range(cols):
        column = g_own.arrive(step)
        value = dot(lower_update[...], x_pin[column, child])
        if step < last:
            s_up[step] = value.astype(BF)
            t_up.copy(step).start()
        else:
            par_sum[...] = update_rhs[...] + value
    g_other.pass_on()
    t_up.add(par_sum)
    update = par_sum[...].astype(BF)
    uhalf[0] = update[: m // 2]
    uhalf[1] = update[m // 2 :]
    first = lax.rem(me_p, half) * 2

    def shuffle(side):
        return pltpu.make_async_remote_copy(
            src_ref=uhalf.at[side],
            dst_ref=moved.at[child],
            send_sem=sh_send.at[side],
            recv_sem=sh_recv.at[child],
            device_id=(first + side, me_r),
            device_id_type=MESH,
        )

    for side in range(2):

        @pl.when(first + side != me_p)
        def _():
            shuffle(side).start()

        @pl.when(first + side == me_p)
        def _():
            pltpu.make_async_copy(uhalf.at[side], moved.at[child], sh_recv.at[child]).start()

    child_sum[...] = jnp.zeros_like(child_sum)

    def pivots():
        for step in range(cols):
            column = g_other.arrive(step)
            for k in range(2):
                value = dot(lower_pivot[k], x_pin[column, k])
                if step < last:
                    s_piv[step, k] = value.astype(BF)
                else:
                    child_sum[k] = value
            if step < last:
                t_piv.copy(step).start()

    guard(g_other.active, pivots)

    rows = lax.broadcasted_iota(jnp.int32, (m, m // 2), 0)
    for k in range(2):
        pltpu.make_async_copy(moved.at[k], moved.at[k], sh_recv.at[k]).wait()
        chosen = (rows == targets(row_map, k, me_p, m // 2, me_p * m)).astype(F32).astype(BF)
        spread_sum[...] += dot(chosen, moved[k])
    vec[0, 0] = spread_sum[...].astype(BF)
    g_low.start()

    t_piv.add(child_sum)
    phalf[...] = child_sum[...].astype(BF)
    g_half.start()

    def parent(level, gather, scatter, factor):
        par_sum[...] = jnp.zeros_like(par_sum)
        gather.pass_on()

        def action():
            for step in range(cols):
                column = gather.arrive(step)
                value = dot(factor[...], x_par[level, column, 0])
                if step < last:
                    s_par[level, step] = value.astype(BF)
                    scatter.copy(step).start()
                else:
                    par_sum[...] = value

        guard(gather.active, action)
        scatter.add(par_sum)
        vec[level + 1, 0] = par_sum[...].astype(BF)

    parent(0, g_low, t_low, parent_lower)
    g_up.start()
    g_half.pass_on()

    def known():
        for step in range(cols):
            column = g_half.arrive(step)
            for k in range(2):
                direct[step, k] = dot(upper_pivot[k], x_half[column, k])

    guard(g_half.active, known)
    parent(1, g_up, t_high, parent_upper)
    g_all.start()
    parent_out[...] = par_sum[...]

    g_all.pass_on()
    for step in range(cols):
        column = g_all.arrive(step)
        for k in range(2):
            value = direct[step, k] + dot(picked[k], x_par[2, column, 0])
            if step < last:
                s_ch[step, k] = value.astype(BF)
            else:
                child_out[k] = value
        if step < last:
            t_child.copy(step).start()
    for gather in (g_own, g_other, g_low, g_half, g_up, g_all):
        gather.finish()
    for side in range(2):

        @pl.when(first + side != me_p)
        def _():
            shuffle(side).wait_send()

    t_child.add(child_out)
    for scatter in (t_up, t_piv, t_low, t_high, t_child):
        scatter.finish()


def plain_shards(panels, cols, *arguments):
    *arrays, maps = arguments
    m, width = arrays[1].shape
    mk = arrays[0].shape[1]
    per = panels // cols
    sides = maps.reshape(2, -1)
    me_p, me_r = lax.axis_index("panel"), lax.axis_index("rhs")
    wide = arrays[8].shape[2]

    def cut(index, size, base):
        if size % 128 == 0:
            return maps.reshape(1, -1)
        return lax.dynamic_slice_in_dim(sides, index * size, size, 1) - base

    row_map = cut(me_p, m // 2, me_p * m)
    col_map = cut(me_r, wide, me_r * per * m)
    vm = pltpu.VMEM
    dma = pltpu.SemaphoreType.DMA
    return pl.pallas_call(
        functools.partial(plain_kernel, panels, cols),
        out_shape=(
            jax.ShapeDtypeStruct((m, width), F32),
            jax.ShapeDtypeStruct((2, mk, width), F32),
        ),
        in_specs=[pl.BlockSpec(memory_space=pltpu.VMEM)] * 11,
        out_specs=(pl.BlockSpec(memory_space=pltpu.VMEM),) * 2,
        scratch_shapes=[
            vm((2, mk, width), BF),
            vm((2, mk, width), BF),
            vm((3, 1, m, width), BF),
            vm((cols, 2, per * mk, width), BF),
            vm((cols, 2, per * mk, width), BF),
            vm((3, cols, 1, per * m, width), BF),
            vm((cols - 1, m, width), BF),
            vm((cols - 1, m, width), BF),
            vm((cols - 1, 2, mk, width), BF),
            vm((cols - 1, 2, mk, width), BF),
            vm((2, cols - 1, m, width), BF),
            vm((2, cols - 1, m, width), BF),
            vm((cols - 1, 2, mk, width), BF),
            vm((cols - 1, 2, mk, width), BF),
            vm((2, m // 2, width), BF),
            vm((2, m // 2, width), BF),
            vm((2, mk, per * m), BF),
            vm((cols, 2, mk, width), F32),
            vm((m, width), F32),
            vm((m, width), F32),
            vm((2, mk, width), F32),
            dma((6, panels // 2)),
            dma((6, cols, per)),
            dma((6, cols, per // 2)),
            dma((5, cols - 1)),
            dma((5, cols - 1)),
            dma((2,)),
            dma((2,)),
        ],
        compiler_params=pltpu.CompilerParams(
            collective_id=0, has_side_effects=True, vmem_limit_bytes=60 * 1024 * 1024
        ),
    )(*arrays, row_map, col_map)


SPLIT = 2


def dot_rows(left, right):
    return lax.dot_general(left, right, (((1,), (1,)), ((), ())), preferred_element_type=F32)


def split_kernel(
    panels,
    cols,
    pivot_rhs,
    update_rhs,
    parent_rhs,
    lower_pivot,
    lower_update,
    parent_lower,
    parent_upper,
    upper_pivot,
    upper_update,
    row_map,
    col_map,
    parent_out,
    child_out,
    pin,
    x_pin,
    uhalf,
    moved,
    chosen,
    vec,
    x_par,
    phalf,
    x_half,
    picked,
    direct,
    s_up,
    r_up,
    s_piv,
    r_piv,
    s_par,
    r_par,
    s_ch,
    r_ch,
    own_up,
    own_piv,
    own_par,
    own_ch,
    rhs_up,
    rhs_par,
    g_send,
    g_recv,
    f_send,
    rs_send,
    rs_recv,
    sh_send,
    sh_recv,
):
    me_p, me_r = lax.axis_index("panel"), lax.axis_index("rhs")
    total = panels * cols
    me = me_p * cols + me_r
    core = lax.rem(me_p, 2)
    mate = me_p + 1 - 2 * core
    half = panels // 2
    m, width = parent_rhs.shape
    mk = pivot_rhs.shape[1]
    wq = width // SPLIT
    child = me_p // half
    group = me_p // 2
    last = cols - 1
    chunks = range(SPLIT)

    barrier = pltpu.get_barrier_semaphore()

    @pl.loop(1, total)
    def _(step):
        other = lax.rem(me + step, total)
        pl.semaphore_signal(
            barrier,
            inc=1,
            device_id=(other // cols, lax.rem(other, cols)),
            device_id_type=MESH,
        )

    for k in range(2):
        turned = pivot_rhs[k].T.astype(BF)
        for q in chunks:
            pin[k, q] = turned[q * wq : (q + 1) * wq]
    with jax.named_scope("barrier"):
        pl.semaphore_wait(barrier, total - 1)

    def every(source, goal):
        return None

    def below(source, goal):
        return goal >= source

    def above(source, goal):
        return goal <= source

    def guard(condition, action):
        if condition is None:
            action()
        else:
            pl.when(condition)(action)

    def both(first, second):
        return second if first is None else jnp.logical_and(first, second)

    sent_place = lax.rem(me_r - group - 1 + 2 * cols, cols)

    class Gather:
        def __init__(self, stage, piece, place, keep):
            self.stage, self.piece, self.place, self.keep = stage, piece, place, keep
            self.active = keep(me_r, group)

        def goal(self, step):
            return lax.rem(group + step, half) * 2 + core

        def copy(self, q, step):
            goal = self.goal(step)
            return pltpu.make_async_remote_copy(
                src_ref=self.piece(q, goal),
                dst_ref=self.place(q, core, sent_place, goal),
                send_sem=g_send.at[self.stage, q, step],
                recv_sem=g_recv.at[self.stage, q, sent_place, core],
                device_id=(goal, group),
                device_id_type=MESH,
            )

        def sends(self, action):
            for step in list(range(1, half)) + [0]:
                condition = self.keep(group, self.goal(step) // 2)
                if step == 0:
                    condition = both(condition, group != me_r)
                guard(condition, functools.partial(action, step))

        def start(self, q):
            self.sends(lambda step: self.copy(q, step).start())

            @pl.when(group == me_r)
            def _():
                pltpu.make_async_copy(
                    self.piece(q, me_p),
                    self.place(q, core, last, me_p),
                    g_recv.at[self.stage, q, last, core],
                ).start()

        def landed(self, q, spot, part):
            place = self.place(q, part, spot, me_p)
            pltpu.make_async_copy(place, place, g_recv.at[self.stage, q, spot, part]).wait()

        def forward(self, q, spot):
            return pltpu.make_async_remote_copy(
                src_ref=self.place(q, core, spot, me_p),
                dst_ref=self.place(q, core, spot, me_p),
                send_sem=f_send.at[self.stage, q, spot],
                recv_sem=g_recv.at[self.stage, q, spot, core],
                device_id=(mate, me_r),
                device_id_type=MESH,
            )

        def pass_on(self, q):
            def action():
                for spot in [last] + list(range(last)):
                    self.landed(q, spot, core)
                    self.forward(q, spot).start()

            guard(self.active, action)

        def arrive(self, q):
            for spot in range(cols):
                self.landed(q, spot, 1 - core)

        def finish(self, q):
            self.sends(lambda step: self.copy(q, step).wait_send())

            def action():
                for spot in range(cols):
                    self.forward(q, spot).wait_send()

            guard(self.active, action)

    class Scatter:
        def __init__(self, stage, source, target, keep):
            self.stage, self.source, self.target, self.keep = stage, source, target, keep
            self.active = keep(me_r, group)

        def copy(self, q, step):
            return pltpu.make_async_remote_copy(
                src_ref=self.source(q).at[step],
                dst_ref=self.target(q).at[step],
                send_sem=rs_send.at[self.stage, q, step],
                recv_sem=rs_recv.at[self.stage, q, step],
                device_id=(me_p, lax.rem(me_r + 1 + step, cols)),
                device_id_type=MESH,
            )

        def give(self, q, value, own):
            rows = value.shape[0] // cols
            for step in range(last):
                self.source(q)[step] = value[step * rows : (step + 1) * rows].astype(BF)
                self.copy(q, step).start()
            own[...] = value[last * rows :]

        def add(self, q, total_ref):
            for step in range(last):
                sender = lax.rem(me_r + last - step, cols)

                def action(step=step):
                    self.copy(q, step).wait_recv()
                    total_ref[...] += self.target(q)[step].astype(F32)

                guard(self.keep(sender, group), action)

        def finish(self, q):
            def action():
                for step in range(last):
                    self.copy(q, step).wait_send()

            guard(self.active, action)

    def targets(ref, k, index, size, base):
        if ref.shape[0] == 2:
            return ref[k : k + 1, :]
        start = pl.multiple_of(k * (ref.shape[1] // 2) + index * size, 128)
        return ref[:, pl.ds(start, size)] - base

    def same(panel):
        return panel // half

    def other(panel):
        return 1 - panel // half

    def pins(side):
        return (
            lambda q, goal: pin.at[side(goal), q],
            lambda q, part, spot, goal: x_pin.at[side(goal), q, part, spot],
        )

    def level_parts(level):
        return (
            lambda q, goal: vec.at[level, q],
            lambda q, part, spot, goal: x_par.at[level, q, part, spot],
        )

    g_own = Gather(0, *pins(same), every)
    g_other = Gather(5, *pins(other), below)
    g_low = Gather(1, *level_parts(0), below)
    g_up = Gather(3, *level_parts(1), above)
    g_all = Gather(4, *level_parts(2), every)
    g_half = Gather(
        2, lambda q, goal: phalf, lambda q, part, spot, goal: x_half.at[part, spot], above
    )
    t_up = Scatter(0, lambda q: s_up.at[q], lambda q: r_up.at[q], every)
    t_piv = Scatter(1, lambda q: s_piv, lambda q: r_piv, below)
    t_low = Scatter(2, lambda q: s_par.at[0, q], lambda q: r_par.at[0, q], below)
    t_high = Scatter(3, lambda q: s_par.at[1, q], lambda q: r_par.at[1, q], above)
    t_child = Scatter(4, lambda q: s_ch.at[q], lambda q: r_ch.at[q], every)

    def gathered(block):
        return block.reshape(cols * block.shape[1], block.shape[2])

    for q in chunks:
        g_own.start(q)

    rhs_up[...] = update_rhs[...].T
    rhs_par[...] = parent_rhs[...].T
    own_par[...] = jnp.zeros_like(own_par)
    own_piv[...] = jnp.zeros_like(own_piv)
    direct[...] = jnp.zeros_like(direct)
    rows = lax.broadcasted_iota(jnp.int32, (m, m // 2), 0)
    for k in range(2):
        chosen[k] = (rows == targets(row_map, k, me_p, m // 2, me_p * m)).astype(F32).astype(BF)

    for q in chunks:
        with jax.named_scope("s1_pass"):
            g_own.pass_on(q)
    for q in chunks:
        with jax.named_scope("s1_arrive"):
            g_own.arrive(q)
        with jax.named_scope("s1_comp"):
            value = sum(
                dot_rows(gathered(x_pin[child, q, part]), lower_update[:, part * mk : (part + 1) * mk])
                for part in range(2)
            )
            t_up.give(q, value, own_up.at[q])
    for q in chunks:
        g_other.start(q)

    wide = upper_update.shape[2]
    with jax.named_scope("picked"):
        for k in range(2):
            rows = lax.broadcasted_iota(jnp.int32, (2 * m, wide), 0)
            hot = (rows == targets(col_map, k, me_r, wide, me_r * 2 * m)).astype(F32).astype(BF)
            picked[k] = dot_rows(upper_update[k], hot).astype(BF)

    first = lax.rem(me_p, half) * 2

    def shuffle(q, side):
        return pltpu.make_async_remote_copy(
            src_ref=uhalf.at[q, side],
            dst_ref=moved.at[q, child],
            send_sem=sh_send.at[q, side],
            recv_sem=sh_recv.at[q, child],
            device_id=(first + side, me_r),
            device_id_type=MESH,
        )

    for q in chunks:
        own_up[q] += rhs_up[q * wq : (q + 1) * wq]
        with jax.named_scope("s1_add"):
            t_up.add(q, own_up.at[q])
        update = own_up[q].astype(BF)
        for side in range(2):
            uhalf[q, side] = update[:, side * (m // 2) : (side + 1) * (m // 2)]

            @pl.when(first + side != me_p)
            def _():
                shuffle(q, side).start()

            @pl.when(first + side == me_p)
            def _():
                pltpu.make_async_copy(uhalf.at[q, side], moved.at[q, child], sh_recv.at[q, child]).start()

    for q in chunks:
        value = rhs_par[q * wq : (q + 1) * wq]
        for k in range(2):
            with jax.named_scope("moved"):
                pltpu.make_async_copy(moved.at[q, k], moved.at[q, k], sh_recv.at[q, k]).wait()
            value = value + dot_rows(moved[q, k], chosen[k])
        vec[0, q] = value.astype(BF)
        g_low.start(q)

    for q in chunks:
        with jax.named_scope("other_pass"):
            g_other.pass_on(q)

    def pivots():
        for q in chunks:
            g_other.arrive(q)
        parts = []
        for k in range(2):
            sums = []
            for q in chunks:
                sums.append(
                    sum(
                        dot_rows(gathered(x_pin[k, q, part]), lower_pivot[k, :, part * mk : (part + 1) * mk])
                        for part in range(2)
                    ).reshape(cols, wq, mk)
                )
            parts.append(sums)
        for step in range(cols):
            for k in range(2):
                for q in chunks:
                    place = (slice(q * wq, (q + 1) * wq), slice(k * mk, (k + 1) * mk))
                    if step < last:
                        s_piv[(step,) + place] = parts[k][q][step].astype(BF)
                    else:
                        own_piv[place] = parts[k][q][step]
            if step < last:
                t_piv.copy(0, step).start()

    with jax.named_scope("pivots"):
        guard(g_other.active, pivots)

    def multiply(level, gather, scatter, factor, q):
        def action():
            with jax.named_scope("arrive"):
                gather.arrive(q)
            value = sum(
                dot_rows(gathered(x_par[level, q, part]), factor[:, part * m : (part + 1) * m])
                for part in range(2)
            )
            scatter.give(q, value, own_par.at[level, q])

        guard(gather.active, action)

    def combine(level, scatter, following, q):
        scatter.add(q, own_par.at[level, q])
        vec[level + 1, q] = own_par[level, q].astype(BF)
        following.start(q)

    def parent(level, gather, scatter, factor, following, name):
        for q in chunks:
            with jax.named_scope(name + "_pass"):
                gather.pass_on(q)
            if q:
                with jax.named_scope(name + "_add"):
                    combine(level, scatter, following, q - 1)
            with jax.named_scope(name + "_mul"):
                multiply(level, gather, scatter, factor, q)
        with jax.named_scope(name + "_add"):
            combine(level, scatter, following, SPLIT - 1)

    parent(0, g_low, t_low, parent_lower, g_up, "low")

    with jax.named_scope("piv_add"):
        t_piv.add(0, own_piv)
    phalf[...] = own_piv[...].astype(BF)
    g_half.start(0)

    parent(1, g_up, t_high, parent_upper, g_all, "up")

    with jax.named_scope("half_pass"):
        g_half.pass_on(0)

    def known():
        g_half.arrive(0)
        for k in range(2):
            value = sum(
                dot_rows(
                    gathered(x_half[part, :, :, k * mk : (k + 1) * mk]),
                    upper_pivot[k, :, part * mk : (part + 1) * mk],
                )
                for part in range(2)
            )
            direct[:, :, k * mk : (k + 1) * mk] = value.reshape(cols, width, mk)

    with jax.named_scope("known"):
        guard(g_half.active, known)
    parent_out[...] = own_par[1].reshape(width, m).T

    for q in chunks:
        with jax.named_scope("all_pass"):
            g_all.pass_on(q)
        with jax.named_scope("all_arrive"):
            g_all.arrive(q)
        with jax.named_scope("all_comp"):
            for k in range(2):
                lanes = slice(k * mk, (k + 1) * mk)
                value = gathered(direct[:, q * wq : (q + 1) * wq, lanes]) + sum(
                    dot_rows(gathered(x_par[2, q, part]), picked[k, :, part * m : (part + 1) * m])
                    for part in range(2)
                )
                for step in range(last):
                    s_ch[q, step, :, lanes] = value[step * wq : (step + 1) * wq].astype(BF)
                own_ch[q, :, lanes] = value[last * wq :]
            for step in range(last):
                t_child.copy(q, step).start()

    with jax.named_scope("gfinish"):
        for q in chunks:
            for gather in (g_own, g_other, g_low, g_up, g_all):
                gather.finish(q)
            for side in range(2):

                @pl.when(first + side != me_p)
                def _():
                    shuffle(q, side).wait_send()

        g_half.finish(0)
    for q in chunks:
        with jax.named_scope("ch_add"):
            t_child.add(q, own_ch.at[q])
    result = own_ch[...].reshape(width, 2 * mk).T
    for k in range(2):
        child_out[k] = result[k * mk : (k + 1) * mk]
    for q in chunks:
        for scatter in (t_up, t_low, t_high, t_child):
            scatter.finish(q)
    t_piv.finish(0)


def shards(panels, cols, *arguments):
    *arrays, maps = arguments
    m, width = arrays[1].shape
    mk = arrays[0].shape[1]
    wide = arrays[8].shape[2]
    if panels != 2 * cols or mk % 128 or m % 256 or wide % 128 or width % (16 * SPLIT):
        return plain_shards(panels, cols, *arguments)
    wq = width // SPLIT
    maps = maps.reshape(1, -1)
    vm = pltpu.VMEM
    dma = pltpu.SemaphoreType.DMA
    return pl.pallas_call(
        functools.partial(split_kernel, panels, cols),
        out_shape=(
            jax.ShapeDtypeStruct((m, width), F32),
            jax.ShapeDtypeStruct((2, mk, width), F32),
        ),
        in_specs=[pl.BlockSpec(memory_space=pltpu.VMEM)] * 11,
        out_specs=(pl.BlockSpec(memory_space=pltpu.VMEM),) * 2,
        scratch_shapes=[
            vm((2, SPLIT, wq, mk), BF),
            vm((2, SPLIT, 2, cols, wq, mk), BF),
            vm((SPLIT, 2, wq, m // 2), BF),
            vm((SPLIT, 2, wq, m // 2), BF),
            vm((2, m, m // 2), BF),
            vm((3, SPLIT, wq, m), BF),
            vm((3, SPLIT, 2, cols, wq, m), BF),
            vm((width, 2 * mk), BF),
            vm((2, cols, width, 2 * mk), BF),
            vm((2, mk, 2 * m), BF),
            vm((cols, width, 2 * mk), F32),
            vm((SPLIT, cols - 1, wq, m), BF),
            vm((SPLIT, cols - 1, wq, m), BF),
            vm((cols - 1, width, 2 * mk), BF),
            vm((cols - 1, width, 2 * mk), BF),
            vm((2, SPLIT, cols - 1, wq, m), BF),
            vm((2, SPLIT, cols - 1, wq, m), BF),
            vm((SPLIT, cols - 1, wq, 2 * mk), BF),
            vm((SPLIT, cols - 1, wq, 2 * mk), BF),
            vm((SPLIT, wq, m), F32),
            vm((width, 2 * mk), F32),
            vm((2, SPLIT, wq, m), F32),
            vm((SPLIT, wq, 2 * mk), F32),
            vm((width, m), F32),
            vm((width, m), F32),
            dma((6, SPLIT, panels // 2)),
            dma((6, SPLIT, cols, 2)),
            dma((6, SPLIT, cols)),
            dma((5, SPLIT, cols - 1)),
            dma((5, SPLIT, cols - 1)),
            dma((SPLIT, 2)),
            dma((SPLIT, 2)),
        ],
        compiler_params=pltpu.CompilerParams(
            collective_id=0, has_side_effects=True, vmem_limit_bytes=60 * 1024 * 1024
        ),
    )(*arrays, maps, maps)


def solution(mesh):
    panels, cols = mesh.shape["panel"], mesh.shape["rhs"]
    placed = (
        P(None, "panel", "rhs"),
        P("panel", "rhs"),
        P("panel", "rhs"),
        P(None, "panel", "rhs"),
        P("panel", "rhs"),
        P("panel", "rhs"),
        P("panel", "rhs"),
        P(None, "panel", "rhs"),
        P(None, "panel", "rhs"),
        P(),
    )
    return jax.shard_map(
        functools.partial(shards, panels, cols),
        mesh=mesh,
        in_specs=placed,
        out_specs=(P("panel", "rhs"), P(None, "panel", "rhs")),
        check_vma=False,
    )
```

```python
import functools

import jax
import jax.numpy as jnp
from jax import lax
from jax.experimental import pallas as pl
from jax.experimental.pallas import tpu as pltpu
from jax.sharding import PartitionSpec as P

BF = jnp.bfloat16
F32 = jnp.float32
MESH = pl.DeviceIdType.MESH


def dot(left, right):
    return jnp.dot(left, right, preferred_element_type=F32)


def plain_kernel(
    panels,
    cols,
    pivot_rhs,
    update_rhs,
    parent_rhs,
    lower_pivot,
    lower_update,
    parent_lower,
    parent_upper,
    upper_pivot,
    upper_update,
    row_map,
    col_map,
    parent_out,
    child_out,
    pin,
    phalf,
    vec,
    x_pin,
    x_half,
    x_par,
    s_up,
    r_up,
    s_piv,
    r_piv,
    s_par,
    r_par,
    s_ch,
    r_ch,
    uhalf,
    moved,
    picked,
    direct,
    par_sum,
    spread_sum,
    child_sum,
    g_send,
    g_recv,
    f_send,
    rs_send,
    rs_recv,
    sh_send,
    sh_recv,
):
    me_p, me_r = lax.axis_index("panel"), lax.axis_index("rhs")
    total = panels * cols
    me = me_p * cols + me_r
    core = lax.rem(me_p, 2)
    mate = me_p + 1 - 2 * core
    per = panels // cols
    half = panels // 2
    m = parent_rhs.shape[0]
    mk = pivot_rhs.shape[1]
    child = me_p // half

    barrier = pltpu.get_barrier_semaphore()

    @pl.loop(1, total)
    def _(step):
        other = lax.rem(me + step, total)
        pl.semaphore_signal(
            barrier,
            inc=1,
            device_id=(other // cols, lax.rem(other, cols)),
            device_id_type=MESH,
        )

    pin[...] = pivot_rhs[...].astype(BF)
    direct[...] = jnp.zeros_like(direct)
    pl.semaphore_wait(barrier, total - 1)

    group = me_p // per
    last = cols - 1

    def every(source, goal):
        return None

    def below(source, goal):
        return goal >= source

    def above(source, goal):
        return goal <= source

    def guard(condition, action):
        if condition is None:
            action()
        else:
            pl.when(condition)(action)

    def both(first, second):
        return second if first is None else jnp.logical_and(first, second)

    def spot(buffer, depth, column, part, lead):
        rows = pl.ds(pl.multiple_of(part * depth, depth), depth)
        return buffer.at[column, slice(None) if lead is None else pl.ds(lead, 1), rows, :]

    class Gather:
        def __init__(self, stage, block, buffer, depth, keep, lead):
            self.stage, self.block, self.buffer, self.depth = stage, block, buffer, depth
            self.keep, self.lead = keep, lead
            self.active = keep(me_r, group)

        def place(self, column, part, panel):
            return spot(self.buffer, self.depth, column, part, self.lead(panel))

        def piece(self, panel):
            lead = self.lead(panel)
            return self.block if lead is None else self.block.at[pl.ds(lead, 1)]

        def goal(self, step):
            return lax.rem(me_p // 2 + step, half) * 2 + core

        def copy(self, step):
            goal = self.goal(step)
            return pltpu.make_async_remote_copy(
                src_ref=self.piece(goal),
                dst_ref=self.place(me_r, lax.rem(me_p, per), goal),
                send_sem=g_send.at[self.stage, step],
                recv_sem=g_recv.at[self.stage, me_r, lax.rem(me_p, per)],
                device_id=(goal, group),
                device_id_type=MESH,
            )

        def sends(self, action):
            for step in list(range(1, half)) + [0]:
                condition = self.keep(group, self.goal(step) // per)
                if step == 0:
                    condition = both(condition, group != me_r)
                guard(condition, functools.partial(action, step))

        def start(self):
            self.sends(lambda step: self.copy(step).start())

            @pl.when(group == me_r)
            def _():
                part = lax.rem(me_p, per)
                pltpu.make_async_copy(
                    self.piece(me_p),
                    self.place(me_r, part, me_p),
                    g_recv.at[self.stage, me_r, part],
                ).start()

        def landed(self, column, part):
            place = self.place(column, part, me_p)
            pltpu.make_async_copy(place, place, g_recv.at[self.stage, column, part]).wait()

        def forward(self, step, pair):
            column = lax.rem(me_r + 1 + step, cols)
            part = 2 * pair + core
            return pltpu.make_async_remote_copy(
                src_ref=self.place(column, part, me_p),
                dst_ref=self.place(column, part, me_p),
                send_sem=f_send.at[self.stage, step, pair],
                recv_sem=g_recv.at[self.stage, column, part],
                device_id=(mate, me_r),
                device_id_type=MESH,
            )

        def pass_on(self):
            def action():
                for step in [last] + list(range(last)):
                    for pair in range(per // 2):
                        self.landed(lax.rem(me_r + 1 + step, cols), 2 * pair + core)
                        self.forward(step, pair).start()

            guard(self.active, action)

        def arrive(self, step):
            column = lax.rem(me_r + 1 + step, cols)
            for pair in range(per // 2):
                self.landed(column, 2 * pair + 1 - core)
            return column

        def finish(self):
            self.sends(lambda step: self.copy(step).wait_send())

            def action():
                for step in range(cols):
                    for pair in range(per // 2):
                        self.forward(step, pair).wait_send()

            guard(self.active, action)

    class Scatter:
        def __init__(self, stage, source, target, keep):
            self.stage, self.source, self.target, self.keep = stage, source, target, keep
            self.active = keep(me_r, group)

        def copy(self, step):
            return pltpu.make_async_remote_copy(
                src_ref=self.source.at[step],
                dst_ref=self.target.at[step],
                send_sem=rs_send.at[self.stage, step],
                recv_sem=rs_recv.at[self.stage, step],
                device_id=(me_p, lax.rem(me_r + 1 + step, cols)),
                device_id_type=MESH,
            )

        def add(self, total_ref):
            for step in range(last):
                sender = lax.rem(me_r + last - step, cols)

                def action(step=step):
                    self.copy(step).wait_recv()
                    total_ref[...] += self.target[step].astype(F32)

                guard(self.keep(sender, group), action)

        def finish(self):
            def action():
                for step in range(last):
                    self.copy(step).wait_send()

            guard(self.active, action)

    def targets(ref, k, index, size, base):
        if ref.shape[0] == 2:
            return ref[k : k + 1, :]
        start = pl.multiple_of(k * (ref.shape[1] // 2) + index * size, 128)
        return ref[:, pl.ds(start, size)] - base

    def whole(panel):
        return None

    def same(panel):
        return panel // half

    def other(panel):
        return 1 - panel // half

    g_own = Gather(0, pin, x_pin, mk, every, same)
    g_other = Gather(5, pin, x_pin, mk, below, other)
    g_low = Gather(1, vec.at[0], x_par.at[0], m, below, whole)
    g_half = Gather(2, phalf, x_half, mk, above, whole)
    g_up = Gather(3, vec.at[1], x_par.at[1], m, above, whole)
    g_all = Gather(4, vec.at[2], x_par.at[2], m, every, whole)
    t_up = Scatter(0, s_up, r_up, every)
    t_piv = Scatter(1, s_piv, r_piv, below)
    t_low = Scatter(2, s_par.at[0], r_par.at[0], below)
    t_high = Scatter(3, s_par.at[1], r_par.at[1], above)
    t_child = Scatter(4, s_ch, r_ch, every)

    g_own.start()
    g_other.start()

    width = upper_update.shape[2]
    for k in range(2):
        rows = lax.broadcasted_iota(jnp.int32, (per * m, width), 0)
        chosen = (rows == targets(col_map, k, me_r, width, me_r * per * m)).astype(F32).astype(BF)
        picked[k] = lax.dot_general(
            upper_update[k], chosen, (((1,), (1,)), ((), ())), preferred_element_type=F32
        ).astype(BF)
    spread_sum[...] = parent_rhs[...]

    g_own.pass_on()
    for step in range(cols):
        column = g_own.arrive(step)
        value = dot(lower_update[...], x_pin[column, child])
        if step < last:
            s_up[step] = value.astype(BF)
            t_up.copy(step).start()
        else:
            par_sum[...] = update_rhs[...] + value
    g_other.pass_on()
    t_up.add(par_sum)
    update = par_sum[...].astype(BF)
    uhalf[0] = update[: m // 2]
    uhalf[1] = update[m // 2 :]
    first = lax.rem(me_p, half) * 2

    def shuffle(side):
        return pltpu.make_async_remote_copy(
            src_ref=uhalf.at[side],
            dst_ref=moved.at[child],
            send_sem=sh_send.at[side],
            recv_sem=sh_recv.at[child],
            device_id=(first + side, me_r),
            device_id_type=MESH,
        )

    for side in range(2):

        @pl.when(first + side != me_p)
        def _():
            shuffle(side).start()

        @pl.when(first + side == me_p)
        def _():
            pltpu.make_async_copy(uhalf.at[side], moved.at[child], sh_recv.at[child]).start()

    child_sum[...] = jnp.zeros_like(child_sum)

    def pivots():
        for step in range(cols):
            column = g_other.arrive(step)
            for k in range(2):
                value = dot(lower_pivot[k], x_pin[column, k])
                if step < last:
                    s_piv[step, k] = value.astype(BF)
                else:
                    child_sum[k] = value
            if step < last:
                t_piv.copy(step).start()

    guard(g_other.active, pivots)

    rows = lax.broadcasted_iota(jnp.int32, (m, m // 2), 0)
    for k in range(2):
        pltpu.make_async_copy(moved.at[k], moved.at[k], sh_recv.at[k]).wait()
        chosen = (rows == targets(row_map, k, me_p, m // 2, me_p * m)).astype(F32).astype(BF)
        spread_sum[...] += dot(chosen, moved[k])
    vec[0, 0] = spread_sum[...].astype(BF)
    g_low.start()

    t_piv.add(child_sum)
    phalf[...] = child_sum[...].astype(BF)
    g_half.start()

    def parent(level, gather, scatter, factor):
        par_sum[...] = jnp.zeros_like(par_sum)
        gather.pass_on()

        def action():
            for step in range(cols):
                column = gather.arrive(step)
                value = dot(factor[...], x_par[level, column, 0])
                if step < last:
                    s_par[level, step] = value.astype(BF)
                    scatter.copy(step).start()
                else:
                    par_sum[...] = value

        guard(gather.active, action)
        scatter.add(par_sum)
        vec[level + 1, 0] = par_sum[...].astype(BF)

    parent(0, g_low, t_low, parent_lower)
    g_up.start()
    g_half.pass_on()

    def known():
        for step in range(cols):
            column = g_half.arrive(step)
            for k in range(2):
                direct[step, k] = dot(upper_pivot[k], x_half[column, k])

    guard(g_half.active, known)
    parent(1, g_up, t_high, parent_upper)
    g_all.start()
    parent_out[...] = par_sum[...]

    g_all.pass_on()
    for step in range(cols):
        column = g_all.arrive(step)
        for k in range(2):
            value = direct[step, k] + dot(picked[k], x_par[2, column, 0])
            if step < last:
                s_ch[step, k] = value.astype(BF)
            else:
                child_out[k] = value
        if step < last:
            t_child.copy(step).start()
    for gather in (g_own, g_other, g_low, g_half, g_up, g_all):
        gather.finish()
    for side in range(2):

        @pl.when(first + side != me_p)
        def _():
            shuffle(side).wait_send()

    t_child.add(child_out)
    for scatter in (t_up, t_piv, t_low, t_high, t_child):
        scatter.finish()


def plain_shards(panels, cols, *arguments):
    *arrays, maps = arguments
    m, width = arrays[1].shape
    mk = arrays[0].shape[1]
    per = panels // cols
    sides = maps.reshape(2, -1)
    me_p, me_r = lax.axis_index("panel"), lax.axis_index("rhs")
    wide = arrays[8].shape[2]

    def cut(index, size, base):
        if size % 128 == 0:
            return maps.reshape(1, -1)
        return lax.dynamic_slice_in_dim(sides, index * size, size, 1) - base

    row_map = cut(me_p, m // 2, me_p * m)
    col_map = cut(me_r, wide, me_r * per * m)
    vm = pltpu.VMEM
    dma = pltpu.SemaphoreType.DMA
    return pl.pallas_call(
        functools.partial(plain_kernel, panels, cols),
        out_shape=(
            jax.ShapeDtypeStruct((m, width), F32),
            jax.ShapeDtypeStruct((2, mk, width), F32),
        ),
        in_specs=[pl.BlockSpec(memory_space=pltpu.VMEM)] * 11,
        out_specs=(pl.BlockSpec(memory_space=pltpu.VMEM),) * 2,
        scratch_shapes=[
            vm((2, mk, width), BF),
            vm((2, mk, width), BF),
            vm((3, 1, m, width), BF),
            vm((cols, 2, per * mk, width), BF),
            vm((cols, 2, per * mk, width), BF),
            vm((3, cols, 1, per * m, width), BF),
            vm((cols - 1, m, width), BF),
            vm((cols - 1, m, width), BF),
            vm((cols - 1, 2, mk, width), BF),
            vm((cols - 1, 2, mk, width), BF),
            vm((2, cols - 1, m, width), BF),
            vm((2, cols - 1, m, width), BF),
            vm((cols - 1, 2, mk, width), BF),
            vm((cols - 1, 2, mk, width), BF),
            vm((2, m // 2, width), BF),
            vm((2, m // 2, width), BF),
            vm((2, mk, per * m), BF),
            vm((cols, 2, mk, width), F32),
            vm((m, width), F32),
            vm((m, width), F32),
            vm((2, mk, width), F32),
            dma((6, panels // 2)),
            dma((6, cols, per)),
            dma((6, cols, per // 2)),
            dma((5, cols - 1)),
            dma((5, cols - 1)),
            dma((2,)),
            dma((2,)),
        ],
        compiler_params=pltpu.CompilerParams(
            collective_id=0, has_side_effects=True, vmem_limit_bytes=60 * 1024 * 1024
        ),
    )(*arrays, row_map, col_map)


SPLIT = 2


def dot_rows(left, right):
    return lax.dot_general(left, right, (((1,), (1,)), ((), ())), preferred_element_type=F32)


def split_kernel(
    panels,
    cols,
    pivot_rhs_at,
    update_rhs_at,
    parent_rhs_at,
    lower_pivot_at,
    lower_update_at,
    parent_lower_at,
    parent_upper_at,
    upper_pivot_at,
    upper_update_at,
    maps,
    parent_out,
    child_out,
    pin,
    x_pin,
    uhalf,
    moved,
    chosen,
    vec,
    x_par,
    phalf,
    x_half,
    picked,
    direct,
    s_up,
    r_up,
    s_piv,
    r_piv,
    s_par,
    r_par,
    s_ch,
    r_ch,
    own_up,
    own_piv,
    own_par,
    own_ch,
    rhs_up,
    rhs_par,
    g_send,
    g_recv,
    f_send,
    rs_send,
    rs_recv,
    sh_send,
    sh_recv,
    pivot_rhs,
    update_rhs,
    parent_rhs,
    lower_pivot,
    lower_update,
    parent_lower,
    parent_upper,
    upper_pivot,
    upper_update,
    in_sem,
):
    me_p, me_r = lax.axis_index("panel"), lax.axis_index("rhs")
    total = panels * cols
    me = me_p * cols + me_r
    core = lax.rem(me_p, 2)
    mate = me_p + 1 - 2 * core
    half = panels // 2
    m, width = parent_rhs.shape
    mk = pivot_rhs.shape[1]
    wq = width // SPLIT
    child = me_p // half
    group = me_p // 2
    last = cols - 1
    chunks = range(SPLIT)

    arrays = (
        (pivot_rhs_at, pivot_rhs),
        (lower_update_at, lower_update),
        (update_rhs_at, update_rhs),
        (parent_rhs_at, parent_rhs),
        (upper_update_at, upper_update),
        (lower_pivot_at, lower_pivot),
        (parent_lower_at, parent_lower),
        (parent_upper_at, parent_upper),
        (upper_pivot_at, upper_pivot),
    )

    def fetch(held):
        index = [pair[1] is held for pair in arrays].index(True)
        return pltpu.make_async_copy(*arrays[index], in_sem.at[index])

    barrier = pltpu.get_barrier_semaphore()

    @pl.loop(1, total)
    def _(step):
        other = lax.rem(me + step, total)
        pl.semaphore_signal(
            barrier,
            inc=1,
            device_id=(other // cols, lax.rem(other, cols)),
            device_id_type=MESH,
        )

    for _, held in arrays:
        fetch(held).start()
    fetch(pivot_rhs).wait()
    for k in range(2):
        turned = pivot_rhs[k].T.astype(BF)
        for q in chunks:
            pin[k, q] = turned[q * wq : (q + 1) * wq]
    with jax.named_scope("barrier"):
        pl.semaphore_wait(barrier, total - 1)

    def every(source, goal):
        return None

    def below(source, goal):
        return goal >= source

    def above(source, goal):
        return goal <= source

    def guard(condition, action):
        if condition is None:
            action()
        else:
            pl.when(condition)(action)

    def both(first, second):
        return second if first is None else jnp.logical_and(first, second)

    sent_place = lax.rem(me_r - group - 1 + 2 * cols, cols)

    class Gather:
        def __init__(self, stage, piece, place, keep):
            self.stage, self.piece, self.place, self.keep = stage, piece, place, keep
            self.active = keep(me_r, group)

        def goal(self, step):
            return lax.rem(group + step, half) * 2 + core

        def copy(self, q, step):
            goal = self.goal(step)
            return pltpu.make_async_remote_copy(
                src_ref=self.piece(q, goal),
                dst_ref=self.place(q, core, sent_place, goal),
                send_sem=g_send.at[self.stage, q, step],
                recv_sem=g_recv.at[self.stage, q, sent_place, core],
                device_id=(goal, group),
                device_id_type=MESH,
            )

        def sends(self, action):
            for step in list(range(1, half)) + [0]:
                condition = self.keep(group, self.goal(step) // 2)
                if step == 0:
                    condition = both(condition, group != me_r)
                guard(condition, functools.partial(action, step))

        def start(self, q):
            self.sends(lambda step: self.copy(q, step).start())

            @pl.when(group == me_r)
            def _():
                pltpu.make_async_copy(
                    self.piece(q, me_p),
                    self.place(q, core, last, me_p),
                    g_recv.at[self.stage, q, last, core],
                ).start()

        def landed(self, q, spot, part):
            place = self.place(q, part, spot, me_p)
            pltpu.make_async_copy(place, place, g_recv.at[self.stage, q, spot, part]).wait()

        def forward(self, q, spot):
            return pltpu.make_async_remote_copy(
                src_ref=self.place(q, core, spot, me_p),
                dst_ref=self.place(q, core, spot, me_p),
                send_sem=f_send.at[self.stage, q, spot],
                recv_sem=g_recv.at[self.stage, q, spot, core],
                device_id=(mate, me_r),
                device_id_type=MESH,
            )

        def pass_on(self, q):
            def action():
                for spot in [last] + list(range(last)):
                    self.landed(q, spot, core)
                    self.forward(q, spot).start()

            guard(self.active, action)

        def arrive(self, q):
            for spot in range(cols):
                self.landed(q, spot, 1 - core)

        def finish(self, q):
            self.sends(lambda step: self.copy(q, step).wait_send())

            def action():
                for spot in range(cols):
                    self.forward(q, spot).wait_send()

            guard(self.active, action)

    class Scatter:
        def __init__(self, stage, source, target, keep):
            self.stage, self.source, self.target, self.keep = stage, source, target, keep
            self.active = keep(me_r, group)

        def copy(self, q, step):
            return pltpu.make_async_remote_copy(
                src_ref=self.source(q).at[step],
                dst_ref=self.target(q).at[step],
                send_sem=rs_send.at[self.stage, q, step],
                recv_sem=rs_recv.at[self.stage, q, step],
                device_id=(me_p, lax.rem(me_r + 1 + step, cols)),
                device_id_type=MESH,
            )

        def give(self, q, value, own):
            rows = value.shape[0] // cols
            for step in range(last):
                self.source(q)[step] = value[step * rows : (step + 1) * rows].astype(BF)
                self.copy(q, step).start()
            own[...] = value[last * rows :]

        def add(self, q, total_ref):
            for step in range(last):
                sender = lax.rem(me_r + last - step, cols)

                def action(step=step):
                    self.copy(q, step).wait_recv()
                    total_ref[...] += self.target(q)[step].astype(F32)

                guard(self.keep(sender, group), action)

        def finish(self, q):
            def action():
                for step in range(last):
                    self.copy(q, step).wait_send()

            guard(self.active, action)

    def targets(ref, k, index, size, base):
        if ref.shape[0] == 2:
            return ref[k : k + 1, :]
        start = pl.multiple_of(k * (ref.shape[1] // 2) + index * size, 128)
        return ref[:, pl.ds(start, size)] - base

    def same(panel):
        return panel // half

    def other(panel):
        return 1 - panel // half

    def pins(side):
        return (
            lambda q, goal: pin.at[side(goal), q],
            lambda q, part, spot, goal: x_pin.at[side(goal), q, part, spot],
        )

    def level_parts(level):
        return (
            lambda q, goal: vec.at[level, q],
            lambda q, part, spot, goal: x_par.at[level, q, part, spot],
        )

    g_own = Gather(0, *pins(same), every)
    g_other = Gather(5, *pins(other), below)
    g_low = Gather(1, *level_parts(0), below)
    g_up = Gather(3, *level_parts(1), above)
    g_all = Gather(4, *level_parts(2), every)
    g_half = Gather(
        2, lambda q, goal: phalf, lambda q, part, spot, goal: x_half.at[part, spot], above
    )
    t_up = Scatter(0, lambda q: s_up.at[q], lambda q: r_up.at[q], every)
    t_piv = Scatter(1, lambda q: s_piv, lambda q: r_piv, below)
    t_low = Scatter(2, lambda q: s_par.at[0, q], lambda q: r_par.at[0, q], below)
    t_high = Scatter(3, lambda q: s_par.at[1, q], lambda q: r_par.at[1, q], above)
    t_child = Scatter(4, lambda q: s_ch.at[q], lambda q: r_ch.at[q], every)

    def gathered(block):
        return block.reshape(cols * block.shape[1], block.shape[2])

    for q in chunks:
        g_own.start(q)

    fetch(update_rhs).wait()
    fetch(parent_rhs).wait()
    fetch(lower_update).wait()
    rhs_up[...] = update_rhs[...].T
    rhs_par[...] = parent_rhs[...].T
    own_par[...] = jnp.zeros_like(own_par)
    own_piv[...] = jnp.zeros_like(own_piv)
    direct[...] = jnp.zeros_like(direct)
    rows = lax.broadcasted_iota(jnp.int32, (m, m // 2), 0)
    for k in range(2):
        chosen[k] = (rows == targets(maps, k, me_p, m // 2, me_p * m)).astype(F32).astype(BF)

    for q in chunks:
        with jax.named_scope("s1_pass"):
            g_own.pass_on(q)
    for q in chunks:
        with jax.named_scope("s1_arrive"):
            g_own.arrive(q)
        with jax.named_scope("s1_comp"):
            value = sum(
                dot_rows(gathered(x_pin[child, q, part]), lower_update[:, part * mk : (part + 1) * mk])
                for part in range(2)
            )
            t_up.give(q, value, own_up.at[q])
    for q in chunks:
        g_other.start(q)

    wide = upper_update.shape[2]
    fetch(upper_update).wait()
    with jax.named_scope("picked"):
        for k in range(2):
            rows = lax.broadcasted_iota(jnp.int32, (2 * m, wide), 0)
            hot = (rows == targets(maps, k, me_r, wide, me_r * 2 * m)).astype(F32).astype(BF)
            picked[k] = dot_rows(upper_update[k], hot).astype(BF)

    first = lax.rem(me_p, half) * 2

    def shuffle(q, side):
        return pltpu.make_async_remote_copy(
            src_ref=uhalf.at[q, side],
            dst_ref=moved.at[q, child],
            send_sem=sh_send.at[q, side],
            recv_sem=sh_recv.at[q, child],
            device_id=(first + side, me_r),
            device_id_type=MESH,
        )

    for q in chunks:
        own_up[q] += rhs_up[q * wq : (q + 1) * wq]
        with jax.named_scope("s1_add"):
            t_up.add(q, own_up.at[q])
        update = own_up[q].astype(BF)
        for side in range(2):
            uhalf[q, side] = update[:, side * (m // 2) : (side + 1) * (m // 2)]

            @pl.when(first + side != me_p)
            def _():
                shuffle(q, side).start()

            @pl.when(first + side == me_p)
            def _():
                pltpu.make_async_copy(uhalf.at[q, side], moved.at[q, child], sh_recv.at[q, child]).start()

    for q in chunks:
        value = rhs_par[q * wq : (q + 1) * wq]
        for k in range(2):
            with jax.named_scope("moved"):
                pltpu.make_async_copy(moved.at[q, k], moved.at[q, k], sh_recv.at[q, k]).wait()
            value = value + dot_rows(moved[q, k], chosen[k])
        vec[0, q] = value.astype(BF)
        g_low.start(q)

    for q in chunks:
        with jax.named_scope("other_pass"):
            g_other.pass_on(q)

    def pivots():
        for q in chunks:
            g_other.arrive(q)
        parts = []
        for k in range(2):
            sums = []
            for q in chunks:
                sums.append(
                    sum(
                        dot_rows(gathered(x_pin[k, q, part]), lower_pivot[k, :, part * mk : (part + 1) * mk])
                        for part in range(2)
                    ).reshape(cols, wq, mk)
                )
            parts.append(sums)
        for step in range(cols):
            for k in range(2):
                for q in chunks:
                    place = (slice(q * wq, (q + 1) * wq), slice(k * mk, (k + 1) * mk))
                    if step < last:
                        s_piv[(step,) + place] = parts[k][q][step].astype(BF)
                    else:
                        own_piv[place] = parts[k][q][step]
            if step < last:
                t_piv.copy(0, step).start()

    fetch(lower_pivot).wait()
    with jax.named_scope("pivots"):
        guard(g_other.active, pivots)

    def multiply(level, gather, scatter, factor, q):
        def action():
            with jax.named_scope("arrive"):
                gather.arrive(q)
            value = sum(
                dot_rows(gathered(x_par[level, q, part]), factor[:, part * m : (part + 1) * m])
                for part in range(2)
            )
            scatter.give(q, value, own_par.at[level, q])

        guard(gather.active, action)

    def combine(level, scatter, following, q):
        scatter.add(q, own_par.at[level, q])
        vec[level + 1, q] = own_par[level, q].astype(BF)
        following.start(q)

    def parent(level, gather, scatter, factor, following, name):
        for q in chunks:
            with jax.named_scope(name + "_pass"):
                gather.pass_on(q)
            if q:
                with jax.named_scope(name + "_add"):
                    combine(level, scatter, following, q - 1)
            with jax.named_scope(name + "_mul"):
                multiply(level, gather, scatter, factor, q)
        with jax.named_scope(name + "_add"):
            combine(level, scatter, following, SPLIT - 1)

    fetch(parent_lower).wait()
    parent(0, g_low, t_low, parent_lower, g_up, "low")

    with jax.named_scope("piv_add"):
        t_piv.add(0, own_piv)
    phalf[...] = own_piv[...].astype(BF)
    g_half.start(0)

    fetch(parent_upper).wait()
    parent(1, g_up, t_high, parent_upper, g_all, "up")

    fetch(upper_pivot).wait()
    with jax.named_scope("half_pass"):
        g_half.pass_on(0)

    def known():
        g_half.arrive(0)
        for k in range(2):
            value = sum(
                dot_rows(
                    gathered(x_half[part, :, :, k * mk : (k + 1) * mk]),
                    upper_pivot[k, :, part * mk : (part + 1) * mk],
                )
                for part in range(2)
            )
            direct[:, :, k * mk : (k + 1) * mk] = value.reshape(cols, width, mk)

    with jax.named_scope("known"):
        guard(g_half.active, known)
    parent_out[...] = own_par[1].reshape(width, m).T

    for q in chunks:
        with jax.named_scope("all_pass"):
            g_all.pass_on(q)
        with jax.named_scope("all_arrive"):
            g_all.arrive(q)
        with jax.named_scope("all_comp"):
            for k in range(2):
                lanes = slice(k * mk, (k + 1) * mk)
                value = gathered(direct[:, q * wq : (q + 1) * wq, lanes]) + sum(
                    dot_rows(gathered(x_par[2, q, part]), picked[k, :, part * m : (part + 1) * m])
                    for part in range(2)
                )
                for step in range(last):
                    s_ch[q, step, :, lanes] = value[step * wq : (step + 1) * wq].astype(BF)
                own_ch[q, :, lanes] = value[last * wq :]
            for step in range(last):
                t_child.copy(q, step).start()

    with jax.named_scope("gfinish"):
        for q in chunks:
            for gather in (g_own, g_other, g_low, g_up, g_all):
                gather.finish(q)
            for side in range(2):

                @pl.when(first + side != me_p)
                def _():
                    shuffle(q, side).wait_send()

        g_half.finish(0)
    for q in chunks:
        with jax.named_scope("ch_add"):
            t_child.add(q, own_ch.at[q])
    result = own_ch[...].reshape(width, 2 * mk).T
    for k in range(2):
        child_out[k] = result[k * mk : (k + 1) * mk]
    for q in chunks:
        for scatter in (t_up, t_low, t_high, t_child):
            scatter.finish(q)
    t_piv.finish(0)


def shards(panels, cols, *arguments):
    *arrays, maps = arguments
    m, width = arrays[1].shape
    mk = arrays[0].shape[1]
    wide = arrays[8].shape[2]
    if panels != 2 * cols or mk % 128 or m % 256 or wide % 128 or width % (16 * SPLIT):
        return plain_shards(panels, cols, *arguments)
    wq = width // SPLIT
    maps = maps.reshape(1, -1)
    vm = pltpu.VMEM
    dma = pltpu.SemaphoreType.DMA
    return pl.pallas_call(
        functools.partial(split_kernel, panels, cols),
        out_shape=(
            pltpu.VMEM((m, width), F32),
            pltpu.VMEM((2, mk, width), F32),
        ),
        in_specs=[pl.BlockSpec(memory_space=pl.ANY)] * 9 + [pl.BlockSpec(memory_space=pltpu.VMEM)],
        out_specs=(pl.BlockSpec(memory_space=pltpu.VMEM),) * 2,
        scratch_shapes=[
            vm((2, SPLIT, wq, mk), BF),
            vm((2, SPLIT, 2, cols, wq, mk), BF),
            vm((SPLIT, 2, wq, m // 2), BF),
            vm((SPLIT, 2, wq, m // 2), BF),
            vm((2, m, m // 2), BF),
            vm((3, SPLIT, wq, m), BF),
            vm((3, SPLIT, 2, cols, wq, m), BF),
            vm((width, 2 * mk), BF),
            vm((2, cols, width, 2 * mk), BF),
            vm((2, mk, 2 * m), BF),
            vm((cols, width, 2 * mk), F32),
            vm((SPLIT, cols - 1, wq, m), BF),
            vm((SPLIT, cols - 1, wq, m), BF),
            vm((cols - 1, width, 2 * mk), BF),
            vm((cols - 1, width, 2 * mk), BF),
            vm((2, SPLIT, cols - 1, wq, m), BF),
            vm((2, SPLIT, cols - 1, wq, m), BF),
            vm((SPLIT, cols - 1, wq, 2 * mk), BF),
            vm((SPLIT, cols - 1, wq, 2 * mk), BF),
            vm((SPLIT, wq, m), F32),
            vm((width, 2 * mk), F32),
            vm((2, SPLIT, wq, m), F32),
            vm((SPLIT, wq, 2 * mk), F32),
            vm((width, m), F32),
            vm((width, m), F32),
            dma((6, SPLIT, panels // 2)),
            dma((6, SPLIT, cols, 2)),
            dma((6, SPLIT, cols)),
            dma((5, SPLIT, cols - 1)),
            dma((5, SPLIT, cols - 1)),
            dma((SPLIT, 2)),
            dma((SPLIT, 2)),
            *[vm(array.shape, array.dtype) for array in arrays],
            dma((9,)),
        ],
        compiler_params=pltpu.CompilerParams(
            collective_id=0, has_side_effects=True, vmem_limit_bytes=60 * 1024 * 1024
        ),
    )(*arrays, maps)


def solution(mesh):
    panels, cols = mesh.shape["panel"], mesh.shape["rhs"]
    placed = (
        P(None, "panel", "rhs"),
        P("panel", "rhs"),
        P("panel", "rhs"),
        P(None, "panel", "rhs"),
        P("panel", "rhs"),
        P("panel", "rhs"),
        P("panel", "rhs"),
        P(None, "panel", "rhs"),
        P(None, "panel", "rhs"),
        P(),
    )
    return jax.shard_map(
        functools.partial(shards, panels, cols),
        mesh=mesh,
        in_specs=placed,
        out_specs=(P("panel", "rhs"), P(None, "panel", "rhs")),
        check_vma=False,
    )
```

```python
import functools

import jax
import jax.numpy as jnp
from jax import lax
from jax.experimental import pallas as pl
from jax.experimental.pallas import tpu as pltpu
from jax.sharding import PartitionSpec as P

BF = jnp.bfloat16
F32 = jnp.float32
MESH = pl.DeviceIdType.MESH


def dot(left, right):
    return jnp.dot(left, right, preferred_element_type=F32)


def plain_kernel(
    panels,
    cols,
    pivot_rhs,
    update_rhs,
    parent_rhs,
    lower_pivot,
    lower_update,
    parent_lower,
    parent_upper,
    upper_pivot,
    upper_update,
    row_map,
    col_map,
    parent_out,
    child_out,
    pin,
    phalf,
    vec,
    x_pin,
    x_half,
    x_par,
    s_up,
    r_up,
    s_piv,
    r_piv,
    s_par,
    r_par,
    s_ch,
    r_ch,
    uhalf,
    moved,
    picked,
    direct,
    par_sum,
    spread_sum,
    child_sum,
    g_send,
    g_recv,
    f_send,
    rs_send,
    rs_recv,
    sh_send,
    sh_recv,
):
    me_p, me_r = lax.axis_index("panel"), lax.axis_index("rhs")
    total = panels * cols
    me = me_p * cols + me_r
    core = lax.rem(me_p, 2)
    mate = me_p + 1 - 2 * core
    per = panels // cols
    half = panels // 2
    m = parent_rhs.shape[0]
    mk = pivot_rhs.shape[1]
    child = me_p // half

    barrier = pltpu.get_barrier_semaphore()

    @pl.loop(1, total)
    def _(step):
        other = lax.rem(me + step, total)
        pl.semaphore_signal(
            barrier,
            inc=1,
            device_id=(other // cols, lax.rem(other, cols)),
            device_id_type=MESH,
        )

    pin[...] = pivot_rhs[...].astype(BF)
    direct[...] = jnp.zeros_like(direct)
    pl.semaphore_wait(barrier, total - 1)

    group = me_p // per
    last = cols - 1

    def every(source, goal):
        return None

    def below(source, goal):
        return goal >= source

    def above(source, goal):
        return goal <= source

    def guard(condition, action):
        if condition is None:
            action()
        else:
            pl.when(condition)(action)

    def both(first, second):
        return second if first is None else jnp.logical_and(first, second)

    def spot(buffer, depth, column, part, lead):
        rows = pl.ds(pl.multiple_of(part * depth, depth), depth)
        return buffer.at[column, slice(None) if lead is None else pl.ds(lead, 1), rows, :]

    class Gather:
        def __init__(self, stage, block, buffer, depth, keep, lead):
            self.stage, self.block, self.buffer, self.depth = stage, block, buffer, depth
            self.keep, self.lead = keep, lead
            self.active = keep(me_r, group)

        def place(self, column, part, panel):
            return spot(self.buffer, self.depth, column, part, self.lead(panel))

        def piece(self, panel):
            lead = self.lead(panel)
            return self.block if lead is None else self.block.at[pl.ds(lead, 1)]

        def goal(self, step):
            return lax.rem(me_p // 2 + step, half) * 2 + core

        def copy(self, step):
            goal = self.goal(step)
            return pltpu.make_async_remote_copy(
                src_ref=self.piece(goal),
                dst_ref=self.place(me_r, lax.rem(me_p, per), goal),
                send_sem=g_send.at[self.stage, step],
                recv_sem=g_recv.at[self.stage, me_r, lax.rem(me_p, per)],
                device_id=(goal, group),
                device_id_type=MESH,
            )

        def sends(self, action):
            for step in list(range(1, half)) + [0]:
                condition = self.keep(group, self.goal(step) // per)
                if step == 0:
                    condition = both(condition, group != me_r)
                guard(condition, functools.partial(action, step))

        def start(self):
            self.sends(lambda step: self.copy(step).start())

            @pl.when(group == me_r)
            def _():
                part = lax.rem(me_p, per)
                pltpu.make_async_copy(
                    self.piece(me_p),
                    self.place(me_r, part, me_p),
                    g_recv.at[self.stage, me_r, part],
                ).start()

        def landed(self, column, part):
            place = self.place(column, part, me_p)
            pltpu.make_async_copy(place, place, g_recv.at[self.stage, column, part]).wait()

        def forward(self, step, pair):
            column = lax.rem(me_r + 1 + step, cols)
            part = 2 * pair + core
            return pltpu.make_async_remote_copy(
                src_ref=self.place(column, part, me_p),
                dst_ref=self.place(column, part, me_p),
                send_sem=f_send.at[self.stage, step, pair],
                recv_sem=g_recv.at[self.stage, column, part],
                device_id=(mate, me_r),
                device_id_type=MESH,
            )

        def pass_on(self):
            def action():
                for step in [last] + list(range(last)):
                    for pair in range(per // 2):
                        self.landed(lax.rem(me_r + 1 + step, cols), 2 * pair + core)
                        self.forward(step, pair).start()

            guard(self.active, action)

        def arrive(self, step):
            column = lax.rem(me_r + 1 + step, cols)
            for pair in range(per // 2):
                self.landed(column, 2 * pair + 1 - core)
            return column

        def finish(self):
            self.sends(lambda step: self.copy(step).wait_send())

            def action():
                for step in range(cols):
                    for pair in range(per // 2):
                        self.forward(step, pair).wait_send()

            guard(self.active, action)

    class Scatter:
        def __init__(self, stage, source, target, keep):
            self.stage, self.source, self.target, self.keep = stage, source, target, keep
            self.active = keep(me_r, group)

        def copy(self, step):
            return pltpu.make_async_remote_copy(
                src_ref=self.source.at[step],
                dst_ref=self.target.at[step],
                send_sem=rs_send.at[self.stage, step],
                recv_sem=rs_recv.at[self.stage, step],
                device_id=(me_p, lax.rem(me_r + 1 + step, cols)),
                device_id_type=MESH,
            )

        def add(self, total_ref):
            for step in range(last):
                sender = lax.rem(me_r + last - step, cols)

                def action(step=step):
                    self.copy(step).wait_recv()
                    total_ref[...] += self.target[step].astype(F32)

                guard(self.keep(sender, group), action)

        def finish(self):
            def action():
                for step in range(last):
                    self.copy(step).wait_send()

            guard(self.active, action)

    def targets(ref, k, index, size, base):
        if ref.shape[0] == 2:
            return ref[k : k + 1, :]
        start = pl.multiple_of(k * (ref.shape[1] // 2) + index * size, 128)
        return ref[:, pl.ds(start, size)] - base

    def whole(panel):
        return None

    def same(panel):
        return panel // half

    def other(panel):
        return 1 - panel // half

    g_own = Gather(0, pin, x_pin, mk, every, same)
    g_other = Gather(5, pin, x_pin, mk, below, other)
    g_low = Gather(1, vec.at[0], x_par.at[0], m, below, whole)
    g_half = Gather(2, phalf, x_half, mk, above, whole)
    g_up = Gather(3, vec.at[1], x_par.at[1], m, above, whole)
    g_all = Gather(4, vec.at[2], x_par.at[2], m, every, whole)
    t_up = Scatter(0, s_up, r_up, every)
    t_piv = Scatter(1, s_piv, r_piv, below)
    t_low = Scatter(2, s_par.at[0], r_par.at[0], below)
    t_high = Scatter(3, s_par.at[1], r_par.at[1], above)
    t_child = Scatter(4, s_ch, r_ch, every)

    g_own.start()
    g_other.start()

    width = upper_update.shape[2]
    for k in range(2):
        rows = lax.broadcasted_iota(jnp.int32, (per * m, width), 0)
        chosen = (rows == targets(col_map, k, me_r, width, me_r * per * m)).astype(F32).astype(BF)
        picked[k] = lax.dot_general(
            upper_update[k], chosen, (((1,), (1,)), ((), ())), preferred_element_type=F32
        ).astype(BF)
    spread_sum[...] = parent_rhs[...]

    g_own.pass_on()
    for step in range(cols):
        column = g_own.arrive(step)
        value = dot(lower_update[...], x_pin[column, child])
        if step < last:
            s_up[step] = value.astype(BF)
            t_up.copy(step).start()
        else:
            par_sum[...] = update_rhs[...] + value
    g_other.pass_on()
    t_up.add(par_sum)
    update = par_sum[...].astype(BF)
    uhalf[0] = update[: m // 2]
    uhalf[1] = update[m // 2 :]
    first = lax.rem(me_p, half) * 2

    def shuffle(side):
        return pltpu.make_async_remote_copy(
            src_ref=uhalf.at[side],
            dst_ref=moved.at[child],
            send_sem=sh_send.at[side],
            recv_sem=sh_recv.at[child],
            device_id=(first + side, me_r),
            device_id_type=MESH,
        )

    for side in range(2):

        @pl.when(first + side != me_p)
        def _():
            shuffle(side).start()

        @pl.when(first + side == me_p)
        def _():
            pltpu.make_async_copy(uhalf.at[side], moved.at[child], sh_recv.at[child]).start()

    child_sum[...] = jnp.zeros_like(child_sum)

    def pivots():
        for step in range(cols):
            column = g_other.arrive(step)
            for k in range(2):
                value = dot(lower_pivot[k], x_pin[column, k])
                if step < last:
                    s_piv[step, k] = value.astype(BF)
                else:
                    child_sum[k] = value
            if step < last:
                t_piv.copy(step).start()

    guard(g_other.active, pivots)

    rows = lax.broadcasted_iota(jnp.int32, (m, m // 2), 0)
    for k in range(2):
        pltpu.make_async_copy(moved.at[k], moved.at[k], sh_recv.at[k]).wait()
        chosen = (rows == targets(row_map, k, me_p, m // 2, me_p * m)).astype(F32).astype(BF)
        spread_sum[...] += dot(chosen, moved[k])
    vec[0, 0] = spread_sum[...].astype(BF)
    g_low.start()

    t_piv.add(child_sum)
    phalf[...] = child_sum[...].astype(BF)
    g_half.start()

    def parent(level, gather, scatter, factor):
        par_sum[...] = jnp.zeros_like(par_sum)
        gather.pass_on()

        def action():
            for step in range(cols):
                column = gather.arrive(step)
                value = dot(factor[...], x_par[level, column, 0])
                if step < last:
                    s_par[level, step] = value.astype(BF)
                    scatter.copy(step).start()
                else:
                    par_sum[...] = value

        guard(gather.active, action)
        scatter.add(par_sum)
        vec[level + 1, 0] = par_sum[...].astype(BF)

    parent(0, g_low, t_low, parent_lower)
    g_up.start()
    g_half.pass_on()

    def known():
        for step in range(cols):
            column = g_half.arrive(step)
            for k in range(2):
                direct[step, k] = dot(upper_pivot[k], x_half[column, k])

    guard(g_half.active, known)
    parent(1, g_up, t_high, parent_upper)
    g_all.start()
    parent_out[...] = par_sum[...]

    g_all.pass_on()
    for step in range(cols):
        column = g_all.arrive(step)
        for k in range(2):
            value = direct[step, k] + dot(picked[k], x_par[2, column, 0])
            if step < last:
                s_ch[step, k] = value.astype(BF)
            else:
                child_out[k] = value
        if step < last:
            t_child.copy(step).start()
    for gather in (g_own, g_other, g_low, g_half, g_up, g_all):
        gather.finish()
    for side in range(2):

        @pl.when(first + side != me_p)
        def _():
            shuffle(side).wait_send()

    t_child.add(child_out)
    for scatter in (t_up, t_piv, t_low, t_high, t_child):
        scatter.finish()


def plain_shards(panels, cols, *arguments):
    *arrays, maps = arguments
    m, width = arrays[1].shape
    mk = arrays[0].shape[1]
    per = panels // cols
    sides = maps.reshape(2, -1)
    me_p, me_r = lax.axis_index("panel"), lax.axis_index("rhs")
    wide = arrays[8].shape[2]

    def cut(index, size, base):
        if size % 128 == 0:
            return maps.reshape(1, -1)
        return lax.dynamic_slice_in_dim(sides, index * size, size, 1) - base

    row_map = cut(me_p, m // 2, me_p * m)
    col_map = cut(me_r, wide, me_r * per * m)
    vm = pltpu.VMEM
    dma = pltpu.SemaphoreType.DMA
    return pl.pallas_call(
        functools.partial(plain_kernel, panels, cols),
        out_shape=(
            jax.ShapeDtypeStruct((m, width), F32),
            jax.ShapeDtypeStruct((2, mk, width), F32),
        ),
        in_specs=[pl.BlockSpec(memory_space=pltpu.VMEM)] * 11,
        out_specs=(pl.BlockSpec(memory_space=pltpu.VMEM),) * 2,
        scratch_shapes=[
            vm((2, mk, width), BF),
            vm((2, mk, width), BF),
            vm((3, 1, m, width), BF),
            vm((cols, 2, per * mk, width), BF),
            vm((cols, 2, per * mk, width), BF),
            vm((3, cols, 1, per * m, width), BF),
            vm((cols - 1, m, width), BF),
            vm((cols - 1, m, width), BF),
            vm((cols - 1, 2, mk, width), BF),
            vm((cols - 1, 2, mk, width), BF),
            vm((2, cols - 1, m, width), BF),
            vm((2, cols - 1, m, width), BF),
            vm((cols - 1, 2, mk, width), BF),
            vm((cols - 1, 2, mk, width), BF),
            vm((2, m // 2, width), BF),
            vm((2, m // 2, width), BF),
            vm((2, mk, per * m), BF),
            vm((cols, 2, mk, width), F32),
            vm((m, width), F32),
            vm((m, width), F32),
            vm((2, mk, width), F32),
            dma((6, panels // 2)),
            dma((6, cols, per)),
            dma((6, cols, per // 2)),
            dma((5, cols - 1)),
            dma((5, cols - 1)),
            dma((2,)),
            dma((2,)),
        ],
        compiler_params=pltpu.CompilerParams(
            collective_id=0, has_side_effects=True, vmem_limit_bytes=60 * 1024 * 1024
        ),
    )(*arrays, row_map, col_map)


SPLIT = 2
LAG = 1
FAR = (4,)


def dot_rows(left, right):
    return lax.dot_general(left, right, (((1,), (1,)), ((), ())), preferred_element_type=F32)


def split_kernel(
    panels,
    cols,
    pivot_rhs_at,
    update_rhs_at,
    parent_rhs_at,
    lower_pivot_at,
    lower_update_at,
    parent_lower_at,
    parent_upper_at,
    upper_pivot_at,
    upper_update_at,
    maps,
    parent_out,
    child_out,
    pin,
    x_pin,
    uhalf,
    moved,
    chosen,
    vec,
    x_par,
    phalf,
    x_half,
    picked,
    direct,
    s_up,
    r_up,
    s_piv,
    r_piv,
    s_par,
    r_par,
    s_ch,
    r_ch,
    own_up,
    own_piv,
    own_par,
    own_ch,
    rhs_up,
    rhs_par,
    g_send,
    g_recv,
    f_send,
    rs_send,
    rs_recv,
    sh_send,
    sh_recv,
    pivot_rhs,
    update_rhs,
    parent_rhs,
    lower_pivot,
    lower_update,
    parent_lower,
    parent_upper,
    upper_pivot,
    upper_update,
    in_sem,
):
    me_p, me_r = lax.axis_index("panel"), lax.axis_index("rhs")
    total = panels * cols
    me = me_p * cols + me_r
    core = lax.rem(me_p, 2)
    mate = me_p + 1 - 2 * core
    half = panels // 2
    m, width = parent_rhs.shape
    mk = pivot_rhs.shape[1]
    wq = width // SPLIT
    child = me_p // half
    group = me_p // 2
    last = cols - 1
    chunks = range(SPLIT)

    arrays = (
        (pivot_rhs_at, pivot_rhs),
        (lower_update_at, lower_update),
        (update_rhs_at, update_rhs),
        (parent_rhs_at, parent_rhs),
        (upper_update_at, upper_update),
        (lower_pivot_at, lower_pivot),
        (parent_lower_at, parent_lower),
        (parent_upper_at, parent_upper),
        (upper_pivot_at, upper_pivot),
    )

    def fetch(held):
        index = [pair[1] is held for pair in arrays].index(True)
        return pltpu.make_async_copy(*arrays[index], in_sem.at[index])

    barrier = pltpu.get_barrier_semaphore()

    @pl.loop(1, total)
    def _(step):
        other = lax.rem(me + step, total)
        pl.semaphore_signal(
            barrier,
            inc=1,
            device_id=(other // cols, lax.rem(other, cols)),
            device_id_type=MESH,
        )

    for _, held in arrays:
        fetch(held).start()
    fetch(pivot_rhs).wait()
    for k in range(2):
        turned = pivot_rhs[k].T.astype(BF)
        for q in chunks:
            pin[k, q] = turned[q * wq : (q + 1) * wq]
    with jax.named_scope("barrier"):
        pl.semaphore_wait(barrier, total - 1)

    def every(source, goal):
        return None

    def below(source, goal):
        return goal >= source

    def above(source, goal):
        return goal <= source

    def guard(condition, action):
        if condition is None:
            action()
        else:
            pl.when(condition)(action)

    def both(first, second):
        return second if first is None else jnp.logical_and(first, second)

    sent_place = lax.rem(me_r - group - 1 + 2 * cols, cols)

    class Gather:
        def __init__(self, stage, piece, place, keep):
            self.stage, self.piece, self.place, self.keep = stage, piece, place, keep
            self.active = keep(me_r, group)

        def goal(self, step):
            if self.stage in FAR:
                return jnp.where(group < half // 2, half - 1 - step, step) * 2 + core
            return lax.rem(group + 1 + step, half) * 2 + core

        def copy(self, q, step):
            goal = self.goal(step)
            return pltpu.make_async_remote_copy(
                src_ref=self.piece(q, goal),
                dst_ref=self.place(q, core, sent_place, goal),
                send_sem=g_send.at[self.stage, q, step],
                recv_sem=g_recv.at[self.stage, q, sent_place, core],
                device_id=(goal, group),
                device_id_type=MESH,
            )

        def sends(self, action):
            for step in range(half):
                goal = self.goal(step) // 2
                elsewhere = jnp.logical_or(goal != group, group != me_r)
                guard(both(self.keep(group, goal), elsewhere), functools.partial(action, step))

        def start(self, q):
            self.sends(lambda step: self.copy(q, step).start())

            @pl.when(group == me_r)
            def _():
                pltpu.make_async_copy(
                    self.piece(q, me_p),
                    self.place(q, core, last, me_p),
                    g_recv.at[self.stage, q, last, core],
                ).start()

        def landed(self, q, spot, part):
            place = self.place(q, part, spot, me_p)
            pltpu.make_async_copy(place, place, g_recv.at[self.stage, q, spot, part]).wait()

        def forward(self, q, spot):
            return pltpu.make_async_remote_copy(
                src_ref=self.place(q, core, spot, me_p),
                dst_ref=self.place(q, core, spot, me_p),
                send_sem=f_send.at[self.stage, q, spot],
                recv_sem=g_recv.at[self.stage, q, spot, core],
                device_id=(mate, me_r),
                device_id_type=MESH,
            )

        def pass_on(self, q):
            def action():
                for spot in [last] + list(range(last)):
                    self.landed(q, spot, core)
                    self.forward(q, spot).start()

            guard(self.active, action)

        def arrive(self, q):
            for spot in range(cols):
                self.landed(q, spot, 1 - core)

        def finish(self, q):
            self.sends(lambda step: self.copy(q, step).wait_send())

            def action():
                for spot in range(cols):
                    self.forward(q, spot).wait_send()

            guard(self.active, action)

    class Scatter:
        def __init__(self, stage, source, target, keep):
            self.stage, self.source, self.target, self.keep = stage, source, target, keep
            self.active = keep(me_r, group)

        def copy(self, q, step):
            return pltpu.make_async_remote_copy(
                src_ref=self.source(q).at[step],
                dst_ref=self.target(q).at[step],
                send_sem=rs_send.at[self.stage, q, step],
                recv_sem=rs_recv.at[self.stage, q, step],
                device_id=(me_p, lax.rem(me_r + 1 + step, cols)),
                device_id_type=MESH,
            )

        def give(self, q, value, own):
            rows = value.shape[0] // cols
            for step in range(last):
                self.source(q)[step] = value[step * rows : (step + 1) * rows].astype(BF)
                self.copy(q, step).start()
            own[...] = value[last * rows :]

        def add(self, q, total_ref):
            for step in range(last):
                sender = lax.rem(me_r + last - step, cols)

                def action(step=step):
                    self.copy(q, step).wait_recv()
                    total_ref[...] += self.target(q)[step].astype(F32)

                guard(self.keep(sender, group), action)

        def finish(self, q):
            def action():
                for step in range(last):
                    self.copy(q, step).wait_send()

            guard(self.active, action)

    def targets(ref, k, index, size, base):
        if ref.shape[0] == 2:
            return ref[k : k + 1, :]
        start = pl.multiple_of(k * (ref.shape[1] // 2) + index * size, 128)
        return ref[:, pl.ds(start, size)] - base

    def same(panel):
        return panel // half

    def other(panel):
        return 1 - panel // half

    def pins(side):
        return (
            lambda q, goal: pin.at[side(goal), q],
            lambda q, part, spot, goal: x_pin.at[side(goal), q, part, spot],
        )

    def level_parts(level):
        return (
            lambda q, goal: vec.at[level, q],
            lambda q, part, spot, goal: x_par.at[level, q, part, spot],
        )

    g_own = Gather(0, *pins(same), every)
    g_other = Gather(5, *pins(other), below)
    g_low = Gather(1, *level_parts(0), below)
    g_up = Gather(3, *level_parts(1), above)
    g_all = Gather(4, *level_parts(2), every)
    g_half = Gather(
        2, lambda q, goal: phalf, lambda q, part, spot, goal: x_half.at[part, spot], above
    )
    t_up = Scatter(0, lambda q: s_up.at[q], lambda q: r_up.at[q], every)
    t_piv = Scatter(1, lambda q: s_piv, lambda q: r_piv, below)
    t_low = Scatter(2, lambda q: s_par.at[0, q], lambda q: r_par.at[0, q], below)
    t_high = Scatter(3, lambda q: s_par.at[1, q], lambda q: r_par.at[1, q], above)
    t_child = Scatter(4, lambda q: s_ch.at[q], lambda q: r_ch.at[q], every)

    def gathered(block):
        return block.reshape(cols * block.shape[1], block.shape[2])

    for q in chunks:
        g_own.start(q)
    for q in chunks:
        g_other.start(q)

    fetch(update_rhs).wait()
    fetch(parent_rhs).wait()
    fetch(lower_update).wait()
    rhs_up[...] = update_rhs[...].T
    rhs_par[...] = parent_rhs[...].T
    own_par[...] = jnp.zeros_like(own_par)
    own_piv[...] = jnp.zeros_like(own_piv)
    direct[...] = jnp.zeros_like(direct)
    rows = lax.broadcasted_iota(jnp.int32, (m, m // 2), 0)
    for k in range(2):
        chosen[k] = (rows == targets(maps, k, me_p, m // 2, me_p * m)).astype(F32).astype(BF)

    def pivots():
        for q in chunks:
            g_other.arrive(q)
        parts = []
        for k in range(2):
            sums = []
            for q in chunks:
                sums.append(
                    sum(
                        dot_rows(gathered(x_pin[k, q, part]), lower_pivot[k, :, part * mk : (part + 1) * mk])
                        for part in range(2)
                    ).reshape(cols, wq, mk)
                )
            parts.append(sums)
        for step in range(cols):
            for k in range(2):
                for q in chunks:
                    place = (slice(q * wq, (q + 1) * wq), slice(k * mk, (k + 1) * mk))
                    if step < last:
                        s_piv[(step,) + place] = parts[k][q][step].astype(BF)
                    else:
                        own_piv[place] = parts[k][q][step]
            if step < last:
                t_piv.copy(0, step).start()

    for q in chunks:
        with jax.named_scope("s1_pass"):
            g_own.pass_on(q)
    for q in chunks:
        with jax.named_scope("s1_arrive"):
            g_own.arrive(q)
        with jax.named_scope("s1_comp"):
            value = sum(
                dot_rows(gathered(x_pin[child, q, part]), lower_update[:, part * mk : (part + 1) * mk])
                for part in range(2)
            )
            t_up.give(q, value, own_up.at[q])
    for q in chunks:
        with jax.named_scope("other_pass"):
            g_other.pass_on(q)

    fetch(lower_pivot).wait()
    with jax.named_scope("pivots"):
        guard(g_other.active, pivots)


    wide = upper_update.shape[2]
    fetch(upper_update).wait()
    with jax.named_scope("picked"):
        for k in range(2):
            rows = lax.broadcasted_iota(jnp.int32, (2 * m, wide), 0)
            hot = (rows == targets(maps, k, me_r, wide, me_r * 2 * m)).astype(F32).astype(BF)
            picked[k] = dot_rows(upper_update[k], hot).astype(BF)

    first = lax.rem(me_p, half) * 2

    def shuffle(q, side):
        return pltpu.make_async_remote_copy(
            src_ref=uhalf.at[q, side],
            dst_ref=moved.at[q, child],
            send_sem=sh_send.at[q, side],
            recv_sem=sh_recv.at[q, child],
            device_id=(first + side, me_r),
            device_id_type=MESH,
        )

    def reduce(q):
        own_up[q] += rhs_up[q * wq : (q + 1) * wq]
        with jax.named_scope("s1_add"):
            t_up.add(q, own_up.at[q])
        update = own_up[q].astype(BF)
        for side in range(2):
            uhalf[q, side] = update[:, side * (m // 2) : (side + 1) * (m // 2)]

            @pl.when(first + side != me_p)
            def _():
                shuffle(q, side).start()

            @pl.when(first + side == me_p)
            def _():
                pltpu.make_async_copy(uhalf.at[q, side], moved.at[q, child], sh_recv.at[q, child]).start()

    def assemble(q):
        value = rhs_par[q * wq : (q + 1) * wq]
        for k in range(2):
            with jax.named_scope("moved"):
                pltpu.make_async_copy(moved.at[q, k], moved.at[q, k], sh_recv.at[q, k]).wait()
            value = value + dot_rows(moved[q, k], chosen[k])
        vec[0, q] = value.astype(BF)
        g_low.start(q)

    for q in chunks:
        reduce(q)
        if q >= 1:
            assemble(q - 1)
    assemble(SPLIT - 1)

    def multiply(level, gather, scatter, factor, q):
        def action():
            with jax.named_scope("arrive"):
                gather.arrive(q)
            value = sum(
                dot_rows(gathered(x_par[level, q, part]), factor[:, part * m : (part + 1) * m])
                for part in range(2)
            )
            scatter.give(q, value, own_par.at[level, q])

        guard(gather.active, action)

    def combine(level, scatter, following, q):
        scatter.add(q, own_par.at[level, q])
        vec[level + 1, q] = own_par[level, q].astype(BF)
        following.start(q)

    def parent(level, gather, scatter, factor, following, name, extra, between):
        def settle(q):
            with jax.named_scope(name + "_add"):
                combine(level, scatter, following, q)

        for q in chunks:
            with jax.named_scope(name + "_pass"):
                gather.pass_on(q)
            with jax.named_scope(name + "_mul"):
                multiply(level, gather, scatter, factor, q)
            if q == SPLIT - 1:
                extra()
            if q == LAG - 1:
                between()
            if q >= LAG - 1:
                settle(q - LAG + 1)
        for q in range(SPLIT - LAG + 1, SPLIT):
            settle(q)

    def nothing():
        return None

    def start_other():
        for q in chunks:
            g_other.start(q)

    def start_half():
        with jax.named_scope("piv_add"):
            t_piv.add(0, own_piv)
        phalf[...] = own_piv[...].astype(BF)
        g_half.start(0)

    fetch(parent_lower).wait()
    parent(0, g_low, t_low, parent_lower, g_up, "low", nothing, nothing)

    start_half()

    fetch(parent_upper).wait()
    parent(1, g_up, t_high, parent_upper, g_all, "up", nothing, nothing)

    fetch(upper_pivot).wait()
    with jax.named_scope("half_pass"):
        g_half.pass_on(0)

    def known():
        g_half.arrive(0)
        for k in range(2):
            value = sum(
                dot_rows(
                    gathered(x_half[part, :, :, k * mk : (k + 1) * mk]),
                    upper_pivot[k, :, part * mk : (part + 1) * mk],
                )
                for part in range(2)
            )
            direct[:, :, k * mk : (k + 1) * mk] = value.reshape(cols, width, mk)

    with jax.named_scope("known"):
        guard(g_half.active, known)

    parent_out[...] = own_par[1].reshape(width, m).T

    for q in chunks:
        with jax.named_scope("all_pass"):
            g_all.pass_on(q)
        with jax.named_scope("all_arrive"):
            g_all.arrive(q)
        with jax.named_scope("all_comp"):
            for k in range(2):
                lanes = slice(k * mk, (k + 1) * mk)
                value = gathered(direct[:, q * wq : (q + 1) * wq, lanes]) + sum(
                    dot_rows(gathered(x_par[2, q, part]), picked[k, :, part * m : (part + 1) * m])
                    for part in range(2)
                )
                for step in range(last):
                    s_ch[q, step, :, lanes] = value[step * wq : (step + 1) * wq].astype(BF)
                own_ch[q, :, lanes] = value[last * wq :]
            for step in range(last):
                t_child.copy(q, step).start()

    with jax.named_scope("gfinish"):
        for q in chunks:
            for gather in (g_own, g_other, g_low, g_up, g_all):
                gather.finish(q)
            for side in range(2):

                @pl.when(first + side != me_p)
                def _():
                    shuffle(q, side).wait_send()

        g_half.finish(0)
    for q in chunks:
        with jax.named_scope("ch_add"):
            t_child.add(q, own_ch.at[q])
    result = own_ch[...].reshape(width, 2 * mk).T
    for k in range(2):
        child_out[k] = result[k * mk : (k + 1) * mk]
    for q in chunks:
        for scatter in (t_up, t_low, t_high, t_child):
            scatter.finish(q)
    t_piv.finish(0)


def shards(panels, cols, *arguments):
    *arrays, maps = arguments
    m, width = arrays[1].shape
    mk = arrays[0].shape[1]
    wide = arrays[8].shape[2]
    if panels != 2 * cols or mk % 128 or m % 256 or wide % 128 or width % (16 * SPLIT):
        return plain_shards(panels, cols, *arguments)
    wq = width // SPLIT
    maps = maps.reshape(1, -1)
    vm = pltpu.VMEM
    dma = pltpu.SemaphoreType.DMA
    return pl.pallas_call(
        functools.partial(split_kernel, panels, cols),
        out_shape=(
            pltpu.VMEM((m, width), F32),
            pltpu.VMEM((2, mk, width), F32),
        ),
        in_specs=[pl.BlockSpec(memory_space=pl.ANY)] * 9 + [pl.BlockSpec(memory_space=pltpu.VMEM)],
        out_specs=(pl.BlockSpec(memory_space=pltpu.VMEM),) * 2,
        scratch_shapes=[
            vm((2, SPLIT, wq, mk), BF),
            vm((2, SPLIT, 2, cols, wq, mk), BF),
            vm((SPLIT, 2, wq, m // 2), BF),
            vm((SPLIT, 2, wq, m // 2), BF),
            vm((2, m, m // 2), BF),
            vm((3, SPLIT, wq, m), BF),
            vm((3, SPLIT, 2, cols, wq, m), BF),
            vm((width, 2 * mk), BF),
            vm((2, cols, width, 2 * mk), BF),
            vm((2, mk, 2 * m), BF),
            vm((cols, width, 2 * mk), F32),
            vm((SPLIT, cols - 1, wq, m), BF),
            vm((SPLIT, cols - 1, wq, m), BF),
            vm((cols - 1, width, 2 * mk), BF),
            vm((cols - 1, width, 2 * mk), BF),
            vm((2, SPLIT, cols - 1, wq, m), BF),
            vm((2, SPLIT, cols - 1, wq, m), BF),
            vm((SPLIT, cols - 1, wq, 2 * mk), BF),
            vm((SPLIT, cols - 1, wq, 2 * mk), BF),
            vm((SPLIT, wq, m), F32),
            vm((width, 2 * mk), F32),
            vm((2, SPLIT, wq, m), F32),
            vm((SPLIT, wq, 2 * mk), F32),
            vm((width, m), F32),
            vm((width, m), F32),
            dma((6, SPLIT, panels // 2)),
            dma((6, SPLIT, cols, 2)),
            dma((6, SPLIT, cols)),
            dma((5, SPLIT, cols - 1)),
            dma((5, SPLIT, cols - 1)),
            dma((SPLIT, 2)),
            dma((SPLIT, 2)),
            *[vm(array.shape, array.dtype) for array in arrays],
            dma((9,)),
        ],
        compiler_params=pltpu.CompilerParams(
            collective_id=0, has_side_effects=True, vmem_limit_bytes=60 * 1024 * 1024
        ),
    )(*arrays, maps)


def solution(mesh):
    panels, cols = mesh.shape["panel"], mesh.shape["rhs"]
    placed = (
        P(None, "panel", "rhs"),
        P("panel", "rhs"),
        P("panel", "rhs"),
        P(None, "panel", "rhs"),
        P("panel", "rhs"),
        P("panel", "rhs"),
        P("panel", "rhs"),
        P(None, "panel", "rhs"),
        P(None, "panel", "rhs"),
        P(),
    )
    return jax.shard_map(
        functools.partial(shards, panels, cols),
        mesh=mesh,
        in_specs=placed,
        out_specs=(P("panel", "rhs"), P(None, "panel", "rhs")),
        check_vma=False,
    )
```

```python
import functools

import jax
import jax.numpy as jnp
from jax import lax
from jax.experimental import pallas as pl
from jax.experimental.pallas import tpu as pltpu
from jax.sharding import PartitionSpec as P

BF = jnp.bfloat16
F32 = jnp.float32
MESH = pl.DeviceIdType.MESH


def dot(left, right):
    return jnp.dot(left, right, preferred_element_type=F32)


def plain_kernel(
    panels,
    cols,
    pivot_rhs,
    update_rhs,
    parent_rhs,
    lower_pivot,
    lower_update,
    parent_lower,
    parent_upper,
    upper_pivot,
    upper_update,
    row_map,
    col_map,
    parent_out,
    child_out,
    pin,
    phalf,
    vec,
    x_pin,
    x_half,
    x_par,
    s_up,
    r_up,
    s_piv,
    r_piv,
    s_par,
    r_par,
    s_ch,
    r_ch,
    uhalf,
    moved,
    picked,
    direct,
    par_sum,
    spread_sum,
    child_sum,
    g_send,
    g_recv,
    f_send,
    rs_send,
    rs_recv,
    sh_send,
    sh_recv,
):
    me_p, me_r = lax.axis_index("panel"), lax.axis_index("rhs")
    total = panels * cols
    me = me_p * cols + me_r
    core = lax.rem(me_p, 2)
    mate = me_p + 1 - 2 * core
    per = panels // cols
    half = panels // 2
    m = parent_rhs.shape[0]
    mk = pivot_rhs.shape[1]
    child = me_p // half

    barrier = pltpu.get_barrier_semaphore()

    @pl.loop(1, total)
    def _(step):
        other = lax.rem(me + step, total)
        pl.semaphore_signal(
            barrier,
            inc=1,
            device_id=(other // cols, lax.rem(other, cols)),
            device_id_type=MESH,
        )

    pin[...] = pivot_rhs[...].astype(BF)
    direct[...] = jnp.zeros_like(direct)
    pl.semaphore_wait(barrier, total - 1)

    group = me_p // per
    last = cols - 1

    def every(source, goal):
        return None

    def below(source, goal):
        return goal >= source

    def above(source, goal):
        return goal <= source

    def guard(condition, action):
        if condition is None:
            action()
        else:
            pl.when(condition)(action)

    def both(first, second):
        return second if first is None else jnp.logical_and(first, second)

    def spot(buffer, depth, column, part, lead):
        rows = pl.ds(pl.multiple_of(part * depth, depth), depth)
        return buffer.at[column, slice(None) if lead is None else pl.ds(lead, 1), rows, :]

    class Gather:
        def __init__(self, stage, block, buffer, depth, keep, lead):
            self.stage, self.block, self.buffer, self.depth = stage, block, buffer, depth
            self.keep, self.lead = keep, lead
            self.active = keep(me_r, group)

        def place(self, column, part, panel):
            return spot(self.buffer, self.depth, column, part, self.lead(panel))

        def piece(self, panel):
            lead = self.lead(panel)
            return self.block if lead is None else self.block.at[pl.ds(lead, 1)]

        def goal(self, step):
            return lax.rem(me_p // 2 + step, half) * 2 + core

        def copy(self, step):
            goal = self.goal(step)
            return pltpu.make_async_remote_copy(
                src_ref=self.piece(goal),
                dst_ref=self.place(me_r, lax.rem(me_p, per), goal),
                send_sem=g_send.at[self.stage, step],
                recv_sem=g_recv.at[self.stage, me_r, lax.rem(me_p, per)],
                device_id=(goal, group),
                device_id_type=MESH,
            )

        def sends(self, action):
            for step in list(range(1, half)) + [0]:
                condition = self.keep(group, self.goal(step) // per)
                if step == 0:
                    condition = both(condition, group != me_r)
                guard(condition, functools.partial(action, step))

        def start(self):
            self.sends(lambda step: self.copy(step).start())

            @pl.when(group == me_r)
            def _():
                part = lax.rem(me_p, per)
                pltpu.make_async_copy(
                    self.piece(me_p),
                    self.place(me_r, part, me_p),
                    g_recv.at[self.stage, me_r, part],
                ).start()

        def landed(self, column, part):
            place = self.place(column, part, me_p)
            pltpu.make_async_copy(place, place, g_recv.at[self.stage, column, part]).wait()

        def forward(self, step, pair):
            column = lax.rem(me_r + 1 + step, cols)
            part = 2 * pair + core
            return pltpu.make_async_remote_copy(
                src_ref=self.place(column, part, me_p),
                dst_ref=self.place(column, part, me_p),
                send_sem=f_send.at[self.stage, step, pair],
                recv_sem=g_recv.at[self.stage, column, part],
                device_id=(mate, me_r),
                device_id_type=MESH,
            )

        def pass_on(self):
            def action():
                for step in [last] + list(range(last)):
                    for pair in range(per // 2):
                        self.landed(lax.rem(me_r + 1 + step, cols), 2 * pair + core)
                        self.forward(step, pair).start()

            guard(self.active, action)

        def arrive(self, step):
            column = lax.rem(me_r + 1 + step, cols)
            for pair in range(per // 2):
                self.landed(column, 2 * pair + 1 - core)
            return column

        def finish(self):
            self.sends(lambda step: self.copy(step).wait_send())

            def action():
                for step in range(cols):
                    for pair in range(per // 2):
                        self.forward(step, pair).wait_send()

            guard(self.active, action)

    class Scatter:
        def __init__(self, stage, source, target, keep):
            self.stage, self.source, self.target, self.keep = stage, source, target, keep
            self.active = keep(me_r, group)

        def copy(self, step):
            return pltpu.make_async_remote_copy(
                src_ref=self.source.at[step],
                dst_ref=self.target.at[step],
                send_sem=rs_send.at[self.stage, step],
                recv_sem=rs_recv.at[self.stage, step],
                device_id=(me_p, lax.rem(me_r + 1 + step, cols)),
                device_id_type=MESH,
            )

        def add(self, total_ref):
            for step in range(last):
                sender = lax.rem(me_r + last - step, cols)

                def action(step=step):
                    self.copy(step).wait_recv()
                    total_ref[...] += self.target[step].astype(F32)

                guard(self.keep(sender, group), action)

        def finish(self):
            def action():
                for step in range(last):
                    self.copy(step).wait_send()

            guard(self.active, action)

    def targets(ref, k, index, size, base):
        if ref.shape[0] == 2:
            return ref[k : k + 1, :]
        start = pl.multiple_of(k * (ref.shape[1] // 2) + index * size, 128)
        return ref[:, pl.ds(start, size)] - base

    def whole(panel):
        return None

    def same(panel):
        return panel // half

    def other(panel):
        return 1 - panel // half

    g_own = Gather(0, pin, x_pin, mk, every, same)
    g_other = Gather(5, pin, x_pin, mk, below, other)
    g_low = Gather(1, vec.at[0], x_par.at[0], m, below, whole)
    g_half = Gather(2, phalf, x_half, mk, above, whole)
    g_up = Gather(3, vec.at[1], x_par.at[1], m, above, whole)
    g_all = Gather(4, vec.at[2], x_par.at[2], m, every, whole)
    t_up = Scatter(0, s_up, r_up, every)
    t_piv = Scatter(1, s_piv, r_piv, below)
    t_low = Scatter(2, s_par.at[0], r_par.at[0], below)
    t_high = Scatter(3, s_par.at[1], r_par.at[1], above)
    t_child = Scatter(4, s_ch, r_ch, every)

    g_own.start()
    g_other.start()

    width = upper_update.shape[2]
    for k in range(2):
        rows = lax.broadcasted_iota(jnp.int32, (per * m, width), 0)
        chosen = (rows == targets(col_map, k, me_r, width, me_r * per * m)).astype(F32).astype(BF)
        picked[k] = lax.dot_general(
            upper_update[k], chosen, (((1,), (1,)), ((), ())), preferred_element_type=F32
        ).astype(BF)
    spread_sum[...] = parent_rhs[...]

    g_own.pass_on()
    for step in range(cols):
        column = g_own.arrive(step)
        value = dot(lower_update[...], x_pin[column, child])
        if step < last:
            s_up[step] = value.astype(BF)
            t_up.copy(step).start()
        else:
            par_sum[...] = update_rhs[...] + value
    g_other.pass_on()
    t_up.add(par_sum)
    update = par_sum[...].astype(BF)
    uhalf[0] = update[: m // 2]
    uhalf[1] = update[m // 2 :]
    first = lax.rem(me_p, half) * 2

    def shuffle(side):
        return pltpu.make_async_remote_copy(
            src_ref=uhalf.at[side],
            dst_ref=moved.at[child],
            send_sem=sh_send.at[side],
            recv_sem=sh_recv.at[child],
            device_id=(first + side, me_r),
            device_id_type=MESH,
        )

    for side in range(2):

        @pl.when(first + side != me_p)
        def _():
            shuffle(side).start()

        @pl.when(first + side == me_p)
        def _():
            pltpu.make_async_copy(uhalf.at[side], moved.at[child], sh_recv.at[child]).start()

    child_sum[...] = jnp.zeros_like(child_sum)

    def pivots():
        for step in range(cols):
            column = g_other.arrive(step)
            for k in range(2):
                value = dot(lower_pivot[k], x_pin[column, k])
                if step < last:
                    s_piv[step, k] = value.astype(BF)
                else:
                    child_sum[k] = value
            if step < last:
                t_piv.copy(step).start()

    guard(g_other.active, pivots)

    rows = lax.broadcasted_iota(jnp.int32, (m, m // 2), 0)
    for k in range(2):
        pltpu.make_async_copy(moved.at[k], moved.at[k], sh_recv.at[k]).wait()
        chosen = (rows == targets(row_map, k, me_p, m // 2, me_p * m)).astype(F32).astype(BF)
        spread_sum[...] += dot(chosen, moved[k])
    vec[0, 0] = spread_sum[...].astype(BF)
    g_low.start()

    t_piv.add(child_sum)
    phalf[...] = child_sum[...].astype(BF)
    g_half.start()

    def parent(level, gather, scatter, factor):
        par_sum[...] = jnp.zeros_like(par_sum)
        gather.pass_on()

        def action():
            for step in range(cols):
                column = gather.arrive(step)
                value = dot(factor[...], x_par[level, column, 0])
                if step < last:
                    s_par[level, step] = value.astype(BF)
                    scatter.copy(step).start()
                else:
                    par_sum[...] = value

        guard(gather.active, action)
        scatter.add(par_sum)
        vec[level + 1, 0] = par_sum[...].astype(BF)

    parent(0, g_low, t_low, parent_lower)
    g_up.start()
    g_half.pass_on()

    def known():
        for step in range(cols):
            column = g_half.arrive(step)
            for k in range(2):
                direct[step, k] = dot(upper_pivot[k], x_half[column, k])

    guard(g_half.active, known)
    parent(1, g_up, t_high, parent_upper)
    g_all.start()
    parent_out[...] = par_sum[...]

    g_all.pass_on()
    for step in range(cols):
        column = g_all.arrive(step)
        for k in range(2):
            value = direct[step, k] + dot(picked[k], x_par[2, column, 0])
            if step < last:
                s_ch[step, k] = value.astype(BF)
            else:
                child_out[k] = value
        if step < last:
            t_child.copy(step).start()
    for gather in (g_own, g_other, g_low, g_half, g_up, g_all):
        gather.finish()
    for side in range(2):

        @pl.when(first + side != me_p)
        def _():
            shuffle(side).wait_send()

    t_child.add(child_out)
    for scatter in (t_up, t_piv, t_low, t_high, t_child):
        scatter.finish()


def plain_shards(panels, cols, *arguments):
    *arrays, maps = arguments
    m, width = arrays[1].shape
    mk = arrays[0].shape[1]
    per = panels // cols
    sides = maps.reshape(2, -1)
    me_p, me_r = lax.axis_index("panel"), lax.axis_index("rhs")
    wide = arrays[8].shape[2]

    def cut(index, size, base):
        if size % 128 == 0:
            return maps.reshape(1, -1)
        return lax.dynamic_slice_in_dim(sides, index * size, size, 1) - base

    row_map = cut(me_p, m // 2, me_p * m)
    col_map = cut(me_r, wide, me_r * per * m)
    vm = pltpu.VMEM
    dma = pltpu.SemaphoreType.DMA
    return pl.pallas_call(
        functools.partial(plain_kernel, panels, cols),
        out_shape=(
            jax.ShapeDtypeStruct((m, width), F32),
            jax.ShapeDtypeStruct((2, mk, width), F32),
        ),
        in_specs=[pl.BlockSpec(memory_space=pltpu.VMEM)] * 11,
        out_specs=(pl.BlockSpec(memory_space=pltpu.VMEM),) * 2,
        scratch_shapes=[
            vm((2, mk, width), BF),
            vm((2, mk, width), BF),
            vm((3, 1, m, width), BF),
            vm((cols, 2, per * mk, width), BF),
            vm((cols, 2, per * mk, width), BF),
            vm((3, cols, 1, per * m, width), BF),
            vm((cols - 1, m, width), BF),
            vm((cols - 1, m, width), BF),
            vm((cols - 1, 2, mk, width), BF),
            vm((cols - 1, 2, mk, width), BF),
            vm((2, cols - 1, m, width), BF),
            vm((2, cols - 1, m, width), BF),
            vm((cols - 1, 2, mk, width), BF),
            vm((cols - 1, 2, mk, width), BF),
            vm((2, m // 2, width), BF),
            vm((2, m // 2, width), BF),
            vm((2, mk, per * m), BF),
            vm((cols, 2, mk, width), F32),
            vm((m, width), F32),
            vm((m, width), F32),
            vm((2, mk, width), F32),
            dma((6, panels // 2)),
            dma((6, cols, per)),
            dma((6, cols, per // 2)),
            dma((5, cols - 1)),
            dma((5, cols - 1)),
            dma((2,)),
            dma((2,)),
        ],
        compiler_params=pltpu.CompilerParams(
            collective_id=0, has_side_effects=True, vmem_limit_bytes=60 * 1024 * 1024
        ),
    )(*arrays, row_map, col_map)


SPLIT = 2
FAR = (4,)


def dot_rows(left, right):
    return lax.dot_general(left, right, (((1,), (1,)), ((), ())), preferred_element_type=F32)


def split_kernel(
    panels,
    cols,
    pivot_at,
    update_at,
    parent_at,
    lower_pivot_at,
    lower_update_at,
    parent_lower_at,
    parent_upper_at,
    upper_pivot_at,
    upper_update_at,
    maps,
    parent_out,
    child_out,
    pivot_rhs,
    update_rhs,
    parent_rhs,
    lower_pivot,
    lower_update,
    parent_lower,
    parent_upper,
    upper_pivot,
    upper_update,
    pin,
    x_pin,
    uhalf,
    moved,
    chosen,
    vec,
    x_par,
    phalf,
    x_half,
    picked,
    direct,
    s_par,
    r_par,
    s_piv,
    r_piv,
    own_par,
    own_piv,
    sum_par,
    sum_piv,
    g_send,
    g_recv,
    rs_send,
    rs_recv,
    sh_send,
    sh_recv,
    in_sem,
    mate_send,
    mate_recv,
):
    me_p, me_r = lax.axis_index("panel"), lax.axis_index("rhs")
    total = panels * cols
    me = me_p * cols + me_r
    core = lax.rem(me_p, 2)
    mate = me_p + 1 - 2 * core
    half = panels // 2
    m, width = parent_rhs.shape
    mk = pivot_rhs.shape[1]
    wq = width // SPLIT
    wj = wq // 2
    child = me_p // half
    group = me_p // 2
    last = cols - 1
    chunks = range(SPLIT)

    factors = (
        (lower_update_at, lower_update),
        (lower_pivot_at, lower_pivot),
        (upper_update_at, upper_update),
        (parent_lower_at, parent_lower),
        (parent_upper_at, parent_upper),
        (upper_pivot_at, upper_pivot),
    )
    vectors = ((pivot_at, pivot_rhs), (update_at, update_rhs), (parent_at, parent_rhs))

    def own_rows(index):
        return pltpu.make_async_copy(factors[index][0], factors[index][1].at[core], in_sem.at[index])

    def mate_rows(index):
        return pltpu.make_async_remote_copy(
            src_ref=factors[index][0],
            dst_ref=factors[index][1].at[core],
            send_sem=mate_send.at[index],
            recv_sem=mate_recv.at[index],
            device_id=(mate, me_r),
            device_id_type=MESH,
        )

    def ready(held):
        index = [pair[1] is held for pair in factors].index(True)
        own_rows(index).wait()
        place = held.at[1 - core]
        pltpu.make_async_copy(place, place, mate_recv.at[index]).wait()

    def fetch(index):
        return pltpu.make_async_copy(*vectors[index], in_sem.at[6 + index])

    fetch(0).start()
    barrier = pltpu.get_barrier_semaphore()

    @pl.loop(1, total)
    def _(step):
        other = lax.rem(me + step, total)
        pl.semaphore_signal(
            barrier,
            inc=1,
            device_id=(other // cols, lax.rem(other, cols)),
            device_id_type=MESH,
        )

    own_rows(0).start()
    fetch(1).start()
    fetch(2).start()
    for index in range(1, 6):
        own_rows(index).start()
    fetch(0).wait()
    for k in range(2):
        pin[k] = pivot_rhs[k].T.astype(BF).reshape(SPLIT, 2, wj, mk)
    with jax.named_scope("barrier"):
        pl.semaphore_wait(barrier, total - 1)

    def every(source, goal):
        return None

    def below(source, goal):
        return goal >= source

    def above(source, goal):
        return goal <= source

    def guard(condition, action):
        if condition is None:
            action()
        else:
            pl.when(condition)(action)

    def both(first, second):
        return second if first is None else jnp.logical_and(first, second)

    sent_place = lax.rem(me_r - group - 1 + 2 * cols, cols)

    class Gather:
        def __init__(self, stage, piece, place, keep):
            self.stage, self.piece, self.place, self.keep = stage, piece, place, keep
            self.active = keep(me_r, group)

        def plane(self, step):
            if self.stage in FAR:
                return jnp.where(group < half // 2, half - 1 - step, step)
            return lax.rem(group + 1 + step, half)

        def copy(self, q, step, side):
            goal = self.plane(step) * 2 + side
            return pltpu.make_async_remote_copy(
                src_ref=self.piece(q, side, goal),
                dst_ref=self.place(q, core, sent_place, goal),
                send_sem=g_send.at[self.stage, q, side, step],
                recv_sem=g_recv.at[self.stage, q, sent_place, core],
                device_id=(goal, group),
                device_id_type=MESH,
            )

        def sends(self, action):
            for step in range(half):
                goal = self.plane(step)
                for side in range(2):
                    elsewhere = jnp.logical_or(goal != group, group != me_r)
                    elsewhere = jnp.logical_or(elsewhere, core != side)
                    guard(both(self.keep(group, goal), elsewhere), functools.partial(action, step, side))

        def start(self, q):
            self.sends(lambda step, side: self.copy(q, step, side).start())

            @pl.when(group == me_r)
            def _():
                pltpu.make_async_copy(
                    self.piece(q, core, me_p),
                    self.place(q, core, last, me_p),
                    g_recv.at[self.stage, q, last, core],
                ).start()

        def arrive(self, q):
            for spot in [last] + list(range(last)):
                for part in range(2):
                    place = self.place(q, part, spot, me_p)
                    pltpu.make_async_copy(place, place, g_recv.at[self.stage, q, spot, part]).wait()

        def finish(self, q):
            self.sends(lambda step, side: self.copy(q, step, side).wait_send())

    class Scatter:
        def __init__(self, stage, source, target, own, keep):
            self.stage, self.source, self.target, self.own, self.keep = stage, source, target, own, keep
            self.active = keep(me_r, group)

        def copy(self, q, step, side):
            return pltpu.make_async_remote_copy(
                src_ref=self.source.at[q, step, side],
                dst_ref=self.target.at[q, core, step],
                send_sem=rs_send.at[self.stage, q, step, side],
                recv_sem=rs_recv.at[self.stage, q, core, step],
                device_id=(group * 2 + side, lax.rem(me_r + 1 + step, cols)),
                device_id_type=MESH,
            )

        def to_mate(self, q):
            return pltpu.make_async_remote_copy(
                src_ref=self.source.at[q, last, 1 - core],
                dst_ref=self.target.at[q, core, last],
                send_sem=rs_send.at[self.stage, q, last, 0],
                recv_sem=rs_recv.at[self.stage, q, core, last],
                device_id=(mate, me_r),
                device_id_type=MESH,
            )

        def put(self, q, side, lanes, value):
            for step in range(cols):
                block = value[step * wj : (step + 1) * wj]
                self.source[q, step, side, :, lanes] = block.astype(BF)
            self.own[q, side, :, lanes] = value[last * wj :]

        def start(self, q):
            for step in range(last):
                for side in range(2):
                    self.copy(q, step, side).start()
            self.to_mate(q).start()

        def landed(self, q, side, step):
            place = self.target.at[q, side, step]
            pltpu.make_async_copy(place, place, rs_recv.at[self.stage, q, side, step]).wait()

        def add(self, q, total_ref):
            def mine():
                total_ref[core] += self.own[q, core]
                self.landed(q, 1 - core, last)
                total_ref[1 - core] += self.target[q, 1 - core, last].astype(F32)

            guard(self.active, mine)
            for step in range(last):
                sender = lax.rem(me_r + last - step, cols)

                def action(step=step):
                    for side in range(2):
                        self.landed(q, side, step)
                        total_ref[side] += self.target[q, side, step].astype(F32)

                guard(self.keep(sender, group), action)

        def finish(self, q):
            def action():
                for step in range(last):
                    for side in range(2):
                        self.copy(q, step, side).wait_send()
                self.to_mate(q).wait_send()

            guard(self.active, action)

    def same(panel):
        return panel // half

    def other(panel):
        return 1 - panel // half

    def pins(pick):
        return (
            lambda q, side, goal: pin.at[pick(goal), q, side],
            lambda q, part, spot, goal: x_pin.at[pick(goal), q, part, spot],
        )

    def level_parts(level):
        return (
            lambda q, side, goal: vec.at[level, q, side],
            lambda q, part, spot, goal: x_par.at[level, q, part, spot],
        )

    g_own = Gather(0, *pins(same), every)
    g_other = Gather(5, *pins(other), below)
    g_low = Gather(1, *level_parts(0), below)
    g_up = Gather(3, *level_parts(1), above)
    g_all = Gather(4, *level_parts(2), every)
    g_half = Gather(
        2,
        lambda q, side, goal: phalf.at[q, side],
        lambda q, part, spot, goal: x_half.at[q, part, spot],
        above,
    )
    t_up, t_low, t_high = [
        Scatter(stage, s_par.at[stage], r_par.at[stage], own_par.at[stage], keep)
        for stage, keep in enumerate((every, below, above))
    ]
    t_piv, t_child = [
        Scatter(3 + index, s_piv.at[index], r_piv.at[index], own_piv.at[index], keep)
        for index, keep in enumerate((below, every))
    ]

    def gathered(block):
        return block.reshape(cols * block.shape[1], block.shape[2])

    for q in chunks:
        g_own.start(q)
    for index in range(6):
        mate_rows(index).start()
    for q in chunks:
        g_other.start(q)

    fetch(1).wait()
    fetch(2).wait()
    sum_par[0] = update_rhs[...].T.reshape(SPLIT, 2, wj, m)
    sum_par[3] = parent_rhs[...].T.reshape(SPLIT, 2, wj, m)
    for level in (1, 2):
        sum_par[level] = jnp.zeros_like(sum_par[level])
    sum_piv[...] = jnp.zeros_like(sum_piv)
    direct[...] = jnp.zeros_like(direct)
    rows = lax.broadcasted_iota(jnp.int32, (m, m // 2), 0)
    for k in range(2):
        start = pl.multiple_of(k * (maps.shape[1] // 2) + me_p * (m // 2), 128)
        chosen[k] = (rows == maps[:, pl.ds(start, m // 2)] - me_p * m).astype(F32).astype(BF)
    ready(lower_update)

    def spread(scatter, q, value, size):
        for side in range(2):
            scatter.put(q, side, slice(None), value[:, side * size : (side + 1) * size])
        scatter.start(q)

    for q in chunks:
        with jax.named_scope("s1_arrive"):
            g_own.arrive(q)
        with jax.named_scope("s1_comp"):
            held = lower_update[...].reshape(2 * m, 2 * mk)
            value = sum(
                dot_rows(gathered(x_pin[child, q, part]), held[:, part * mk : (part + 1) * mk])
                for part in range(2)
            )
            spread(t_up, q, value, m)

    ready(lower_pivot)

    def pivots():
        for q in chunks:
            g_other.arrive(q)
            for side in range(2):
                for k in range(2):
                    value = sum(
                        dot_rows(
                            gathered(x_pin[k, q, part]),
                            lower_pivot[side, k, :, part * mk : (part + 1) * mk],
                        )
                        for part in range(2)
                    )
                    t_piv.put(q, side, slice(k * mk, (k + 1) * mk), value)
            t_piv.start(q)

    with jax.named_scope("pivots"):
        guard(g_other.active, pivots)

    wide = upper_update.shape[3]
    ready(upper_update)
    with jax.named_scope("picked"):
        rows = lax.broadcasted_iota(jnp.int32, (2 * m, wide), 0)
        for k in range(2):
            start = pl.multiple_of(k * (maps.shape[1] // 2) + me_r * wide, 128)
            hot = (rows == maps[:, pl.ds(start, wide)] - me_r * 2 * m).astype(F32).astype(BF)
            for side in range(2):
                picked[side, k] = dot_rows(upper_update[side, k], hot).astype(BF)

    first = lax.rem(me_p, half) * 2

    def shuffle(q, side):
        return pltpu.make_async_remote_copy(
            src_ref=uhalf.at[q, side],
            dst_ref=moved.at[q, child],
            send_sem=sh_send.at[q, side],
            recv_sem=sh_recv.at[q, child],
            device_id=(first + side, me_r),
            device_id_type=MESH,
        )

    def reduce(q):
        with jax.named_scope("s1_add"):
            t_up.add(q, sum_par.at[0, q])
        update = sum_par[0, q].reshape(wq, m).astype(BF)
        for side in range(2):
            uhalf[q, side] = update[:, side * (m // 2) : (side + 1) * (m // 2)]

            @pl.when(first + side != me_p)
            def _():
                shuffle(q, side).start()

            @pl.when(first + side == me_p)
            def _():
                pltpu.make_async_copy(uhalf.at[q, side], moved.at[q, child], sh_recv.at[q, child]).start()

    def assemble(q):
        value = sum_par[3, q].reshape(wq, m)
        for k in range(2):
            with jax.named_scope("moved"):
                pltpu.make_async_copy(moved.at[q, k], moved.at[q, k], sh_recv.at[q, k]).wait()
            value = value + dot_rows(moved[q, k], chosen[k])
        vec[0, q] = value.astype(BF).reshape(2, wj, m)
        g_low.start(q)

    for q in chunks:
        reduce(q)
        if q >= 1:
            assemble(q - 1)
    assemble(SPLIT - 1)

    def parent(level, gather, scatter, factor, following, name):
        ready(factor)
        for q in chunks:

            def action(q=q):
                with jax.named_scope(name + "_arrive"):
                    gather.arrive(q)
                held = factor[...].reshape(2 * m, 2 * m)
                value = sum(
                    dot_rows(gathered(x_par[level, q, part]), held[:, part * m : (part + 1) * m])
                    for part in range(2)
                )
                spread(scatter, q, value, m)

            guard(gather.active, action)
            with jax.named_scope(name + "_add"):
                scatter.add(q, sum_par.at[level + 1, q])
            vec[level + 1, q] = sum_par[level + 1, q].astype(BF)
            following.start(q)

    parent(0, g_low, t_low, parent_lower, g_up, "low")

    for q in chunks:
        with jax.named_scope("piv_add"):
            t_piv.add(q, sum_piv.at[0, q])
        phalf[q] = sum_piv[0, q].astype(BF)
        g_half.start(q)

    parent(1, g_up, t_high, parent_upper, g_all, "up")

    ready(upper_pivot)

    def known():
        for q in chunks:
            g_half.arrive(q)
            for side in range(2):
                for k in range(2):
                    value = sum(
                        dot_rows(
                            gathered(x_half[q, part, :, :, k * mk : (k + 1) * mk]),
                            upper_pivot[side, k, :, part * mk : (part + 1) * mk],
                        )
                        for part in range(2)
                    )
                    base = (side * 2 + k) * mk
                    direct[q, :, base : base + mk] = value

    with jax.named_scope("known"):
        guard(g_half.active, known)
    parent_out[...] = sum_par[2].reshape(width, m).T

    for q in chunks:
        with jax.named_scope("all_arrive"):
            g_all.arrive(q)
        with jax.named_scope("all_comp"):
            held = picked[...].reshape(4 * mk, 2 * m)
            value = direct[q] + sum(
                dot_rows(gathered(x_par[2, q, part]), held[:, part * m : (part + 1) * m])
                for part in range(2)
            )
            spread(t_child, q, value, 2 * mk)

    with jax.named_scope("gfinish"):
        for index in range(6):
            mate_rows(index).wait_send()
        for q in chunks:
            for gather in (g_own, g_other, g_low, g_half, g_up, g_all):
                gather.finish(q)
            for side in range(2):

                @pl.when(first + side != me_p)
                def _():
                    shuffle(q, side).wait_send()

    for q in chunks:
        with jax.named_scope("ch_add"):
            t_child.add(q, sum_piv.at[1, q])
    result = sum_piv[1].reshape(width, 2 * mk).T
    for k in range(2):
        child_out[k] = result[k * mk : (k + 1) * mk]
    for q in chunks:
        for scatter in (t_up, t_low, t_high, t_piv, t_child):
            scatter.finish(q)


def shards(panels, cols, *arguments):
    *arrays, maps = arguments
    m, width = arrays[1].shape
    mk = arrays[0].shape[1]
    wide = arrays[8].shape[2]
    if panels != 2 * cols or mk % 128 or m != 2 * mk or m % 256 or wide % 128 or width % (32 * SPLIT):
        return plain_shards(panels, cols, *arguments)
    wj = width // SPLIT // 2
    vm = pltpu.VMEM
    dma = pltpu.SemaphoreType.DMA
    return pl.pallas_call(
        functools.partial(split_kernel, panels, cols),
        out_shape=(
            pltpu.VMEM((m, width), F32),
            pltpu.VMEM((2, mk, width), F32),
        ),
        in_specs=[pl.BlockSpec(memory_space=pl.ANY)] * 9 + [pl.BlockSpec(memory_space=pltpu.VMEM)],
        out_specs=(pl.BlockSpec(memory_space=pltpu.VMEM),) * 2,
        scratch_shapes=[
            *[vm(array.shape, array.dtype) for array in arrays[:3]],
            *[vm((2,) + array.shape, array.dtype) for array in arrays[3:]],
            vm((2, SPLIT, 2, wj, mk), BF),
            vm((2, SPLIT, 2, cols, wj, mk), BF),
            vm((SPLIT, 2, 2 * wj, m // 2), BF),
            vm((SPLIT, 2, 2 * wj, m // 2), BF),
            vm((2, m, m // 2), BF),
            vm((3, SPLIT, 2, wj, m), BF),
            vm((3, SPLIT, 2, cols, wj, m), BF),
            vm((SPLIT, 2, wj, 2 * mk), BF),
            vm((SPLIT, 2, cols, wj, 2 * mk), BF),
            vm((2, 2, mk, 2 * m), BF),
            vm((SPLIT, cols * wj, 4 * mk), F32),
            vm((3, SPLIT, cols, 2, wj, m), BF),
            vm((3, SPLIT, 2, cols, wj, m), BF),
            vm((2, SPLIT, cols, 2, wj, 2 * mk), BF),
            vm((2, SPLIT, 2, cols, wj, 2 * mk), BF),
            vm((3, SPLIT, 2, wj, m), F32),
            vm((2, SPLIT, 2, wj, 2 * mk), F32),
            vm((4, SPLIT, 2, wj, m), F32),
            vm((2, SPLIT, 2, wj, 2 * mk), F32),
            dma((6, SPLIT, 2, panels // 2)),
            dma((6, SPLIT, cols, 2)),
            dma((5, SPLIT, cols, 2)),
            dma((5, SPLIT, 2, cols)),
            dma((SPLIT, 2)),
            dma((SPLIT, 2)),
            dma((9,)),
            dma((6,)),
            dma((6,)),
        ],
        compiler_params=pltpu.CompilerParams(
            collective_id=0, has_side_effects=True, vmem_limit_bytes=60 * 1024 * 1024
        ),
    )(*arrays, maps.reshape(1, -1))


def solution(mesh):
    panels, cols = mesh.shape["panel"], mesh.shape["rhs"]
    placed = (
        P(None, "panel", "rhs"),
        P("panel", "rhs"),
        P("panel", "rhs"),
        P(None, "panel", "rhs"),
        P("panel", "rhs"),
        P("panel", "rhs"),
        P("panel", "rhs"),
        P(None, "panel", "rhs"),
        P(None, "panel", "rhs"),
        P(),
    )
    return jax.shard_map(
        functools.partial(shards, panels, cols),
        mesh=mesh,
        in_specs=placed,
        out_specs=(P("panel", "rhs"), P(None, "panel", "rhs")),
        check_vma=False,
    )
```

```python
import functools

import jax
import jax.numpy as jnp
from jax import lax
from jax.experimental import pallas as pl
from jax.experimental.pallas import tpu as pltpu
from jax.sharding import PartitionSpec as P

BF = jnp.bfloat16
F32 = jnp.float32
MESH = pl.DeviceIdType.MESH


def dot(left, right):
    return jnp.dot(left, right, preferred_element_type=F32)


def plain_kernel(
    panels,
    cols,
    pivot_rhs,
    update_rhs,
    parent_rhs,
    lower_pivot,
    lower_update,
    parent_lower,
    parent_upper,
    upper_pivot,
    upper_update,
    row_map,
    col_map,
    parent_out,
    child_out,
    pin,
    phalf,
    vec,
    x_pin,
    x_half,
    x_par,
    s_up,
    r_up,
    s_piv,
    r_piv,
    s_par,
    r_par,
    s_ch,
    r_ch,
    uhalf,
    moved,
    picked,
    direct,
    par_sum,
    spread_sum,
    child_sum,
    g_send,
    g_recv,
    f_send,
    rs_send,
    rs_recv,
    sh_send,
    sh_recv,
):
    me_p, me_r = lax.axis_index("panel"), lax.axis_index("rhs")
    total = panels * cols
    me = me_p * cols + me_r
    core = lax.rem(me_p, 2)
    mate = me_p + 1 - 2 * core
    per = panels // cols
    half = panels // 2
    m = parent_rhs.shape[0]
    mk = pivot_rhs.shape[1]
    child = me_p // half

    barrier = pltpu.get_barrier_semaphore()

    @pl.loop(1, total)
    def _(step):
        other = lax.rem(me + step, total)
        pl.semaphore_signal(
            barrier,
            inc=1,
            device_id=(other // cols, lax.rem(other, cols)),
            device_id_type=MESH,
        )

    pin[...] = pivot_rhs[...].astype(BF)
    direct[...] = jnp.zeros_like(direct)
    pl.semaphore_wait(barrier, total - 1)

    group = me_p // per
    last = cols - 1

    def every(source, goal):
        return None

    def below(source, goal):
        return goal >= source

    def above(source, goal):
        return goal <= source

    def guard(condition, action):
        if condition is None:
            action()
        else:
            pl.when(condition)(action)

    def both(first, second):
        return second if first is None else jnp.logical_and(first, second)

    def spot(buffer, depth, column, part, lead):
        rows = pl.ds(pl.multiple_of(part * depth, depth), depth)
        return buffer.at[column, slice(None) if lead is None else pl.ds(lead, 1), rows, :]

    class Gather:
        def __init__(self, stage, block, buffer, depth, keep, lead):
            self.stage, self.block, self.buffer, self.depth = stage, block, buffer, depth
            self.keep, self.lead = keep, lead
            self.active = keep(me_r, group)

        def place(self, column, part, panel):
            return spot(self.buffer, self.depth, column, part, self.lead(panel))

        def piece(self, panel):
            lead = self.lead(panel)
            return self.block if lead is None else self.block.at[pl.ds(lead, 1)]

        def goal(self, step):
            return lax.rem(me_p // 2 + step, half) * 2 + core

        def copy(self, step):
            goal = self.goal(step)
            return pltpu.make_async_remote_copy(
                src_ref=self.piece(goal),
                dst_ref=self.place(me_r, lax.rem(me_p, per), goal),
                send_sem=g_send.at[self.stage, step],
                recv_sem=g_recv.at[self.stage, me_r, lax.rem(me_p, per)],
                device_id=(goal, group),
                device_id_type=MESH,
            )

        def sends(self, action):
            for step in list(range(1, half)) + [0]:
                condition = self.keep(group, self.goal(step) // per)
                if step == 0:
                    condition = both(condition, group != me_r)
                guard(condition, functools.partial(action, step))

        def start(self):
            self.sends(lambda step: self.copy(step).start())

            @pl.when(group == me_r)
            def _():
                part = lax.rem(me_p, per)
                pltpu.make_async_copy(
                    self.piece(me_p),
                    self.place(me_r, part, me_p),
                    g_recv.at[self.stage, me_r, part],
                ).start()

        def landed(self, column, part):
            place = self.place(column, part, me_p)
            pltpu.make_async_copy(place, place, g_recv.at[self.stage, column, part]).wait()

        def forward(self, step, pair):
            column = lax.rem(me_r + 1 + step, cols)
            part = 2 * pair + core
            return pltpu.make_async_remote_copy(
                src_ref=self.place(column, part, me_p),
                dst_ref=self.place(column, part, me_p),
                send_sem=f_send.at[self.stage, step, pair],
                recv_sem=g_recv.at[self.stage, column, part],
                device_id=(mate, me_r),
                device_id_type=MESH,
            )

        def pass_on(self):
            def action():
                for step in [last] + list(range(last)):
                    for pair in range(per // 2):
                        self.landed(lax.rem(me_r + 1 + step, cols), 2 * pair + core)
                        self.forward(step, pair).start()

            guard(self.active, action)

        def arrive(self, step):
            column = lax.rem(me_r + 1 + step, cols)
            for pair in range(per // 2):
                self.landed(column, 2 * pair + 1 - core)
            return column

        def finish(self):
            self.sends(lambda step: self.copy(step).wait_send())

            def action():
                for step in range(cols):
                    for pair in range(per // 2):
                        self.forward(step, pair).wait_send()

            guard(self.active, action)

    class Scatter:
        def __init__(self, stage, source, target, keep):
            self.stage, self.source, self.target, self.keep = stage, source, target, keep
            self.active = keep(me_r, group)

        def copy(self, step):
            return pltpu.make_async_remote_copy(
                src_ref=self.source.at[step],
                dst_ref=self.target.at[step],
                send_sem=rs_send.at[self.stage, step],
                recv_sem=rs_recv.at[self.stage, step],
                device_id=(me_p, lax.rem(me_r + 1 + step, cols)),
                device_id_type=MESH,
            )

        def add(self, total_ref):
            for step in range(last):
                sender = lax.rem(me_r + last - step, cols)

                def action(step=step):
                    self.copy(step).wait_recv()
                    total_ref[...] += self.target[step].astype(F32)

                guard(self.keep(sender, group), action)

        def finish(self):
            def action():
                for step in range(last):
                    self.copy(step).wait_send()

            guard(self.active, action)

    def targets(ref, k, index, size, base):
        if ref.shape[0] == 2:
            return ref[k : k + 1, :]
        start = pl.multiple_of(k * (ref.shape[1] // 2) + index * size, 128)
        return ref[:, pl.ds(start, size)] - base

    def whole(panel):
        return None

    def same(panel):
        return panel // half

    def other(panel):
        return 1 - panel // half

    g_own = Gather(0, pin, x_pin, mk, every, same)
    g_other = Gather(5, pin, x_pin, mk, below, other)
    g_low = Gather(1, vec.at[0], x_par.at[0], m, below, whole)
    g_half = Gather(2, phalf, x_half, mk, above, whole)
    g_up = Gather(3, vec.at[1], x_par.at[1], m, above, whole)
    g_all = Gather(4, vec.at[2], x_par.at[2], m, every, whole)
    t_up = Scatter(0, s_up, r_up, every)
    t_piv = Scatter(1, s_piv, r_piv, below)
    t_low = Scatter(2, s_par.at[0], r_par.at[0], below)
    t_high = Scatter(3, s_par.at[1], r_par.at[1], above)
    t_child = Scatter(4, s_ch, r_ch, every)

    g_own.start()
    g_other.start()

    width = upper_update.shape[2]
    for k in range(2):
        rows = lax.broadcasted_iota(jnp.int32, (per * m, width), 0)
        chosen = (rows == targets(col_map, k, me_r, width, me_r * per * m)).astype(F32).astype(BF)
        picked[k] = lax.dot_general(
            upper_update[k], chosen, (((1,), (1,)), ((), ())), preferred_element_type=F32
        ).astype(BF)
    spread_sum[...] = parent_rhs[...]

    g_own.pass_on()
    for step in range(cols):
        column = g_own.arrive(step)
        value = dot(lower_update[...], x_pin[column, child])
        if step < last:
            s_up[step] = value.astype(BF)
            t_up.copy(step).start()
        else:
            par_sum[...] = update_rhs[...] + value
    g_other.pass_on()
    t_up.add(par_sum)
    update = par_sum[...].astype(BF)
    uhalf[0] = update[: m // 2]
    uhalf[1] = update[m // 2 :]
    first = lax.rem(me_p, half) * 2

    def shuffle(side):
        return pltpu.make_async_remote_copy(
            src_ref=uhalf.at[side],
            dst_ref=moved.at[child],
            send_sem=sh_send.at[side],
            recv_sem=sh_recv.at[child],
            device_id=(first + side, me_r),
            device_id_type=MESH,
        )

    for side in range(2):

        @pl.when(first + side != me_p)
        def _():
            shuffle(side).start()

        @pl.when(first + side == me_p)
        def _():
            pltpu.make_async_copy(uhalf.at[side], moved.at[child], sh_recv.at[child]).start()

    child_sum[...] = jnp.zeros_like(child_sum)

    def pivots():
        for step in range(cols):
            column = g_other.arrive(step)
            for k in range(2):
                value = dot(lower_pivot[k], x_pin[column, k])
                if step < last:
                    s_piv[step, k] = value.astype(BF)
                else:
                    child_sum[k] = value
            if step < last:
                t_piv.copy(step).start()

    guard(g_other.active, pivots)

    rows = lax.broadcasted_iota(jnp.int32, (m, m // 2), 0)
    for k in range(2):
        pltpu.make_async_copy(moved.at[k], moved.at[k], sh_recv.at[k]).wait()
        chosen = (rows == targets(row_map, k, me_p, m // 2, me_p * m)).astype(F32).astype(BF)
        spread_sum[...] += dot(chosen, moved[k])
    vec[0, 0] = spread_sum[...].astype(BF)
    g_low.start()

    t_piv.add(child_sum)
    phalf[...] = child_sum[...].astype(BF)
    g_half.start()

    def parent(level, gather, scatter, factor):
        par_sum[...] = jnp.zeros_like(par_sum)
        gather.pass_on()

        def action():
            for step in range(cols):
                column = gather.arrive(step)
                value = dot(factor[...], x_par[level, column, 0])
                if step < last:
                    s_par[level, step] = value.astype(BF)
                    scatter.copy(step).start()
                else:
                    par_sum[...] = value

        guard(gather.active, action)
        scatter.add(par_sum)
        vec[level + 1, 0] = par_sum[...].astype(BF)

    parent(0, g_low, t_low, parent_lower)
    g_up.start()
    g_half.pass_on()

    def known():
        for step in range(cols):
            column = g_half.arrive(step)
            for k in range(2):
                direct[step, k] = dot(upper_pivot[k], x_half[column, k])

    guard(g_half.active, known)
    parent(1, g_up, t_high, parent_upper)
    g_all.start()
    parent_out[...] = par_sum[...]

    g_all.pass_on()
    for step in range(cols):
        column = g_all.arrive(step)
        for k in range(2):
            value = direct[step, k] + dot(picked[k], x_par[2, column, 0])
            if step < last:
                s_ch[step, k] = value.astype(BF)
            else:
                child_out[k] = value
        if step < last:
            t_child.copy(step).start()
    for gather in (g_own, g_other, g_low, g_half, g_up, g_all):
        gather.finish()
    for side in range(2):

        @pl.when(first + side != me_p)
        def _():
            shuffle(side).wait_send()

    t_child.add(child_out)
    for scatter in (t_up, t_piv, t_low, t_high, t_child):
        scatter.finish()


def plain_shards(panels, cols, *arguments):
    *arrays, maps = arguments
    m, width = arrays[1].shape
    mk = arrays[0].shape[1]
    per = panels // cols
    sides = maps.reshape(2, -1)
    me_p, me_r = lax.axis_index("panel"), lax.axis_index("rhs")
    wide = arrays[8].shape[2]

    def cut(index, size, base):
        if size % 128 == 0:
            return maps.reshape(1, -1)
        return lax.dynamic_slice_in_dim(sides, index * size, size, 1) - base

    row_map = cut(me_p, m // 2, me_p * m)
    col_map = cut(me_r, wide, me_r * per * m)
    vm = pltpu.VMEM
    dma = pltpu.SemaphoreType.DMA
    return pl.pallas_call(
        functools.partial(plain_kernel, panels, cols),
        out_shape=(
            jax.ShapeDtypeStruct((m, width), F32),
            jax.ShapeDtypeStruct((2, mk, width), F32),
        ),
        in_specs=[pl.BlockSpec(memory_space=pltpu.VMEM)] * 11,
        out_specs=(pl.BlockSpec(memory_space=pltpu.VMEM),) * 2,
        scratch_shapes=[
            vm((2, mk, width), BF),
            vm((2, mk, width), BF),
            vm((3, 1, m, width), BF),
            vm((cols, 2, per * mk, width), BF),
            vm((cols, 2, per * mk, width), BF),
            vm((3, cols, 1, per * m, width), BF),
            vm((cols - 1, m, width), BF),
            vm((cols - 1, m, width), BF),
            vm((cols - 1, 2, mk, width), BF),
            vm((cols - 1, 2, mk, width), BF),
            vm((2, cols - 1, m, width), BF),
            vm((2, cols - 1, m, width), BF),
            vm((cols - 1, 2, mk, width), BF),
            vm((cols - 1, 2, mk, width), BF),
            vm((2, m // 2, width), BF),
            vm((2, m // 2, width), BF),
            vm((2, mk, per * m), BF),
            vm((cols, 2, mk, width), F32),
            vm((m, width), F32),
            vm((m, width), F32),
            vm((2, mk, width), F32),
            dma((6, panels // 2)),
            dma((6, cols, per)),
            dma((6, cols, per // 2)),
            dma((5, cols - 1)),
            dma((5, cols - 1)),
            dma((2,)),
            dma((2,)),
        ],
        compiler_params=pltpu.CompilerParams(
            collective_id=0, has_side_effects=True, vmem_limit_bytes=60 * 1024 * 1024
        ),
    )(*arrays, row_map, col_map)


SPLIT = 2
FAR = (4,)


def dot_rows(left, right):
    return lax.dot_general(left, right, (((1,), (1,)), ((), ())), preferred_element_type=F32)


def split_kernel(
    panels,
    cols,
    pivot_at,
    update_at,
    parent_at,
    lower_pivot_at,
    lower_update_at,
    parent_lower_at,
    parent_upper_at,
    upper_pivot_at,
    upper_update_at,
    maps,
    parent_out,
    child_out,
    pivot_rhs,
    update_rhs,
    parent_rhs,
    lower_pivot,
    lower_update,
    parent_lower,
    parent_upper,
    upper_pivot,
    upper_update,
    pin,
    x_pin,
    uhalf,
    moved,
    chosen,
    vec,
    x_par,
    phalf,
    x_half,
    picked,
    direct,
    s_par,
    r_par,
    s_piv,
    r_piv,
    own_par,
    own_piv,
    sum_par,
    sum_piv,
    g_send,
    g_recv,
    rs_send,
    rs_recv,
    sh_send,
    sh_recv,
    in_sem,
    mate_send,
    mate_recv,
):
    me_p, me_r = lax.axis_index("panel"), lax.axis_index("rhs")
    total = panels * cols
    me = me_p * cols + me_r
    core = lax.rem(me_p, 2)
    mate = me_p + 1 - 2 * core
    half = panels // 2
    m, width = parent_rhs.shape
    mk = pivot_rhs.shape[1]
    wq = width // SPLIT
    wj = wq // 2
    child = me_p // half
    group = me_p // 2
    last = cols - 1
    chunks = range(SPLIT)

    factors = (
        (lower_update_at, lower_update),
        (lower_pivot_at, lower_pivot),
        (upper_update_at, upper_update),
        (parent_lower_at, parent_lower),
        (parent_upper_at, parent_upper),
        (upper_pivot_at, upper_pivot),
    )
    vectors = ((pivot_at, pivot_rhs), (update_at, update_rhs), (parent_at, parent_rhs))

    def own_rows(index):
        return pltpu.make_async_copy(factors[index][0], factors[index][1].at[core], in_sem.at[index])

    def mate_rows(index):
        return pltpu.make_async_remote_copy(
            src_ref=factors[index][0],
            dst_ref=factors[index][1].at[core],
            send_sem=mate_send.at[index],
            recv_sem=mate_recv.at[index],
            device_id=(mate, me_r),
            device_id_type=MESH,
        )

    def ready(held):
        index = [pair[1] is held for pair in factors].index(True)
        own_rows(index).wait()
        place = held.at[1 - core]
        pltpu.make_async_copy(place, place, mate_recv.at[index]).wait()

    def fetch(index):
        return pltpu.make_async_copy(*vectors[index], in_sem.at[6 + index])

    fetch(0).start()
    barrier = pltpu.get_barrier_semaphore()

    @pl.loop(1, total)
    def _(step):
        other = lax.rem(me + step, total)
        pl.semaphore_signal(
            barrier,
            inc=1,
            device_id=(other // cols, lax.rem(other, cols)),
            device_id_type=MESH,
        )

    own_rows(0).start()
    fetch(1).start()
    fetch(2).start()
    for index in range(1, 6):
        own_rows(index).start()
    fetch(0).wait()
    for k in range(2):
        pin[k] = pivot_rhs[k].T.astype(BF).reshape(SPLIT, 2, wj, mk)
    with jax.named_scope("barrier"):
        pl.semaphore_wait(barrier, total - 1)

    def every(source, goal):
        return None

    def below(source, goal):
        return goal >= source

    def above(source, goal):
        return goal <= source

    def guard(condition, action):
        if condition is None:
            action()
        else:
            pl.when(condition)(action)

    def both(first, second):
        return second if first is None else jnp.logical_and(first, second)

    sent_place = lax.rem(me_r - group - 1 + 2 * cols, cols)

    class Gather:
        def __init__(self, stage, piece, place, keep):
            self.stage, self.piece, self.place, self.keep = stage, piece, place, keep
            self.active = keep(me_r, group)

        def plane(self, step):
            if self.stage in FAR:
                return jnp.where(group < half // 2, half - 1 - step, step)
            return lax.rem(group + 1 + step, half)

        def copy(self, q, step, side):
            goal = self.plane(step) * 2 + side
            return pltpu.make_async_remote_copy(
                src_ref=self.piece(q, side, goal),
                dst_ref=self.place(q, core, sent_place, goal),
                send_sem=g_send.at[self.stage, q, side, step],
                recv_sem=g_recv.at[self.stage, q, sent_place, core],
                device_id=(goal, group),
                device_id_type=MESH,
            )

        def sends(self, action):
            for step in range(half):
                goal = self.plane(step)
                for side in range(2):
                    elsewhere = jnp.logical_or(goal != group, group != me_r)
                    elsewhere = jnp.logical_or(elsewhere, core != side)
                    guard(both(self.keep(group, goal), elsewhere), functools.partial(action, step, side))

        def start(self, q):
            self.sends(lambda step, side: self.copy(q, step, side).start())

            @pl.when(group == me_r)
            def _():
                pltpu.make_async_copy(
                    self.piece(q, core, me_p),
                    self.place(q, core, last, me_p),
                    g_recv.at[self.stage, q, last, core],
                ).start()

        def arrive(self, q):
            for spot in [last] + list(range(last)):
                for part in range(2):
                    place = self.place(q, part, spot, me_p)
                    pltpu.make_async_copy(place, place, g_recv.at[self.stage, q, spot, part]).wait()

        def finish(self, q):
            self.sends(lambda step, side: self.copy(q, step, side).wait_send())

    class Scatter:
        def __init__(self, stage, source, target, own, keep):
            self.stage, self.source, self.target, self.own, self.keep = stage, source, target, own, keep
            self.active = keep(me_r, group)

        def copy(self, q, step, side):
            return pltpu.make_async_remote_copy(
                src_ref=self.source.at[q, step, side],
                dst_ref=self.target.at[q, core, step],
                send_sem=rs_send.at[self.stage, q, step, side],
                recv_sem=rs_recv.at[self.stage, q, core, step],
                device_id=(group * 2 + side, lax.rem(me_r + 1 + step, cols)),
                device_id_type=MESH,
            )

        def to_mate(self, q):
            return pltpu.make_async_remote_copy(
                src_ref=self.source.at[q, last, 1 - core],
                dst_ref=self.target.at[q, core, last],
                send_sem=rs_send.at[self.stage, q, last, 0],
                recv_sem=rs_recv.at[self.stage, q, core, last],
                device_id=(mate, me_r),
                device_id_type=MESH,
            )

        def put(self, q, side, lanes, value):
            for step in range(cols):
                block = value[step * wj : (step + 1) * wj]
                self.source[q, step, side, :, lanes] = block.astype(BF)
            self.own[q, side, :, lanes] = value[last * wj :]

        def start(self, q):
            for step in range(last):
                for side in range(2):
                    self.copy(q, step, side).start()
            self.to_mate(q).start()

        def landed(self, q, side, step):
            place = self.target.at[q, side, step]
            pltpu.make_async_copy(place, place, rs_recv.at[self.stage, q, side, step]).wait()

        def add(self, q, total_ref):
            def mine():
                total_ref[core] += self.own[q, core]
                self.landed(q, 1 - core, last)
                total_ref[1 - core] += self.target[q, 1 - core, last].astype(F32)

            guard(self.active, mine)
            for step in range(last):
                sender = lax.rem(me_r + last - step, cols)

                def action(step=step):
                    for side in range(2):
                        self.landed(q, side, step)
                        total_ref[side] += self.target[q, side, step].astype(F32)

                guard(self.keep(sender, group), action)

        def finish(self, q):
            def action():
                for step in range(last):
                    for side in range(2):
                        self.copy(q, step, side).wait_send()
                self.to_mate(q).wait_send()

            guard(self.active, action)

    def same(panel):
        return panel // half

    def other(panel):
        return 1 - panel // half

    def pins(pick):
        return (
            lambda q, side, goal: pin.at[pick(goal), q, side],
            lambda q, part, spot, goal: x_pin.at[pick(goal), q, part, spot],
        )

    def level_parts(level):
        return (
            lambda q, side, goal: vec.at[level, q, side],
            lambda q, part, spot, goal: x_par.at[level, q, part, spot],
        )

    g_own = Gather(0, *pins(same), every)
    g_other = Gather(5, *pins(other), below)
    g_low = Gather(1, *level_parts(0), below)
    g_up = Gather(3, *level_parts(1), above)
    g_all = Gather(4, *level_parts(2), every)
    g_half = Gather(
        2,
        lambda q, side, goal: phalf.at[q, side],
        lambda q, part, spot, goal: x_half.at[q, part, spot],
        above,
    )
    t_up, t_low, t_high = [
        Scatter(stage, s_par.at[stage], r_par.at[stage], own_par.at[stage], keep)
        for stage, keep in enumerate((every, below, above))
    ]
    t_piv, t_child = [
        Scatter(3 + index, s_piv.at[index], r_piv.at[index], own_piv.at[index], keep)
        for index, keep in enumerate((below, every))
    ]

    def gathered(block):
        return block.reshape(cols * block.shape[1], block.shape[2])

    for q in chunks:
        g_own.start(q)
    for index in range(6):
        mate_rows(index).start()
    for q in chunks:
        g_other.start(q)

    fetch(1).wait()
    fetch(2).wait()
    sum_par[0] = update_rhs[...].T.reshape(SPLIT, 2, wj, m)
    sum_par[3] = parent_rhs[...].T.reshape(SPLIT, 2, wj, m)
    for level in (1, 2):
        sum_par[level] = jnp.zeros_like(sum_par[level])
    sum_piv[...] = jnp.zeros_like(sum_piv)
    direct[...] = jnp.zeros_like(direct)
    rows = lax.broadcasted_iota(jnp.int32, (m, m // 2), 0)
    for k in range(2):
        start = pl.multiple_of(k * (maps.shape[1] // 2) + me_p * (m // 2), 128)
        chosen[k] = (rows == maps[:, pl.ds(start, m // 2)] - me_p * m).astype(F32).astype(BF)
    ready(lower_update)

    def spread(scatter, q, value, size):
        for side in range(2):
            scatter.put(q, side, slice(None), value[:, side * size : (side + 1) * size])
        scatter.start(q)

    for q in chunks:
        with jax.named_scope("s1_arrive"):
            g_own.arrive(q)
        with jax.named_scope("s1_comp"):
            held = lower_update[...].reshape(2 * m, 2 * mk)
            value = sum(
                dot_rows(gathered(x_pin[child, q, part]), held[:, part * mk : (part + 1) * mk])
                for part in range(2)
            )
            spread(t_up, q, value, m)

    def pivots():
        for q in chunks:
            g_other.arrive(q)
            for side in range(2):
                for k in range(2):
                    value = sum(
                        dot_rows(
                            gathered(x_pin[k, q, part]),
                            lower_pivot[side, k, :, part * mk : (part + 1) * mk],
                        )
                        for part in range(2)
                    )
                    t_piv.put(q, side, slice(k * mk, (k + 1) * mk), value)
            t_piv.start(q)

    ready(lower_pivot)
    with jax.named_scope("pivots"):
        guard(g_other.active, pivots)

    first = lax.rem(me_p, half) * 2

    def shuffle(q, side):
        return pltpu.make_async_remote_copy(
            src_ref=uhalf.at[q, side],
            dst_ref=moved.at[q, child],
            send_sem=sh_send.at[q, side],
            recv_sem=sh_recv.at[q, child],
            device_id=(first + side, me_r),
            device_id_type=MESH,
        )

    def reduce(q):
        with jax.named_scope("s1_add"):
            t_up.add(q, sum_par.at[0, q])
        update = sum_par[0, q].reshape(wq, m).astype(BF)
        for side in range(2):
            uhalf[q, side] = update[:, side * (m // 2) : (side + 1) * (m // 2)]

            @pl.when(first + side != me_p)
            def _():
                shuffle(q, side).start()

            @pl.when(first + side == me_p)
            def _():
                pltpu.make_async_copy(uhalf.at[q, side], moved.at[q, child], sh_recv.at[q, child]).start()

    def assemble(q):
        value = sum_par[3, q].reshape(wq, m)
        for k in range(2):
            with jax.named_scope("moved"):
                pltpu.make_async_copy(moved.at[q, k], moved.at[q, k], sh_recv.at[q, k]).wait()
            value = value + dot_rows(moved[q, k], chosen[k])
        vec[0, q] = value.astype(BF).reshape(2, wj, m)
        g_low.start(q)

    reduce(0)
    reduce(1)
    assemble(0)
    assemble(1)
    wide = upper_update.shape[3]
    ready(upper_update)
    with jax.named_scope("picked"):
        rows = lax.broadcasted_iota(jnp.int32, (2 * m, wide), 0)
        for k in range(2):
            start = pl.multiple_of(k * (maps.shape[1] // 2) + me_r * wide, 128)
            hot = (rows == maps[:, pl.ds(start, wide)] - me_r * 2 * m).astype(F32).astype(BF)
            for side in range(2):
                picked[side, k] = dot_rows(upper_update[side, k], hot).astype(BF)


    def parent(level, gather, scatter, factor, following, name):
        ready(factor)
        for q in chunks:

            def action(q=q):
                with jax.named_scope(name + "_arrive"):
                    gather.arrive(q)
                held = factor[...].reshape(2 * m, 2 * m)
                value = sum(
                    dot_rows(gathered(x_par[level, q, part]), held[:, part * m : (part + 1) * m])
                    for part in range(2)
                )
                spread(scatter, q, value, m)

            guard(gather.active, action)
            with jax.named_scope(name + "_add"):
                scatter.add(q, sum_par.at[level + 1, q])
            vec[level + 1, q] = sum_par[level + 1, q].astype(BF)
            following.start(q)

    for q in chunks:
        with jax.named_scope("piv_add"):
            t_piv.add(q, sum_piv.at[0, q])
        phalf[q] = sum_piv[0, q].astype(BF)
        g_half.start(q)

    parent(0, g_low, t_low, parent_lower, g_up, "low")

    parent(1, g_up, t_high, parent_upper, g_all, "up")

    ready(upper_pivot)

    def known():
        for q in chunks:
            g_half.arrive(q)
            for side in range(2):
                for k in range(2):
                    value = sum(
                        dot_rows(
                            gathered(x_half[q, part, :, :, k * mk : (k + 1) * mk]),
                            upper_pivot[side, k, :, part * mk : (part + 1) * mk],
                        )
                        for part in range(2)
                    )
                    base = (side * 2 + k) * mk
                    direct[q, :, base : base + mk] = value

    with jax.named_scope("known"):
        guard(g_half.active, known)
    parent_out[...] = sum_par[2].reshape(width, m).T

    for q in chunks:
        with jax.named_scope("all_arrive"):
            g_all.arrive(q)
        with jax.named_scope("all_comp"):
            held = picked[...].reshape(4 * mk, 2 * m)
            value = direct[q] + sum(
                dot_rows(gathered(x_par[2, q, part]), held[:, part * m : (part + 1) * m])
                for part in range(2)
            )
            spread(t_child, q, value, 2 * mk)

    with jax.named_scope("gfinish"):
        for index in range(6):
            mate_rows(index).wait_send()
        for q in chunks:
            for gather in (g_own, g_other, g_low, g_half, g_up, g_all):
                gather.finish(q)
            for side in range(2):

                @pl.when(first + side != me_p)
                def _():
                    shuffle(q, side).wait_send()

    for q in chunks:
        with jax.named_scope("ch_add"):
            t_child.add(q, sum_piv.at[1, q])
    result = sum_piv[1].reshape(width, 2 * mk).T
    for k in range(2):
        child_out[k] = result[k * mk : (k + 1) * mk]
    for q in chunks:
        for scatter in (t_up, t_low, t_high, t_piv, t_child):
            scatter.finish(q)


def shards(panels, cols, *arguments):
    *arrays, maps = arguments
    m, width = arrays[1].shape
    mk = arrays[0].shape[1]
    wide = arrays[8].shape[2]
    if panels != 2 * cols or mk % 128 or m != 2 * mk or m % 256 or wide % 128 or width % (32 * SPLIT):
        return plain_shards(panels, cols, *arguments)
    wj = width // SPLIT // 2
    vm = pltpu.VMEM
    dma = pltpu.SemaphoreType.DMA
    return pl.pallas_call(
        functools.partial(split_kernel, panels, cols),
        out_shape=(
            pltpu.VMEM((m, width), F32),
            pltpu.VMEM((2, mk, width), F32),
        ),
        in_specs=[pl.BlockSpec(memory_space=pl.ANY)] * 9 + [pl.BlockSpec(memory_space=pltpu.VMEM)],
        out_specs=(pl.BlockSpec(memory_space=pltpu.VMEM),) * 2,
        scratch_shapes=[
            *[vm(array.shape, array.dtype) for array in arrays[:3]],
            *[vm((2,) + array.shape, array.dtype) for array in arrays[3:]],
            vm((2, SPLIT, 2, wj, mk), BF),
            vm((2, SPLIT, 2, cols, wj, mk), BF),
            vm((SPLIT, 2, 2 * wj, m // 2), BF),
            vm((SPLIT, 2, 2 * wj, m // 2), BF),
            vm((2, m, m // 2), BF),
            vm((3, SPLIT, 2, wj, m), BF),
            vm((3, SPLIT, 2, cols, wj, m), BF),
            vm((SPLIT, 2, wj, 2 * mk), BF),
            vm((SPLIT, 2, cols, wj, 2 * mk), BF),
            vm((2, 2, mk, 2 * m), BF),
            vm((SPLIT, cols * wj, 4 * mk), F32),
            vm((3, SPLIT, cols, 2, wj, m), BF),
            vm((3, SPLIT, 2, cols, wj, m), BF),
            vm((2, SPLIT, cols, 2, wj, 2 * mk), BF),
            vm((2, SPLIT, 2, cols, wj, 2 * mk), BF),
            vm((3, SPLIT, 2, wj, m), F32),
            vm((2, SPLIT, 2, wj, 2 * mk), F32),
            vm((4, SPLIT, 2, wj, m), F32),
            vm((2, SPLIT, 2, wj, 2 * mk), F32),
            dma((6, SPLIT, 2, panels // 2)),
            dma((6, SPLIT, cols, 2)),
            dma((5, SPLIT, cols, 2)),
            dma((5, SPLIT, 2, cols)),
            dma((SPLIT, 2)),
            dma((SPLIT, 2)),
            dma((9,)),
            dma((6,)),
            dma((6,)),
        ],
        compiler_params=pltpu.CompilerParams(
            collective_id=0, has_side_effects=True, vmem_limit_bytes=60 * 1024 * 1024
        ),
    )(*arrays, maps.reshape(1, -1))


def solution(mesh):
    panels, cols = mesh.shape["panel"], mesh.shape["rhs"]
    placed = (
        P(None, "panel", "rhs"),
        P("panel", "rhs"),
        P("panel", "rhs"),
        P(None, "panel", "rhs"),
        P("panel", "rhs"),
        P("panel", "rhs"),
        P("panel", "rhs"),
        P(None, "panel", "rhs"),
        P(None, "panel", "rhs"),
        P(),
    )
    return jax.shard_map(
        functools.partial(shards, panels, cols),
        mesh=mesh,
        in_specs=placed,
        out_specs=(P("panel", "rhs"), P(None, "panel", "rhs")),
        check_vma=False,
    )
```

```python
import functools

import jax
import jax.numpy as jnp
from jax import lax
from jax.experimental import pallas as pl
from jax.experimental.pallas import tpu as pltpu
from jax.sharding import PartitionSpec as P

BF = jnp.bfloat16
F32 = jnp.float32
MESH = pl.DeviceIdType.MESH


def dot(left, right):
    return jnp.dot(left, right, preferred_element_type=F32)


def plain_kernel(
    panels,
    cols,
    pivot_rhs,
    update_rhs,
    parent_rhs,
    lower_pivot,
    lower_update,
    parent_lower,
    parent_upper,
    upper_pivot,
    upper_update,
    row_map,
    col_map,
    parent_out,
    child_out,
    pin,
    phalf,
    vec,
    x_pin,
    x_half,
    x_par,
    s_up,
    r_up,
    s_piv,
    r_piv,
    s_par,
    r_par,
    s_ch,
    r_ch,
    uhalf,
    moved,
    picked,
    direct,
    par_sum,
    spread_sum,
    child_sum,
    g_send,
    g_recv,
    f_send,
    rs_send,
    rs_recv,
    sh_send,
    sh_recv,
):
    me_p, me_r = lax.axis_index("panel"), lax.axis_index("rhs")
    total = panels * cols
    me = me_p * cols + me_r
    core = lax.rem(me_p, 2)
    mate = me_p + 1 - 2 * core
    per = panels // cols
    half = panels // 2
    m = parent_rhs.shape[0]
    mk = pivot_rhs.shape[1]
    child = me_p // half

    barrier = pltpu.get_barrier_semaphore()

    @pl.loop(1, total)
    def _(step):
        other = lax.rem(me + step, total)
        pl.semaphore_signal(
            barrier,
            inc=1,
            device_id=(other // cols, lax.rem(other, cols)),
            device_id_type=MESH,
        )

    pin[...] = pivot_rhs[...].astype(BF)
    direct[...] = jnp.zeros_like(direct)
    pl.semaphore_wait(barrier, total - 1)

    group = me_p // per
    last = cols - 1

    def every(source, goal):
        return None

    def below(source, goal):
        return goal >= source

    def above(source, goal):
        return goal <= source

    def guard(condition, action):
        if condition is None:
            action()
        else:
            pl.when(condition)(action)

    def both(first, second):
        return second if first is None else jnp.logical_and(first, second)

    def spot(buffer, depth, column, part, lead):
        rows = pl.ds(pl.multiple_of(part * depth, depth), depth)
        return buffer.at[column, slice(None) if lead is None else pl.ds(lead, 1), rows, :]

    class Gather:
        def __init__(self, stage, block, buffer, depth, keep, lead):
            self.stage, self.block, self.buffer, self.depth = stage, block, buffer, depth
            self.keep, self.lead = keep, lead
            self.active = keep(me_r, group)

        def place(self, column, part, panel):
            return spot(self.buffer, self.depth, column, part, self.lead(panel))

        def piece(self, panel):
            lead = self.lead(panel)
            return self.block if lead is None else self.block.at[pl.ds(lead, 1)]

        def goal(self, step):
            return lax.rem(me_p // 2 + step, half) * 2 + core

        def copy(self, step):
            goal = self.goal(step)
            return pltpu.make_async_remote_copy(
                src_ref=self.piece(goal),
                dst_ref=self.place(me_r, lax.rem(me_p, per), goal),
                send_sem=g_send.at[self.stage, step],
                recv_sem=g_recv.at[self.stage, me_r, lax.rem(me_p, per)],
                device_id=(goal, group),
                device_id_type=MESH,
            )

        def sends(self, action):
            for step in list(range(1, half)) + [0]:
                condition = self.keep(group, self.goal(step) // per)
                if step == 0:
                    condition = both(condition, group != me_r)
                guard(condition, functools.partial(action, step))

        def start(self):
            self.sends(lambda step: self.copy(step).start())

            @pl.when(group == me_r)
            def _():
                part = lax.rem(me_p, per)
                pltpu.make_async_copy(
                    self.piece(me_p),
                    self.place(me_r, part, me_p),
                    g_recv.at[self.stage, me_r, part],
                ).start()

        def landed(self, column, part):
            place = self.place(column, part, me_p)
            pltpu.make_async_copy(place, place, g_recv.at[self.stage, column, part]).wait()

        def forward(self, step, pair):
            column = lax.rem(me_r + 1 + step, cols)
            part = 2 * pair + core
            return pltpu.make_async_remote_copy(
                src_ref=self.place(column, part, me_p),
                dst_ref=self.place(column, part, me_p),
                send_sem=f_send.at[self.stage, step, pair],
                recv_sem=g_recv.at[self.stage, column, part],
                device_id=(mate, me_r),
                device_id_type=MESH,
            )

        def pass_on(self):
            def action():
                for step in [last] + list(range(last)):
                    for pair in range(per // 2):
                        self.landed(lax.rem(me_r + 1 + step, cols), 2 * pair + core)
                        self.forward(step, pair).start()

            guard(self.active, action)

        def arrive(self, step):
            column = lax.rem(me_r + 1 + step, cols)
            for pair in range(per // 2):
                self.landed(column, 2 * pair + 1 - core)
            return column

        def finish(self):
            self.sends(lambda step: self.copy(step).wait_send())

            def action():
                for step in range(cols):
                    for pair in range(per // 2):
                        self.forward(step, pair).wait_send()

            guard(self.active, action)

    class Scatter:
        def __init__(self, stage, source, target, keep):
            self.stage, self.source, self.target, self.keep = stage, source, target, keep
            self.active = keep(me_r, group)

        def copy(self, step):
            return pltpu.make_async_remote_copy(
                src_ref=self.source.at[step],
                dst_ref=self.target.at[step],
                send_sem=rs_send.at[self.stage, step],
                recv_sem=rs_recv.at[self.stage, step],
                device_id=(me_p, lax.rem(me_r + 1 + step, cols)),
                device_id_type=MESH,
            )

        def add(self, total_ref):
            for step in range(last):
                sender = lax.rem(me_r + last - step, cols)

                def action(step=step):
                    self.copy(step).wait_recv()
                    total_ref[...] += self.target[step].astype(F32)

                guard(self.keep(sender, group), action)

        def finish(self):
            def action():
                for step in range(last):
                    self.copy(step).wait_send()

            guard(self.active, action)

    def targets(ref, k, index, size, base):
        if ref.shape[0] == 2:
            return ref[k : k + 1, :]
        start = pl.multiple_of(k * (ref.shape[1] // 2) + index * size, 128)
        return ref[:, pl.ds(start, size)] - base

    def whole(panel):
        return None

    def same(panel):
        return panel // half

    def other(panel):
        return 1 - panel // half

    g_own = Gather(0, pin, x_pin, mk, every, same)
    g_other = Gather(5, pin, x_pin, mk, below, other)
    g_low = Gather(1, vec.at[0], x_par.at[0], m, below, whole)
    g_half = Gather(2, phalf, x_half, mk, above, whole)
    g_up = Gather(3, vec.at[1], x_par.at[1], m, above, whole)
    g_all = Gather(4, vec.at[2], x_par.at[2], m, every, whole)
    t_up = Scatter(0, s_up, r_up, every)
    t_piv = Scatter(1, s_piv, r_piv, below)
    t_low = Scatter(2, s_par.at[0], r_par.at[0], below)
    t_high = Scatter(3, s_par.at[1], r_par.at[1], above)
    t_child = Scatter(4, s_ch, r_ch, every)

    g_own.start()
    g_other.start()

    width = upper_update.shape[2]
    for k in range(2):
        rows = lax.broadcasted_iota(jnp.int32, (per * m, width), 0)
        chosen = (rows == targets(col_map, k, me_r, width, me_r * per * m)).astype(F32).astype(BF)
        picked[k] = lax.dot_general(
            upper_update[k], chosen, (((1,), (1,)), ((), ())), preferred_element_type=F32
        ).astype(BF)
    spread_sum[...] = parent_rhs[...]

    g_own.pass_on()
    for step in range(cols):
        column = g_own.arrive(step)
        value = dot(lower_update[...], x_pin[column, child])
        if step < last:
            s_up[step] = value.astype(BF)
            t_up.copy(step).start()
        else:
            par_sum[...] = update_rhs[...] + value
    g_other.pass_on()
    t_up.add(par_sum)
    update = par_sum[...].astype(BF)
    uhalf[0] = update[: m // 2]
    uhalf[1] = update[m // 2 :]
    first = lax.rem(me_p, half) * 2

    def shuffle(side):
        return pltpu.make_async_remote_copy(
            src_ref=uhalf.at[side],
            dst_ref=moved.at[child],
            send_sem=sh_send.at[side],
            recv_sem=sh_recv.at[child],
            device_id=(first + side, me_r),
            device_id_type=MESH,
        )

    for side in range(2):

        @pl.when(first + side != me_p)
        def _():
            shuffle(side).start()

        @pl.when(first + side == me_p)
        def _():
            pltpu.make_async_copy(uhalf.at[side], moved.at[child], sh_recv.at[child]).start()

    child_sum[...] = jnp.zeros_like(child_sum)

    def pivots():
        for step in range(cols):
            column = g_other.arrive(step)
            for k in range(2):
                value = dot(lower_pivot[k], x_pin[column, k])
                if step < last:
                    s_piv[step, k] = value.astype(BF)
                else:
                    child_sum[k] = value
            if step < last:
                t_piv.copy(step).start()

    guard(g_other.active, pivots)

    rows = lax.broadcasted_iota(jnp.int32, (m, m // 2), 0)
    for k in range(2):
        pltpu.make_async_copy(moved.at[k], moved.at[k], sh_recv.at[k]).wait()
        chosen = (rows == targets(row_map, k, me_p, m // 2, me_p * m)).astype(F32).astype(BF)
        spread_sum[...] += dot(chosen, moved[k])
    vec[0, 0] = spread_sum[...].astype(BF)
    g_low.start()

    t_piv.add(child_sum)
    phalf[...] = child_sum[...].astype(BF)
    g_half.start()

    def parent(level, gather, scatter, factor):
        par_sum[...] = jnp.zeros_like(par_sum)
        gather.pass_on()

        def action():
            for step in range(cols):
                column = gather.arrive(step)
                value = dot(factor[...], x_par[level, column, 0])
                if step < last:
                    s_par[level, step] = value.astype(BF)
                    scatter.copy(step).start()
                else:
                    par_sum[...] = value

        guard(gather.active, action)
        scatter.add(par_sum)
        vec[level + 1, 0] = par_sum[...].astype(BF)

    parent(0, g_low, t_low, parent_lower)
    g_up.start()
    g_half.pass_on()

    def known():
        for step in range(cols):
            column = g_half.arrive(step)
            for k in range(2):
                direct[step, k] = dot(upper_pivot[k], x_half[column, k])

    guard(g_half.active, known)
    parent(1, g_up, t_high, parent_upper)
    g_all.start()
    parent_out[...] = par_sum[...]

    g_all.pass_on()
    for step in range(cols):
        column = g_all.arrive(step)
        for k in range(2):
            value = direct[step, k] + dot(picked[k], x_par[2, column, 0])
            if step < last:
                s_ch[step, k] = value.astype(BF)
            else:
                child_out[k] = value
        if step < last:
            t_child.copy(step).start()
    for gather in (g_own, g_other, g_low, g_half, g_up, g_all):
        gather.finish()
    for side in range(2):

        @pl.when(first + side != me_p)
        def _():
            shuffle(side).wait_send()

    t_child.add(child_out)
    for scatter in (t_up, t_piv, t_low, t_high, t_child):
        scatter.finish()


def plain_shards(panels, cols, *arguments):
    *arrays, maps = arguments
    m, width = arrays[1].shape
    mk = arrays[0].shape[1]
    per = panels // cols
    sides = maps.reshape(2, -1)
    me_p, me_r = lax.axis_index("panel"), lax.axis_index("rhs")
    wide = arrays[8].shape[2]

    def cut(index, size, base):
        if size % 128 == 0:
            return maps.reshape(1, -1)
        return lax.dynamic_slice_in_dim(sides, index * size, size, 1) - base

    row_map = cut(me_p, m // 2, me_p * m)
    col_map = cut(me_r, wide, me_r * per * m)
    vm = pltpu.VMEM
    dma = pltpu.SemaphoreType.DMA
    return pl.pallas_call(
        functools.partial(plain_kernel, panels, cols),
        out_shape=(
            jax.ShapeDtypeStruct((m, width), F32),
            jax.ShapeDtypeStruct((2, mk, width), F32),
        ),
        in_specs=[pl.BlockSpec(memory_space=pltpu.VMEM)] * 11,
        out_specs=(pl.BlockSpec(memory_space=pltpu.VMEM),) * 2,
        scratch_shapes=[
            vm((2, mk, width), BF),
            vm((2, mk, width), BF),
            vm((3, 1, m, width), BF),
            vm((cols, 2, per * mk, width), BF),
            vm((cols, 2, per * mk, width), BF),
            vm((3, cols, 1, per * m, width), BF),
            vm((cols - 1, m, width), BF),
            vm((cols - 1, m, width), BF),
            vm((cols - 1, 2, mk, width), BF),
            vm((cols - 1, 2, mk, width), BF),
            vm((2, cols - 1, m, width), BF),
            vm((2, cols - 1, m, width), BF),
            vm((cols - 1, 2, mk, width), BF),
            vm((cols - 1, 2, mk, width), BF),
            vm((2, m // 2, width), BF),
            vm((2, m // 2, width), BF),
            vm((2, mk, per * m), BF),
            vm((cols, 2, mk, width), F32),
            vm((m, width), F32),
            vm((m, width), F32),
            vm((2, mk, width), F32),
            dma((6, panels // 2)),
            dma((6, cols, per)),
            dma((6, cols, per // 2)),
            dma((5, cols - 1)),
            dma((5, cols - 1)),
            dma((2,)),
            dma((2,)),
        ],
        compiler_params=pltpu.CompilerParams(
            collective_id=0, has_side_effects=True, vmem_limit_bytes=60 * 1024 * 1024
        ),
    )(*arrays, row_map, col_map)


SPLIT = 2
FAR = (4,)


def dot_rows(left, right):
    return lax.dot_general(left, right, (((1,), (1,)), ((), ())), preferred_element_type=F32)


def split_kernel(
    panels,
    cols,
    pivot_at,
    update_at,
    parent_at,
    lower_pivot_at,
    lower_update_at,
    parent_lower_at,
    parent_upper_at,
    upper_pivot_at,
    upper_update_at,
    maps,
    parent_out,
    child_out,
    pivot_rhs,
    update_rhs,
    parent_rhs,
    lower_pivot,
    lower_update,
    parent_lower,
    parent_upper,
    upper_pivot,
    upper_update,
    pin,
    x_pin,
    uhalf,
    moved,
    chosen,
    vec,
    x_par,
    phalf,
    x_half,
    picked,
    direct,
    s_par,
    r_par,
    s_piv,
    r_piv,
    own_par,
    own_piv,
    sum_par,
    sum_piv,
    g_send,
    g_recv,
    rs_send,
    rs_recv,
    sh_send,
    sh_recv,
    in_sem,
    mate_send,
    mate_recv,
):
    me_p, me_r = lax.axis_index("panel"), lax.axis_index("rhs")
    total = panels * cols
    me = me_p * cols + me_r
    core = lax.rem(me_p, 2)
    mate = me_p + 1 - 2 * core
    half = panels // 2
    m, width = parent_rhs.shape
    mk = pivot_rhs.shape[1]
    wq = width // SPLIT
    wj = wq // 2
    child = me_p // half
    group = me_p // 2
    last = cols - 1
    chunks = range(SPLIT)

    factors = (
        (lower_update_at, lower_update),
        (lower_pivot_at, lower_pivot),
        (upper_update_at, upper_update),
        (parent_lower_at, parent_lower),
        (parent_upper_at, parent_upper),
        (upper_pivot_at, upper_pivot),
    )
    vectors = ((pivot_at, pivot_rhs), (update_at, update_rhs), (parent_at, parent_rhs))

    def own_rows(index):
        return pltpu.make_async_copy(factors[index][0], factors[index][1].at[core], in_sem.at[index])

    def mate_rows(index):
        return pltpu.make_async_remote_copy(
            src_ref=factors[index][0],
            dst_ref=factors[index][1].at[core],
            send_sem=mate_send.at[index],
            recv_sem=mate_recv.at[index],
            device_id=(mate, me_r),
            device_id_type=MESH,
        )

    def ready(held):
        index = [pair[1] is held for pair in factors].index(True)
        own_rows(index).wait()
        place = held.at[1 - core]
        pltpu.make_async_copy(place, place, mate_recv.at[index]).wait()

    def fetch(index):
        return pltpu.make_async_copy(*vectors[index], in_sem.at[6 + index])

    fetch(0).start()
    barrier = pltpu.get_barrier_semaphore()

    @pl.loop(1, total)
    def _(step):
        other = lax.rem(me + step, total)
        pl.semaphore_signal(
            barrier,
            inc=1,
            device_id=(other // cols, lax.rem(other, cols)),
            device_id_type=MESH,
        )

    own_rows(0).start()
    fetch(1).start()
    fetch(2).start()
    for index in range(1, 6):
        own_rows(index).start()
    fetch(0).wait()
    for k in range(2):
        pin[k] = pivot_rhs[k].T.astype(BF).reshape(SPLIT, 2, wj, mk)
    with jax.named_scope("barrier"):
        pl.semaphore_wait(barrier, total - 1)

    def every(source, goal):
        return None

    def below(source, goal):
        return goal >= source

    def above(source, goal):
        return goal <= source

    def guard(condition, action):
        if condition is None:
            action()
        else:
            pl.when(condition)(action)

    def both(first, second):
        return second if first is None else jnp.logical_and(first, second)

    sent_place = lax.rem(me_r - group - 1 + 2 * cols, cols)

    class Gather:
        def __init__(self, stage, piece, place, keep):
            self.stage, self.piece, self.place, self.keep = stage, piece, place, keep
            self.active = keep(me_r, group)

        def plane(self, step):
            if self.stage in FAR:
                return jnp.where(group < half // 2, half - 1 - step, step)
            return lax.rem(group + 1 + step, half)

        def copy(self, q, step, side):
            goal = self.plane(step) * 2 + side
            return pltpu.make_async_remote_copy(
                src_ref=self.piece(q, side, goal),
                dst_ref=self.place(q, core, sent_place, goal),
                send_sem=g_send.at[self.stage, q, side, step],
                recv_sem=g_recv.at[self.stage, q, sent_place, core],
                device_id=(goal, group),
                device_id_type=MESH,
            )

        def sends(self, action):
            for step in range(half):
                goal = self.plane(step)
                for side in range(2):
                    elsewhere = jnp.logical_or(goal != group, group != me_r)
                    elsewhere = jnp.logical_or(elsewhere, core != side)
                    guard(both(self.keep(group, goal), elsewhere), functools.partial(action, step, side))

        def start(self, q):
            self.start_far(q)
            self.start_near(q)

        def start_far(self, q):
            def action(step, side):
                @pl.when(self.plane(step) != group)
                def _():
                    self.copy(q, step, side).start()

            self.sends(action)

        def start_near(self, q):
            def action(step, side):
                @pl.when(self.plane(step) == group)
                def _():
                    self.copy(q, step, side).start()

            self.sends(action)

            @pl.when(group == me_r)
            def _():
                pltpu.make_async_copy(
                    self.piece(q, core, me_p),
                    self.place(q, core, last, me_p),
                    g_recv.at[self.stage, q, last, core],
                ).start()

        def arrive(self, q):
            for spot in [last] + list(range(last)):
                for part in range(2):
                    place = self.place(q, part, spot, me_p)
                    pltpu.make_async_copy(place, place, g_recv.at[self.stage, q, spot, part]).wait()

        def finish(self, q):
            self.sends(lambda step, side: self.copy(q, step, side).wait_send())

    class Scatter:
        def __init__(self, stage, source, target, own, keep):
            self.stage, self.source, self.target, self.own, self.keep = stage, source, target, own, keep
            self.active = keep(me_r, group)

        def copy(self, q, step, side):
            return pltpu.make_async_remote_copy(
                src_ref=self.source.at[q, step, side],
                dst_ref=self.target.at[q, core, step],
                send_sem=rs_send.at[self.stage, q, step, side],
                recv_sem=rs_recv.at[self.stage, q, core, step],
                device_id=(group * 2 + side, lax.rem(me_r + 1 + step, cols)),
                device_id_type=MESH,
            )

        def to_mate(self, q):
            return pltpu.make_async_remote_copy(
                src_ref=self.source.at[q, last, 1 - core],
                dst_ref=self.target.at[q, core, last],
                send_sem=rs_send.at[self.stage, q, last, 0],
                recv_sem=rs_recv.at[self.stage, q, core, last],
                device_id=(mate, me_r),
                device_id_type=MESH,
            )

        def put(self, q, side, lanes, value):
            for step in range(cols):
                block = value[step * wj : (step + 1) * wj]
                self.source[q, step, side, :, lanes] = block.astype(BF)
            self.own[q, side, :, lanes] = value[last * wj :]

        def start(self, q):
            for step in range(last):
                for side in range(2):
                    self.copy(q, step, side).start()
            self.to_mate(q).start()

        def landed(self, q, side, step):
            place = self.target.at[q, side, step]
            pltpu.make_async_copy(place, place, rs_recv.at[self.stage, q, side, step]).wait()

        def add(self, q, total_ref):
            def mine():
                total_ref[core] += self.own[q, core]
                self.landed(q, 1 - core, last)
                total_ref[1 - core] += self.target[q, 1 - core, last].astype(F32)

            guard(self.active, mine)
            for step in range(last):
                sender = lax.rem(me_r + last - step, cols)

                def action(step=step):
                    for side in range(2):
                        self.landed(q, side, step)
                        total_ref[side] += self.target[q, side, step].astype(F32)

                guard(self.keep(sender, group), action)

        def finish(self, q):
            def action():
                for step in range(last):
                    for side in range(2):
                        self.copy(q, step, side).wait_send()
                self.to_mate(q).wait_send()

            guard(self.active, action)

    def same(panel):
        return panel // half

    def other(panel):
        return 1 - panel // half

    def pins(pick):
        return (
            lambda q, side, goal: pin.at[pick(goal), q, side],
            lambda q, part, spot, goal: x_pin.at[pick(goal), q, part, spot],
        )

    def level_parts(level):
        return (
            lambda q, side, goal: vec.at[level, q, side],
            lambda q, part, spot, goal: x_par.at[level, q, part, spot],
        )

    g_own = Gather(0, *pins(same), every)
    g_other = Gather(5, *pins(other), below)
    g_low = Gather(1, *level_parts(0), below)
    g_up = Gather(3, *level_parts(1), above)
    g_all = Gather(4, *level_parts(2), every)
    g_half = Gather(
        2,
        lambda q, side, goal: phalf.at[q, side],
        lambda q, part, spot, goal: x_half.at[q, part, spot],
        above,
    )
    t_up, t_low, t_high = [
        Scatter(stage, s_par.at[stage], r_par.at[stage], own_par.at[stage], keep)
        for stage, keep in enumerate((every, below, above))
    ]
    t_piv, t_child = [
        Scatter(3 + index, s_piv.at[index], r_piv.at[index], own_piv.at[index], keep)
        for index, keep in enumerate((below, every))
    ]

    def gathered(block):
        return block.reshape(cols * block.shape[1], block.shape[2])

    for q in chunks:
        g_own.start(q)
    for index in range(6):
        mate_rows(index).start()
    for q in chunks:
        g_other.start(q)

    fetch(1).wait()
    fetch(2).wait()
    sum_par[0] = update_rhs[...].T.reshape(SPLIT, 2, wj, m)
    sum_par[3] = parent_rhs[...].T.reshape(SPLIT, 2, wj, m)
    for level in (1, 2):
        sum_par[level] = jnp.zeros_like(sum_par[level])
    sum_piv[...] = jnp.zeros_like(sum_piv)
    direct[...] = jnp.zeros_like(direct)
    rows = lax.broadcasted_iota(jnp.int32, (m, m // 2), 0)
    for k in range(2):
        start = pl.multiple_of(k * (maps.shape[1] // 2) + me_p * (m // 2), 128)
        chosen[k] = (rows == maps[:, pl.ds(start, m // 2)] - me_p * m).astype(F32).astype(BF)
    ready(lower_update)

    def spread(scatter, q, value, size):
        for side in range(2):
            scatter.put(q, side, slice(None), value[:, side * size : (side + 1) * size])
        scatter.start(q)

    for q in chunks:
        with jax.named_scope("s1_arrive"):
            g_own.arrive(q)
        with jax.named_scope("s1_comp"):
            held = lower_update[...].reshape(2 * m, 2 * mk)
            value = sum(
                dot_rows(gathered(x_pin[child, q, part]), held[:, part * mk : (part + 1) * mk])
                for part in range(2)
            )
            spread(t_up, q, value, m)

    def pivots():
        for q in chunks:
            g_other.arrive(q)
            for side in range(2):
                for k in range(2):
                    value = sum(
                        dot_rows(
                            gathered(x_pin[k, q, part]),
                            lower_pivot[side, k, :, part * mk : (part + 1) * mk],
                        )
                        for part in range(2)
                    )
                    t_piv.put(q, side, slice(k * mk, (k + 1) * mk), value)
            t_piv.start(q)

    ready(lower_pivot)
    with jax.named_scope("pivots"):
        guard(g_other.active, pivots)

    first = lax.rem(me_p, half) * 2

    def shuffle(q, side):
        return pltpu.make_async_remote_copy(
            src_ref=uhalf.at[q, side],
            dst_ref=moved.at[q, child],
            send_sem=sh_send.at[q, side],
            recv_sem=sh_recv.at[q, child],
            device_id=(first + side, me_r),
            device_id_type=MESH,
        )

    def reduce(q):
        with jax.named_scope("s1_add"):
            t_up.add(q, sum_par.at[0, q])
        update = sum_par[0, q].reshape(wq, m).astype(BF)
        for side in range(2):
            uhalf[q, side] = update[:, side * (m // 2) : (side + 1) * (m // 2)]

            @pl.when(first + side != me_p)
            def _():
                shuffle(q, side).start()

            @pl.when(first + side == me_p)
            def _():
                pltpu.make_async_copy(uhalf.at[q, side], moved.at[q, child], sh_recv.at[q, child]).start()

    def assemble(q):
        value = sum_par[3, q].reshape(wq, m)
        for k in range(2):
            with jax.named_scope("moved"):
                pltpu.make_async_copy(moved.at[q, k], moved.at[q, k], sh_recv.at[q, k]).wait()
            value = value + dot_rows(moved[q, k], chosen[k])
        vec[0, q] = value.astype(BF).reshape(2, wj, m)
        g_low.start(q)

    reduce(0)
    reduce(1)
    assemble(0)
    assemble(1)
    wide = upper_update.shape[3]
    ready(upper_update)
    with jax.named_scope("picked"):
        rows = lax.broadcasted_iota(jnp.int32, (2 * m, wide), 0)
        for k in range(2):
            start = pl.multiple_of(k * (maps.shape[1] // 2) + me_r * wide, 128)
            hot = (rows == maps[:, pl.ds(start, wide)] - me_r * 2 * m).astype(F32).astype(BF)
            for side in range(2):
                picked[side, k] = dot_rows(upper_update[side, k], hot).astype(BF)


    def parent(level, gather, scatter, factor, following, name):
        ready(factor)
        for q in chunks:

            def action(q=q):
                with jax.named_scope(name + "_arrive"):
                    gather.arrive(q)
                held = factor[...].reshape(2 * m, 2 * m)
                value = sum(
                    dot_rows(gathered(x_par[level, q, part]), held[:, part * m : (part + 1) * m])
                    for part in range(2)
                )
                spread(scatter, q, value, m)

            guard(gather.active, action)
        for q in chunks:
            with jax.named_scope(name + "_add"):
                scatter.add(q, sum_par.at[level + 1, q])
            vec[level + 1, q] = sum_par[level + 1, q].astype(BF)
            following.start(q)

    for q in chunks:
        with jax.named_scope("piv_add"):
            t_piv.add(q, sum_piv.at[0, q])
        phalf[q] = sum_piv[0, q].astype(BF)
        g_half.start_far(q)

    parent(0, g_low, t_low, parent_lower, g_up, "low")

    for q in chunks:
        g_half.start_near(q)
    parent(1, g_up, t_high, parent_upper, g_all, "up")

    ready(upper_pivot)

    def known():
        for q in chunks:
            g_half.arrive(q)
            for side in range(2):
                for k in range(2):
                    value = sum(
                        dot_rows(
                            gathered(x_half[q, part, :, :, k * mk : (k + 1) * mk]),
                            upper_pivot[side, k, :, part * mk : (part + 1) * mk],
                        )
                        for part in range(2)
                    )
                    base = (side * 2 + k) * mk
                    direct[q, :, base : base + mk] = value

    with jax.named_scope("known"):
        guard(g_half.active, known)
    parent_out[...] = sum_par[2].reshape(width, m).T

    for q in chunks:
        with jax.named_scope("all_arrive"):
            g_all.arrive(q)
        with jax.named_scope("all_comp"):
            held = picked[...].reshape(4 * mk, 2 * m)
            value = direct[q] + sum(
                dot_rows(gathered(x_par[2, q, part]), held[:, part * m : (part + 1) * m])
                for part in range(2)
            )
            spread(t_child, q, value, 2 * mk)

    with jax.named_scope("gfinish"):
        for index in range(6):
            mate_rows(index).wait_send()
        for q in chunks:
            for gather in (g_own, g_other, g_low, g_half, g_up, g_all):
                gather.finish(q)
            for side in range(2):

                @pl.when(first + side != me_p)
                def _():
                    shuffle(q, side).wait_send()

    for q in chunks:
        with jax.named_scope("ch_add"):
            t_child.add(q, sum_piv.at[1, q])
    result = sum_piv[1].reshape(width, 2 * mk).T
    for k in range(2):
        child_out[k] = result[k * mk : (k + 1) * mk]
    for q in chunks:
        for scatter in (t_up, t_low, t_high, t_piv, t_child):
            scatter.finish(q)


def shards(panels, cols, *arguments):
    *arrays, maps = arguments
    m, width = arrays[1].shape
    mk = arrays[0].shape[1]
    wide = arrays[8].shape[2]
    if panels != 2 * cols or mk % 128 or m != 2 * mk or m % 256 or wide % 128 or width % (32 * SPLIT):
        return plain_shards(panels, cols, *arguments)
    wj = width // SPLIT // 2
    vm = pltpu.VMEM
    dma = pltpu.SemaphoreType.DMA
    return pl.pallas_call(
        functools.partial(split_kernel, panels, cols),
        out_shape=(
            pltpu.VMEM((m, width), F32),
            pltpu.VMEM((2, mk, width), F32),
        ),
        in_specs=[pl.BlockSpec(memory_space=pl.ANY)] * 9 + [pl.BlockSpec(memory_space=pltpu.VMEM)],
        out_specs=(pl.BlockSpec(memory_space=pltpu.VMEM),) * 2,
        scratch_shapes=[
            *[vm(array.shape, array.dtype) for array in arrays[:3]],
            *[vm((2,) + array.shape, array.dtype) for array in arrays[3:]],
            vm((2, SPLIT, 2, wj, mk), BF),
            vm((2, SPLIT, 2, cols, wj, mk), BF),
            vm((SPLIT, 2, 2 * wj, m // 2), BF),
            vm((SPLIT, 2, 2 * wj, m // 2), BF),
            vm((2, m, m // 2), BF),
            vm((3, SPLIT, 2, wj, m), BF),
            vm((3, SPLIT, 2, cols, wj, m), BF),
            vm((SPLIT, 2, wj, 2 * mk), BF),
            vm((SPLIT, 2, cols, wj, 2 * mk), BF),
            vm((2, 2, mk, 2 * m), BF),
            vm((SPLIT, cols * wj, 4 * mk), F32),
            vm((3, SPLIT, cols, 2, wj, m), BF),
            vm((3, SPLIT, 2, cols, wj, m), BF),
            vm((2, SPLIT, cols, 2, wj, 2 * mk), BF),
            vm((2, SPLIT, 2, cols, wj, 2 * mk), BF),
            vm((3, SPLIT, 2, wj, m), F32),
            vm((2, SPLIT, 2, wj, 2 * mk), F32),
            vm((4, SPLIT, 2, wj, m), F32),
            vm((2, SPLIT, 2, wj, 2 * mk), F32),
            dma((6, SPLIT, 2, panels // 2)),
            dma((6, SPLIT, cols, 2)),
            dma((5, SPLIT, cols, 2)),
            dma((5, SPLIT, 2, cols)),
            dma((SPLIT, 2)),
            dma((SPLIT, 2)),
            dma((9,)),
            dma((6,)),
            dma((6,)),
        ],
        compiler_params=pltpu.CompilerParams(
            collective_id=0, has_side_effects=True, vmem_limit_bytes=60 * 1024 * 1024
        ),
    )(*arrays, maps.reshape(1, -1))


def solution(mesh):
    panels, cols = mesh.shape["panel"], mesh.shape["rhs"]
    placed = (
        P(None, "panel", "rhs"),
        P("panel", "rhs"),
        P("panel", "rhs"),
        P(None, "panel", "rhs"),
        P("panel", "rhs"),
        P("panel", "rhs"),
        P("panel", "rhs"),
        P(None, "panel", "rhs"),
        P(None, "panel", "rhs"),
        P(),
    )
    return jax.shard_map(
        functools.partial(shards, panels, cols),
        mesh=mesh,
        in_specs=placed,
        out_specs=(P("panel", "rhs"), P(None, "panel", "rhs")),
        check_vma=False,
    )
```
